256 devices in a mesh: shell: 16 (over x, z_lo, core), sky: 16 (over y, z_hi).
Axes of the slice: x: 4, y: 4, z: 8 (z_hi: 4, z_lo: 2; z = z_hi * 2 + z_lo), core: 2. Of those that a mesh axis runs over, the one named last changes fastest.
Arguments:
- coords: int32 [3, 16, 16, 512], P(None, 'shell', 'sky'), may hold values from 0 to 4095, as said below
- weights: bfloat16 [16, 16, 512], P('shell', 'sky'), may hold values from 0.5 to 2
- live: int32 [16, 16], P('shell', 'sky'), may hold values from 128 to 512, as said below
Outputs:
- jackknife: float32 [16, 128, 600], P('shell', 'sky')
The draws below stay inside these ranges and needn't reach their ends.
Inputs may be any that keep to these rules, and one draw needn't show every extreme that they name: On device (a, b), coords[0] lies in [a * 256, (a+1) * 256), coords[1] in [b * 256, (b+1) * 256), coords[2] in [0, 1024). `live`: live slots are the first ones of a device; some device is full in every draw.
All inputs are finite; a program needn't handle non-finite values.
Results may differ from the reference program's by a relative error of at most 0.0003.
Values sent between devices are 32-bit elements; how exact they have to be, the bound alone decides.
A program may use at most 64 MiB of HBM per device.

```python
import math
import jax
import jax.numpy as jnp
from jax import lax

PART_DEV = 512
SIDE_CELLS = 256
SPAN_CELLS = 1024
SUBREGIONS = 8
S_BINS = 30
MU_BINS = 20
SHELL_COUNT = 16
PATCH_COUNT = 16
N_SHELL = 16
N_SKY = 16


def draw_coords(key, part):
    keys = jax.random.split(key, 3)
    shape = (SHELL_COUNT, PATCH_COUNT, PART_DEV)
    radial = jax.random.randint(keys[0], shape, 0, SIDE_CELLS) + lax.broadcasted_iota(jnp.int32, shape, 0) * SIDE_CELLS
    across = jax.random.randint(keys[1], shape, 0, SIDE_CELLS) + lax.broadcasted_iota(jnp.int32, shape, 1) * SIDE_CELLS
    depth = jax.random.randint(keys[2], shape, 0, SPAN_CELLS)
    return jnp.stack([radial, across, depth]).astype(jnp.int32)


def draw_live(key, part):
    keys = jax.random.split(key, 2)
    devices = SHELL_COUNT * PATCH_COUNT
    upper = PART_DEV * 3 // 4
    spread = jax.random.randint(keys[0], (devices,), 0, upper + 1)
    counts = PART_DEV // 4 + spread * spread // max(upper, 1)
    chosen = jax.random.randint(keys[1], (), 0, devices)
    counts = jnp.where(jnp.arange(devices) == chosen, PART_DEV, counts)
    return counts.reshape(SHELL_COUNT, PATCH_COUNT).astype(jnp.int32)


def shard_levels(own_key, dims, cuts, least, high):
    factor_of, own = 1.0, jax.random.fold_in(own_key, 6)
    for dim, parts in cuts:
        steps = jnp.exp(jax.random.uniform(jax.random.fold_in(own, dim), (parts,), jnp.float32, least / len(cuts), high / len(cuts)))
        factor_of = factor_of * jnp.repeat(steps, dims[dim] // parts).reshape([-1 if axis == dim else 1 for axis in range(len(dims))])
    return factor_of


def setup_inputs(seed: int = 0) -> dict:
    arg_keys = jax.random.split(jax.random.key(seed), 4)
    return {
        "coords": draw_coords(jax.random.fold_in(arg_keys[3], 71), 0),
        "weights": jnp.clip(jnp.exp(math.log(2.0) - 1.3862944 * jax.random.uniform(arg_keys[1], (SHELL_COUNT, PATCH_COUNT, PART_DEV), jnp.float32) ** shard_levels(arg_keys[1], (SHELL_COUNT, PATCH_COUNT, PART_DEV), ((0, 16), (1, 16)), -0.2, 0.2)), 0.5, 2.0).astype(jnp.bfloat16),
        "live": draw_live(jax.random.fold_in(arg_keys[3], 71), 0),
    }


def edge_values():
    return [int(4.0 * 10.0 ** (4.0 * level / S_BINS) + 0.5) for level in range(S_BINS + 1)]


def bin_scale(patches):
    edges = edge_values()
    factor = SIDE_CELLS * SIDE_CELLS * SPAN_CELLS / (patches * PART_DEV * PART_DEV)
    values = []
    for level in range(S_BINS):
        volume = (4.0 * math.pi / 3.0) * (edges[level + 1] ** 1.5 - edges[level] ** 1.5) / MU_BINS
        values = values + [factor / volume] * MU_BINS
    return jnp.asarray(values, dtype=jnp.float32)


def pair_counts(own_pos, own_weight, far_pos, far_weight):
    edges = edge_values()
    radial_gap = jnp.minimum(jnp.abs(own_pos[0][:, None] - far_pos[0][None, :]), 255)
    across_gap = jnp.minimum(jnp.abs(own_pos[1][:, None] - far_pos[1][None, :]), 255)
    depth_gap = jnp.minimum(jnp.abs(own_pos[2][:, None] - far_pos[2][None, :]), 255)
    squared = radial_gap * radial_gap + across_gap * across_gap + depth_gap * depth_gap
    radial_sq = radial_gap * radial_gap * (MU_BINS * MU_BINS)
    s_index = jnp.zeros_like(squared)
    for level in range(1, S_BINS):
        s_index = s_index + (squared >= edges[level]).astype(jnp.int32)
    mu_index = jnp.zeros_like(squared)
    for level in range(1, MU_BINS):
        mu_index = mu_index + (radial_sq >= level * level * squared).astype(jnp.int32)
    inside = (squared >= edges[0]) & (squared < edges[S_BINS])
    region = own_pos[2] // (SPAN_CELLS // SUBREGIONS)
    segment = jnp.where(inside, region[:, None] * (S_BINS * MU_BINS) + s_index * MU_BINS + mu_index,
                        SUBREGIONS * S_BINS * MU_BINS).astype(jnp.int32)
    pair_weight = own_weight[:, None] * far_weight[None, :]
    totals = jax.ops.segment_sum(pair_weight.reshape(-1), segment.reshape(-1),
                                 num_segments=SUBREGIONS * S_BINS * MU_BINS + 1)
    return totals[:-1]


def reference(coords, weights, live):
    slots = jnp.arange(PART_DEV, dtype=jnp.int32)
    masked = jnp.where(slots[None, None, :] < live[:, :, None], weights.astype(jnp.float32), jnp.float32(0.0))
    pos_padded = jnp.pad(coords, ((0, 0), (1, 1), (1, 1), (0, 0)))
    weight_padded = jnp.pad(masked, ((1, 1), (1, 1), (0, 0)))
    tile_rows = min(256, PART_DEV)
    zero = jnp.int32(0)

    def one_device(flat):
        shell_at = (flat // N_SKY).astype(jnp.int32)
        patch_at = (flat % N_SKY).astype(jnp.int32)
        far_pos = lax.dynamic_slice(pos_padded, (zero, shell_at, patch_at, zero), (3, 3, 3, PART_DEV)).reshape(3, 9 * PART_DEV)
        far_weight = lax.dynamic_slice(weight_padded, (shell_at, patch_at, zero), (3, 3, PART_DEV)).reshape(9 * PART_DEV)
        own_pos = lax.dynamic_slice(coords, (zero, shell_at, patch_at, zero), (3, 1, 1, PART_DEV)).reshape(3, PART_DEV)
        own_weight = lax.dynamic_slice(masked, (shell_at, patch_at, zero), (1, 1, PART_DEV)).reshape(PART_DEV)

        def one_tile(index):
            start = (index * tile_rows).astype(jnp.int32)
            rows_pos = lax.dynamic_slice_in_dim(own_pos, start, tile_rows, 1)
            rows_weight = lax.dynamic_slice_in_dim(own_weight, start, tile_rows, 0)
            return pair_counts(rows_pos, rows_weight, far_pos, far_weight)

        return jnp.sum(lax.map(one_tile, jnp.arange(PART_DEV // tile_rows, dtype=jnp.int32)), axis=0)

    hists = lax.map(one_device, jnp.arange(N_SHELL * N_SKY, dtype=jnp.int32))
    hists = hists.reshape(N_SHELL, N_SKY, SUBREGIONS, S_BINS * MU_BINS)
    totals = jnp.sum(hists, axis=(1, 2))
    leave = totals[:, None, None, :] - hists
    return (leave * bin_scale(N_SKY)).reshape(N_SHELL, N_SKY * SUBREGIONS, S_BINS * MU_BINS)
```

```python
import functools, math
import jax, jax.numpy as jnp
from jax import lax
from jax.experimental import pallas as pl
from jax.experimental.pallas import tpu as pltpu
from jax.sharding import PartitionSpec as P

PART_DEV = 512
SIDE_CELLS = 256
SPAN_CELLS = 1024
SUBREGIONS = 8
S_BINS = 30
MU_BINS = 20
REACH = 199
GROUPS = 24
STEP = 16
ROWS = PART_DEV // STEP
DIRS = tuple((da, db) for da in (-1, 0, 1) for db in (-1, 0, 1) if (da, db) != (0, 0))
F32 = jnp.float32
BF16 = jnp.bfloat16


def sort_kernel(live_ref, coords_ref, weight_ref, lists_ref, own_ref, start_ref):
    def body(acc0, acc1, acc2, acc3, tall0, tall1):
        for acc in (acc0, acc1, acc2, acc3, tall0, tall1):
            pltpu.matmul_pop(acc)
        n = PART_DEV
        x = (coords_ref[0:1, :] & (SIDE_CELLS - 1)).astype(F32)
        y = (coords_ref[1:2, :] & (SIDE_CELLS - 1)).astype(F32)
        zi = coords_ref[2:3, :]
        region = zi >> 7
        z_high = region.astype(F32)
        z_low = (zi & 127).astype(F32)
        slot = lax.broadcasted_iota(jnp.int32, (1, n), 1)
        alive = slot < live_ref[0, 0]
        w = jnp.where(alive, weight_ref[0:1, :].astype(F32), 0.0)
        key = (jnp.where(alive, zi * n, SPAN_CELLS * n) + slot).astype(F32)
        key_column = jnp.transpose(jnp.broadcast_to(key, (128, n)))[:, 0:1]
        before = jnp.where(key_column < key, 1.0, 0.0).astype(BF16)
        valid = []
        for da, db in DIRS:
            ok = alive
            if da > 0:
                ok = ok & (x >= SIDE_CELLS - REACH)
            if da < 0:
                ok = ok & (x <= REACH - 1)
            if db > 0:
                ok = ok & (y >= SIDE_CELLS - REACH)
            if db < 0:
                ok = ok & (y <= REACH - 1)
            valid.append(ok)
        valid.append(alive)
        ones = [jnp.where(ok, 1.0, 0.0) for ok in valid]
        flags = jnp.concatenate(ones + [jnp.zeros((7, n), F32)], axis=0).astype(BF16)
        for half in range(2):
            rows = slice(256 * half, 256 * half + 256)
            pltpu.matmul_push_rhs(before[rows, 0:256], staging_register=0, mxu_index=0)
            pltpu.matmul_acc_lhs(acc0, flags[:, rows], load_staged_rhs=0)
            pltpu.matmul_push_rhs(before[rows, 256:512], staging_register=0, mxu_index=1)
            pltpu.matmul_acc_lhs(acc1, flags[:, rows], load_staged_rhs=0)
        rank = jnp.concatenate([pltpu.matmul_pop(acc0), pltpu.matmul_pop(acc1)], axis=1)
        attrs = jnp.concatenate([x, y, z_high, z_low, w, jnp.zeros((11, n), F32)], axis=0).astype(BF16)
        place = lax.broadcasted_iota(jnp.int32, (n, 1), 0).astype(F32)
        accs = ((acc0, acc1), (acc2, acc3))
        for d in range(9):
            target = jnp.where(valid[d], rank[d : d + 1, :], -1.0)
            hot = jnp.where(place == target, 1.0, 0.0).astype(BF16)
            pair = accs[d % 2]
            for half in range(2):
                cols = slice(256 * half, 256 * half + 256)
                for mxu in range(2):
                    pltpu.matmul_push_rhs(hot[256 * mxu : 256 * mxu + 256, cols], staging_register=0, mxu_index=mxu, transpose=True)
                    pltpu.matmul_acc_lhs(pair[mxu], attrs[:, cols], load_staged_rhs=0)
            da, db = DIRS[d] if d < 8 else (0, 0)
            for mxu in range(2):
                got = pltpu.matmul_pop(pair[mxu])
                lanes = slice(256 * mxu, 256 * mxu + 256)
                lists_ref[d, 0:1, lanes] = got[0:1] - float(SIDE_CELLS * da)
                lists_ref[d, 1:2, lanes] = got[1:2] - float(SIDE_CELLS * db)
                lists_ref[d, 2:3, lanes] = got[2:3] * 128.0 + got[3:4]
                lists_ref[d, 3:4, lanes] = got[4:5]
        shift = jnp.zeros((1, n), F32)
        first = jnp.zeros((1, 1), F32)
        group = jnp.zeros((1, 1), F32)
        starts = []
        for r in range(SUBREGIONS):
            here = alive & (region == r)
            starts.append(group)
            shift = jnp.where(here, 32.0 * group - first, shift)
            count = jnp.sum(jnp.where(here, 1.0, 0.0), axis=1, keepdims=True)
            first = first + count
            group = group + jnp.floor((count + 31.0) * (1.0 / 32.0))
        starts = starts + [group]
        row = lax.broadcasted_iota(jnp.int32, (8, 128), 1)
        table = jnp.zeros((8, 128), F32)
        for r in range(9):
            table = jnp.where(row == r, starts[r], table)
        start_ref[...] = table.astype(jnp.int32)
        target = jnp.where(alive, rank[8:9, :] + shift, -1.0)
        wide = lax.broadcasted_iota(jnp.int32, (GROUPS * 32, 1), 0).astype(F32)
        hot = jnp.where(wide == target, 1.0, 0.0).astype(BF16)
        rhs = jnp.concatenate([attrs, jnp.zeros((240, n), BF16)], axis=0)
        half_rows = GROUPS * 16
        for half in range(2):
            cols = slice(256 * half, 256 * half + 256)
            for mxu, acc in ((0, tall0), (1, tall1)):
                pltpu.matmul_push_rhs(rhs[:, cols], staging_register=0, mxu_index=mxu, transpose=True)
                pltpu.matmul_acc_lhs(acc, hot[half_rows * mxu : half_rows * mxu + half_rows, cols], load_staged_rhs=0)
        lane = lax.broadcasted_iota(jnp.int32, (8, 128), 1) // 32
        for mxu, acc in ((0, tall0), (1, tall1)):
            got = pltpu.matmul_pop(acc)[:, 0:128]
            for g in range(GROUPS // 2):
                parts = []
                for q in range(4):
                    block = got[32 * g + 8 * q : 32 * g + 8 * q + 8]
                    deep = block[:, 2:3] * 128.0 + block[:, 3:4]
                    parts.append([jnp.broadcast_to(v, (8, 128)) for v in (block[:, 0:1], block[:, 1:2], deep, block[:, 4:5])])
                for k in range(4):
                    value = parts[0][k]
                    for q in range(1, 4):
                        value = jnp.where(lane == q, parts[q][k], value)
                    own_ref[k, mxu * (GROUPS // 2) + g] = value

    pl.run_scoped(
        body,
        pltpu.ACC(0)((16, 256), F32),
        pltpu.ACC(1)((16, 256), F32),
        pltpu.ACC(0)((16, 256), F32),
        pltpu.ACC(1)((16, 256), F32),
        pltpu.ACC(0)((GROUPS * 16, 256), F32),
        pltpu.ACC(1)((GROUPS * 16, 256), F32),
    )


def sort_call(coords, weights, live):
    return pl.pallas_call(
        sort_kernel,
        out_shape=(
            jax.ShapeDtypeStruct((9, 4, PART_DEV), F32),
            jax.ShapeDtypeStruct((4, GROUPS, 8, 128), F32),
            jax.ShapeDtypeStruct((8, 128), jnp.int32),
        ),
        in_specs=[
            pl.BlockSpec(memory_space=pltpu.SMEM),
            pl.BlockSpec(memory_space=pltpu.VMEM),
            pl.BlockSpec(memory_space=pltpu.VMEM),
        ],
        out_specs=[pl.BlockSpec(memory_space=pltpu.VMEM)] * 3,
    )(live, coords, weights)


LOG_SCALE = (S_BINS / 4.0) / math.log2(10.0)
LOG_BASE = -4.515457845
LEVELS_U = 24
LEVELS_V = 25
TILES = 4
V_ROWS = 208
DUMMY = 9 * ROWS


def count_kernel(start_ref, lists_ref, got_ref, own_ref, out_ref, rows_ref, table_ref, table_sm, hot_u, hot_v, sem):
    def body(a0, a1, b0, b1):
        sets = ((a0, a1), (b0, b1))
        for acc in (a0, a1, b0, b1):
            pltpu.matmul_pop(acc)
        zs, ws = own_ref[2], own_ref[3]
        z_min = jnp.min(jnp.min(jnp.where(ws > 0.0, zs, 1e6), axis=1), axis=1, keepdims=True)
        z_max = jnp.max(jnp.max(jnp.where(ws > 0.0, zs, -1e6), axis=1), axis=1, keepdims=True)
        lane = lax.broadcasted_iota(jnp.int32, (GROUPS, 256), 1).astype(F32)
        table = jnp.full((GROUPS, 256), float(DUMMY), F32)
        total = jnp.zeros((GROUPS, 1), F32)
        for d in range(9):
            src = lists_ref.at[8] if d == 8 else got_ref.at[d]
            z_row = jnp.where(src[3:4, :] > 0.0, src[2:3, :], 2e6)
            low = jnp.sum(jnp.where(z_row < z_min - float(REACH), 1.0, 0.0), axis=1, keepdims=True)
            high = jnp.sum(jnp.where(z_row <= z_max + float(REACH), 1.0, 0.0), axis=1, keepdims=True)
            first = jnp.floor(low * (1.0 / STEP))
            count = jnp.where(high > low, jnp.floor((high - STEP * first + 31.0) * (1.0 / 32.0)), 0.0)
            at = lane - total
            table = jnp.where((at >= 0.0) & (at < count), at * 2.0 + (first + float(ROWS * d)), table)
            total = total + count
        batches = jnp.floor((total + (TILES - 1.0)) * (1.0 / TILES))
        table = jnp.where(lane == 255.0, batches, table)
        table_ref[0:GROUPS, :] = table.astype(jnp.int32)
        tail = lax.broadcasted_iota(jnp.int32, (8, 256), 1)
        table_ref[GROUPS : GROUPS + 8, :] = jnp.where(tail == 255, 1 << 20, DUMMY)
        copy = pltpu.make_async_copy(table_ref, table_sm, sem)
        copy.start()
        lane = lax.broadcasted_iota(jnp.int32, (8, 128), 1)
        for d in range(9):
            src = lists_ref.at[8] if d == 8 else got_ref.at[d]
            wide = []
            for t in range(4):
                block = src[:, 128 * t : 128 * t + 128]
                block = jnp.concatenate([block, block], axis=0)
                for k in range(4):
                    part = block if k == 0 else pltpu.roll(block, 128 - 32 * k, 1)
                    part = jnp.where(lane < 32, part, pltpu.roll(part, 32, 1))
                    part = jnp.where(lane < 64, part, pltpu.roll(part, 64, 1))
                    wide.append(part)
            turned = [pltpu.roll(part, 16, 1) for part in wide] + [jnp.zeros((8, 128), F32)]
            for k in range(16):
                rows_ref[ROWS * d + 2 * k] = wide[k]
                rows_ref[ROWS * d + 2 * k + 1] = jnp.where((lane & 31) < 16, turned[k], turned[k + 1])
        rows_ref[DUMMY] = jnp.zeros((8, 128), F32)
        for buf in range(2):
            hot_u[buf, 8 * LEVELS_U :, :] = jnp.zeros((256 - 8 * LEVELS_U, 128 * TILES), BF16)
        copy.wait()
        trips = []
        for r in range(SUBREGIONS):
            begin, end = start_ref[0, r], start_ref[0, r + 1]
            number = lax.fori_loop(begin, end, lambda g, n: n + table_sm[g, 255], jnp.int32(0))
            last = jnp.maximum(end - 1, 0)

            @pl.when(number % 2 == 1)
            def _():
                table_sm[last, 255] = table_sm[last, 255] + 1

            trips.append((number + 1) // 2)

        zero = jnp.zeros((16, 128), BF16)

        stop = start_ref[0, SUBREGIONS]

        def fill(state, buf):
            g, b = state
            group = jnp.minimum(g, GROUPS - 1)
            xi, yi, zi, wi = own_ref[0, group], own_ref[1, group], own_ref[2, group], own_ref[3, group]
            w_own = jnp.concatenate([wi, wi], axis=0).astype(BF16)
            for t in range(TILES):
                row = table_sm[g, TILES * b + t]
                dx = xi - rows_ref[row, 0:1, :]
                dy = yi - rows_ref[row, 1:2, :]
                dz = zi - rows_ref[row, 2:3, :]
                w_far = jnp.broadcast_to(rows_ref[row, 3:4, :].astype(BF16), (16, 128))
                dx2 = dx * dx
                q = dx2 + dy * dy + dz * dz
                s = jnp.floor(jnp.log2(q + 0.48) * LOG_SCALE + LOG_BASE)
                near = jnp.floor(jnp.abs(dx) * lax.rsqrt(q) * float(MU_BINS) + 0.5)
                mu = jnp.where(near * near * q > dx2 * float(MU_BINS * MU_BINS), near - 1.0, near)
                c = s * float(MU_BINS) + jnp.minimum(mu, MU_BINS - 1.0)
                u = jnp.floor(c * (1.0 / LEVELS_V) + 0.01)
                v = c - u * float(LEVELS_V)
                u2 = jnp.concatenate([u, u - 1.0], axis=0).astype(BF16)
                v2 = jnp.concatenate([v, v - 1.0], axis=0).astype(BF16)
                lanes = slice(128 * t, 128 * t + 128)
                for k in range(LEVELS_U // 2):
                    hot_u[buf, 16 * k : 16 * k + 16, lanes] = jnp.where(u2 == jnp.bfloat16(2 * k), w_far, zero)
                for k in range(V_ROWS // 16):
                    hot_v[buf, 16 * k : 16 * k + 16, lanes] = jnp.where(v2 == jnp.bfloat16(2 * k), w_own, zero)
            b = b + 1
            over = b >= table_sm[g, 255]
            g = jnp.where(over, g + 1, g)
            g = jnp.where(g >= stop, GROUPS, g)
            return g, jnp.where(over, 0, b)

        def push(buf):
            for mxu in range(2):
                pltpu.matmul_push_rhs(hot_u[buf, :, 256 * mxu : 256 * mxu + 256], staging_register=buf, mxu_index=mxu, transpose=True)

        def multiply(buf, accs):
            for mxu in range(2):
                pltpu.matmul_acc_lhs(accs[mxu], hot_v[buf, :, 256 * mxu : 256 * mxu + 256], load_staged_rhs=buf)

        state = (jnp.where(stop > 0, 0, GROUPS).astype(jnp.int32), jnp.int32(0))
        state = fill(state, 0)
        push(0)
        state = fill(state, 1)
        sub = lax.broadcasted_iota(jnp.int32, (8, 256), 0)
        diagonal = sub == (lax.broadcasted_iota(jnp.int32, (8, 256), 1) & 7)

        def drain(r):
            accs = sets[r % 2]
            both = pltpu.matmul_pop(accs[0]) + pltpu.matmul_pop(accs[1])
            for v in range(V_ROWS // 8):
                out_ref[r, v : v + 1, :] = jnp.sum(jnp.where(diagonal, both[8 * v : 8 * v + 8], 0.0), axis=0, keepdims=True)
            out_ref[r, V_ROWS // 8 :, :] = jnp.zeros((32 - V_ROWS // 8, 256), F32)

        for r in range(SUBREGIONS):
            accs = sets[r % 2]

            def trip(_, state):
                push(1)
                multiply(0, accs)
                state = fill(state, 0)
                push(0)
                multiply(1, accs)
                return fill(state, 1)

            state = lax.fori_loop(0, trips[r], trip, state)
            if r > 0:
                drain(r - 1)
        multiply(0, sets[(SUBREGIONS - 1) % 2])
        drain(SUBREGIONS - 1)

    pl.run_scoped(
        body,
        pltpu.ACC(0)((V_ROWS, 256), F32),
        pltpu.ACC(1)((V_ROWS, 256), F32),
        pltpu.ACC(0)((V_ROWS, 256), F32),
        pltpu.ACC(1)((V_ROWS, 256), F32),
    )


def count_call(start, lists, got, own):
    vmem = pl.BlockSpec(memory_space=pltpu.VMEM)
    return pl.pallas_call(
        count_kernel,
        out_shape=jax.ShapeDtypeStruct((SUBREGIONS, 32, 256), F32),
        in_specs=[pl.BlockSpec(memory_space=pltpu.SMEM), vmem, vmem, vmem],
        out_specs=vmem,
        scratch_shapes=[
            pltpu.VMEM((DUMMY + 1, 8, 128), F32),
            pltpu.VMEM((32, 256), jnp.int32),
            pltpu.SMEM((32, 256), jnp.int32),
            pltpu.VMEM((2, 256, 128 * TILES), BF16),
            pltpu.VMEM((2, V_ROWS, 128 * TILES), BF16),
            pltpu.SemaphoreType.DMA,
        ],
    )(start, lists, got, own)


MESH = pl.DeviceIdType.MESH


def halo_kernel(lists_ref, got_ref, send_sem, recv_sem):
    shell, sky = lax.axis_index("shell"), lax.axis_index("sky")
    shells, skies = lax.axis_size("shell"), lax.axis_size("sky")
    barrier = pltpu.get_barrier_semaphore()

    def present(da, db):
        a, b = shell + da, sky + db
        return (a >= 0) & (a < shells) & (b >= 0) & (b < skies)

    for da, db in DIRS:

        @pl.when(present(da, db))
        def _():
            pl.semaphore_signal(barrier, inc=1, device_id=(shell + da, sky + db), device_id_type=MESH)

    for d, (da, db) in enumerate(DIRS):

        @pl.when(jnp.logical_not(present(da, db)))
        def _():
            got_ref[d] = jnp.zeros((4, PART_DEV), F32)

    beside_shell = 1 + (shell > 0).astype(jnp.int32) + (shell < shells - 1).astype(jnp.int32)
    beside_sky = 1 + (sky > 0).astype(jnp.int32) + (sky < skies - 1).astype(jnp.int32)
    pl.semaphore_wait(barrier, beside_shell * beside_sky - 1)

    def copy(d):
        da, db = DIRS[d]
        return pltpu.make_async_remote_copy(
            src_ref=lists_ref.at[d],
            dst_ref=got_ref.at[7 - d],
            send_sem=send_sem.at[d],
            recv_sem=recv_sem.at[7 - d],
            device_id=(shell + da, sky + db),
            device_id_type=MESH,
        )

    for d, (da, db) in enumerate(DIRS):

        @pl.when(present(da, db))
        def _():
            copy(d).start()

    for d, (da, db) in enumerate(DIRS):

        @pl.when(present(da, db))
        def _():
            copy(d).wait_send()

        @pl.when(present(-da, -db))
        def _():
            copy(d).wait_recv()


def halo_call(lists):
    return pl.pallas_call(
        halo_kernel,
        out_shape=jax.ShapeDtypeStruct((8, 4, PART_DEV), F32),
        in_specs=[pl.BlockSpec(memory_space=pltpu.VMEM)],
        out_specs=pl.BlockSpec(memory_space=pltpu.VMEM),
        scratch_shapes=[pltpu.SemaphoreType.DMA((8,)), pltpu.SemaphoreType.DMA((8,))],
        compiler_params=pltpu.CompilerParams(collective_id=0, has_side_effects=True),
    )(lists)


def total_kernel(skies, counts_ref, own_ref, total_ref, sent_ref, land_ref, send_sem, recv_sem):
    shell, sky = lax.axis_index("shell"), lax.axis_index("sky")
    barrier = pltpu.get_barrier_semaphore()
    for k in range(1, skies):
        pl.semaphore_signal(barrier, inc=1, device_id=(shell, lax.rem(sky + k, skies)), device_id_type=MESH)
    lane_in = lax.broadcasted_iota(jnp.int32, (256, 128), 0)
    lane_out = lax.broadcasted_iota(jnp.int32, (256, 128), 1)
    packed = jnp.zeros((8 * SUBREGIONS, 128), F32)
    for k in range(4):
        rows = jnp.concatenate([counts_ref[r, 8 * k : 8 * k + 8, :] for r in range(SUBREGIONS)], axis=0)
        pick = jnp.where((lane_in >> 3) + 32 * k == lane_out, 1.0, 0.0)
        packed = packed + jnp.dot(rows, pick, precision=lax.Precision.HIGHEST, preferred_element_type=F32)
    own_ref[...] = packed
    mine = packed[0:8]
    for r in range(1, SUBREGIONS):
        mine = mine + packed[8 * r : 8 * r + 8]
    sent_ref[...] = mine
    pl.semaphore_wait(barrier, skies - 1)

    def copy(k):
        return pltpu.make_async_remote_copy(
            src_ref=sent_ref,
            dst_ref=land_ref.at[k - 1],
            send_sem=send_sem.at[k - 1],
            recv_sem=recv_sem.at[k - 1],
            device_id=(shell, lax.rem(sky + k, skies)),
            device_id_type=MESH,
        )

    for k in range(1, skies):
        copy(k).start()
    total = mine
    for k in range(1, skies):
        copy(k).wait_recv()
        total = total + land_ref[k - 1]
    total_ref[...] = total
    for k in range(1, skies):
        copy(k).wait_send()


def total_call(counts):
    skies = lax.axis_size("sky")
    vmem = pl.BlockSpec(memory_space=pltpu.VMEM)
    return pl.pallas_call(
        functools.partial(total_kernel, skies),
        out_shape=(jax.ShapeDtypeStruct((8 * SUBREGIONS, 128), F32), jax.ShapeDtypeStruct((8, 128), F32)),
        in_specs=[vmem],
        out_specs=(vmem, vmem),
        scratch_shapes=[
            pltpu.VMEM((8, 128), F32),
            pltpu.VMEM((skies - 1, 8, 128), F32),
            pltpu.SemaphoreType.DMA((skies - 1,)),
            pltpu.SemaphoreType.DMA((skies - 1,)),
        ],
        compiler_params=pltpu.CompilerParams(collective_id=1, has_side_effects=True),
    )(counts)


def edge_values():
    return [int(4.0 * 10.0 ** (4.0 * level / S_BINS) + 0.5) for level in range(S_BINS + 1)]


def bin_scale(patches):
    edges = edge_values()
    factor = SIDE_CELLS * SIDE_CELLS * SPAN_CELLS / (patches * PART_DEV * PART_DEV)
    values = []
    for level in range(S_BINS):
        volume = 4.0 * math.pi / 3.0 * (edges[level + 1] ** 1.5 - edges[level] ** 1.5) / MU_BINS
        values = values + [factor / volume] * MU_BINS
    return jnp.asarray(values, dtype=F32)


def unpacked(x):
    x = x.reshape(-1, 8, 4, 32).transpose(0, 3, 2, 1).reshape(-1, 32, 32)
    return x[:, :LEVELS_U, :LEVELS_V].reshape(-1, S_BINS * MU_BINS)


def local(coords, weights, live):
    lists, own, start = sort_call(coords.reshape(3, PART_DEV), weights.reshape(1, PART_DEV), live)
    counts = count_call(start, lists, halo_call(lists), own)
    packed, total = total_call(counts)
    leave = total[None] - packed.reshape(SUBREGIONS, 8, 128)
    return (unpacked(leave) * bin_scale(lax.axis_size("sky"))[None, :])[None]


def solution(mesh):
    in_specs = (P(None, "shell", "sky", None), P("shell", "sky", None), P("shell", "sky"))
    out_specs = P("shell", "sky", None)
    return jax.shard_map(local, mesh=mesh, in_specs=in_specs, out_specs=out_specs, check_vma=False)
```

```python
import functools, math
import jax, jax.numpy as jnp
from jax import lax
from jax.experimental import pallas as pl
from jax.experimental.pallas import tpu as pltpu
from jax.sharding import PartitionSpec as P

PART_DEV = 512
SIDE_CELLS = 256
SPAN_CELLS = 1024
SUBREGIONS = 8
S_BINS = 30
MU_BINS = 20
REACH = 199
GROUPS = 24
STEP = 16
ROWS = PART_DEV // STEP
DIRS = tuple((da, db) for da in (-1, 0, 1) for db in (-1, 0, 1) if (da, db) != (0, 0))
F32 = jnp.float32
BF16 = jnp.bfloat16


def sort_kernel(live_ref, coords_ref, weight_ref, lists_ref, own_ref, start_ref):
    def body(acc0, acc1, acc2, acc3, tall0, tall1):
        for acc in (acc0, acc1, acc2, acc3, tall0, tall1):
            pltpu.matmul_pop(acc)
        n = PART_DEV
        x = (coords_ref[0, 0] & (SIDE_CELLS - 1)).astype(F32)
        y = (coords_ref[1, 0] & (SIDE_CELLS - 1)).astype(F32)
        zi = coords_ref[2, 0]
        region = zi >> 7
        z_high = region.astype(F32)
        z_low = (zi & 127).astype(F32)
        slot = lax.broadcasted_iota(jnp.int32, (1, n), 1)
        alive = slot < live_ref[0, 0]
        w = jnp.where(alive, weight_ref[0].astype(F32), 0.0)
        key = (jnp.where(alive, zi * n, SPAN_CELLS * n) + slot).astype(F32)
        key_column = jnp.transpose(jnp.broadcast_to(key, (128, n)))[:, 0:1]
        before = jnp.where(key_column < key, 1.0, 0.0).astype(BF16)
        valid = []
        for da, db in DIRS:
            ok = alive
            if da > 0:
                ok = ok & (x >= SIDE_CELLS - REACH)
            if da < 0:
                ok = ok & (x <= REACH - 1)
            if db > 0:
                ok = ok & (y >= SIDE_CELLS - REACH)
            if db < 0:
                ok = ok & (y <= REACH - 1)
            valid.append(ok)
        valid.append(alive)
        ones = [jnp.where(ok, 1.0, 0.0) for ok in valid]
        flags = jnp.concatenate(ones + [jnp.zeros((7, n), F32)], axis=0).astype(BF16)
        for half in range(2):
            rows = slice(256 * half, 256 * half + 256)
            pltpu.matmul_push_rhs(before[rows, 0:256], staging_register=0, mxu_index=0)
            pltpu.matmul_acc_lhs(acc0, flags[:, rows], load_staged_rhs=0)
            pltpu.matmul_push_rhs(before[rows, 256:512], staging_register=0, mxu_index=1)
            pltpu.matmul_acc_lhs(acc1, flags[:, rows], load_staged_rhs=0)
        rank = jnp.concatenate([pltpu.matmul_pop(acc0), pltpu.matmul_pop(acc1)], axis=1)
        attrs = jnp.concatenate([x, y, z_high, z_low, w, jnp.zeros((11, n), F32)], axis=0).astype(BF16)
        place = lax.broadcasted_iota(jnp.int32, (n, 1), 0).astype(F32)
        accs = ((acc0, acc1), (acc2, acc3))
        for d in range(9):
            target = jnp.where(valid[d], rank[d : d + 1, :], -1.0)
            hot = jnp.where(place == target, 1.0, 0.0).astype(BF16)
            pair = accs[d % 2]
            for half in range(2):
                cols = slice(256 * half, 256 * half + 256)
                for mxu in range(2):
                    pltpu.matmul_push_rhs(hot[256 * mxu : 256 * mxu + 256, cols], staging_register=0, mxu_index=mxu, transpose=True)
                    pltpu.matmul_acc_lhs(pair[mxu], attrs[:, cols], load_staged_rhs=0)
            da, db = DIRS[d] if d < 8 else (0, 0)
            for mxu in range(2):
                got = pltpu.matmul_pop(pair[mxu])
                lanes = slice(256 * mxu, 256 * mxu + 256)
                lists_ref[d, 0:1, lanes] = got[0:1] - float(SIDE_CELLS * da)
                lists_ref[d, 1:2, lanes] = got[1:2] - float(SIDE_CELLS * db)
                lists_ref[d, 2:3, lanes] = got[2:3] * 128.0 + got[3:4]
                lists_ref[d, 3:4, lanes] = got[4:5]
        shift = jnp.zeros((1, n), F32)
        first = jnp.zeros((1, 1), F32)
        group = jnp.zeros((1, 1), F32)
        starts = []
        for r in range(SUBREGIONS):
            here = alive & (region == r)
            starts.append(group)
            shift = jnp.where(here, 32.0 * group - first, shift)
            count = jnp.sum(jnp.where(here, 1.0, 0.0), axis=1, keepdims=True)
            first = first + count
            group = group + jnp.floor((count + 31.0) * (1.0 / 32.0))
        starts = starts + [group]
        row = lax.broadcasted_iota(jnp.int32, (8, 128), 1)
        table = jnp.zeros((8, 128), F32)
        for r in range(9):
            table = jnp.where(row == r, starts[r], table)
        start_ref[...] = table.astype(jnp.int32)
        target = jnp.where(alive, rank[8:9, :] + shift, -1.0)
        wide = lax.broadcasted_iota(jnp.int32, (GROUPS * 32, 1), 0).astype(F32)
        hot = jnp.where(wide == target, 1.0, 0.0).astype(BF16)
        rhs = jnp.concatenate([attrs, jnp.zeros((240, n), BF16)], axis=0)
        half_rows = GROUPS * 16
        for half in range(2):
            cols = slice(256 * half, 256 * half + 256)
            for mxu, acc in ((0, tall0), (1, tall1)):
                pltpu.matmul_push_rhs(rhs[:, cols], staging_register=0, mxu_index=mxu, transpose=True)
                pltpu.matmul_acc_lhs(acc, hot[half_rows * mxu : half_rows * mxu + half_rows, cols], load_staged_rhs=0)
        lane = lax.broadcasted_iota(jnp.int32, (8, 128), 1) // 32
        for mxu, acc in ((0, tall0), (1, tall1)):
            got = pltpu.matmul_pop(acc)[:, 0:128]
            for g in range(GROUPS // 2):
                parts = []
                for q in range(4):
                    block = got[32 * g + 8 * q : 32 * g + 8 * q + 8]
                    deep = block[:, 2:3] * 128.0 + block[:, 3:4]
                    parts.append([jnp.broadcast_to(v, (8, 128)) for v in (block[:, 0:1], block[:, 1:2], deep, block[:, 4:5])])
                for k in range(4):
                    value = parts[0][k]
                    for q in range(1, 4):
                        value = jnp.where(lane == q, parts[q][k], value)
                    own_ref[k, mxu * (GROUPS // 2) + g] = value

    pl.run_scoped(
        body,
        pltpu.ACC(0)((16, 256), F32),
        pltpu.ACC(1)((16, 256), F32),
        pltpu.ACC(0)((16, 256), F32),
        pltpu.ACC(1)((16, 256), F32),
        pltpu.ACC(0)((GROUPS * 16, 256), F32),
        pltpu.ACC(1)((GROUPS * 16, 256), F32),
    )


def sort_call(coords, weights, live):
    return pl.pallas_call(
        sort_kernel,
        out_shape=(
            jax.ShapeDtypeStruct((9, 4, PART_DEV), F32),
            jax.ShapeDtypeStruct((4, GROUPS, 8, 128), F32),
            jax.ShapeDtypeStruct((8, 128), jnp.int32),
        ),
        in_specs=[
            pl.BlockSpec(memory_space=pltpu.SMEM),
            pl.BlockSpec(memory_space=pltpu.VMEM),
            pl.BlockSpec(memory_space=pltpu.VMEM),
        ],
        out_specs=[pl.BlockSpec(memory_space=pltpu.VMEM)] * 3,
        compiler_params=pltpu.CompilerParams(vmem_limit_bytes=8 << 20),
    )(live, coords, weights)


LOG_SCALE = (S_BINS / 4.0) / math.log2(10.0)
LOG_BASE = -4.515457845
LEVELS_U = 24
LEVELS_V = 25
TILES = 4
V_ROWS = 208
DUMMY = 9 * ROWS


def count_kernel(start_ref, lists_ref, got_ref, own_ref, out_ref, rows_ref, table_ref, table_sm, sem):
    def body(a0, a1, b0, b1, hot_u, hot_v, bin_u, bin_v, far_w, own_w):
        sets = ((a0, a1), (b0, b1))
        for acc in (a0, a1, b0, b1):
            pltpu.matmul_pop(acc)
        zs, ws = own_ref[2], own_ref[3]
        z_min = jnp.min(jnp.min(jnp.where(ws > 0.0, zs, 1e6), axis=1), axis=1, keepdims=True)
        z_max = jnp.max(jnp.max(jnp.where(ws > 0.0, zs, -1e6), axis=1), axis=1, keepdims=True)
        lane = lax.broadcasted_iota(jnp.int32, (GROUPS, 256), 1).astype(F32)
        table = jnp.full((GROUPS, 256), float(DUMMY), F32)
        total = jnp.zeros((GROUPS, 1), F32)
        for d in range(9):
            src = lists_ref.at[8] if d == 8 else got_ref.at[d]
            z_row = jnp.where(src[3:4, :] > 0.0, src[2:3, :], 2e6)
            low = jnp.sum(jnp.where(z_row < z_min - float(REACH), 1.0, 0.0), axis=1, keepdims=True)
            high = jnp.sum(jnp.where(z_row <= z_max + float(REACH), 1.0, 0.0), axis=1, keepdims=True)
            first = jnp.floor(low * (1.0 / STEP))
            count = jnp.where(high > low, jnp.floor((high - STEP * first + 31.0) * (1.0 / 32.0)), 0.0)
            at = lane - total
            table = jnp.where((at >= 0.0) & (at < count), at * 2.0 + (first + float(ROWS * d)), table)
            total = total + count
        batches = jnp.floor((total + (TILES - 1.0)) * (1.0 / TILES))
        table = jnp.where(lane == 255.0, batches, table)
        table_ref[0:GROUPS, :] = table.astype(jnp.int32)
        tail = lax.broadcasted_iota(jnp.int32, (8, 256), 1)
        table_ref[GROUPS : GROUPS + 8, :] = jnp.where(tail == 255, 1 << 20, DUMMY)
        copy = pltpu.make_async_copy(table_ref, table_sm, sem)
        copy.start()
        lane = lax.broadcasted_iota(jnp.int32, (8, 128), 1)
        for d in range(9):
            src = lists_ref.at[8] if d == 8 else got_ref.at[d]
            wide = []
            for t in range(4):
                block = src[:, 128 * t : 128 * t + 128]
                block = jnp.concatenate([block, block], axis=0)
                for k in range(4):
                    part = block if k == 0 else pltpu.roll(block, 128 - 32 * k, 1)
                    part = jnp.where(lane < 32, part, pltpu.roll(part, 32, 1))
                    part = jnp.where(lane < 64, part, pltpu.roll(part, 64, 1))
                    wide.append(part)
            turned = [pltpu.roll(part, 16, 1) for part in wide] + [jnp.zeros((8, 128), F32)]
            for k in range(16):
                rows_ref[ROWS * d + 2 * k] = wide[k]
                rows_ref[ROWS * d + 2 * k + 1] = jnp.where((lane & 31) < 16, turned[k], turned[k + 1])
        rows_ref[DUMMY] = jnp.zeros((8, 128), F32)
        for buf in range(2):
            hot_u[buf, 8 * LEVELS_U :, :] = jnp.zeros((256 - 8 * LEVELS_U, 128 * TILES), BF16)
        copy.wait()
        trips = []
        for r in range(SUBREGIONS):
            begin, end = start_ref[0, r], start_ref[0, r + 1]
            number = lax.fori_loop(begin, end, lambda g, n: n + table_sm[g, 255], jnp.int32(0))
            last = jnp.maximum(end - 1, 0)

            @pl.when(number % 2 == 1)
            def _():
                table_sm[last, 255] = table_sm[last, 255] + 1

            trips.append((number + 1) // 2)

        zero = jnp.zeros((16, 128), BF16)

        stop = start_ref[0, SUBREGIONS]

        def index(state):
            g, b = state
            for half in range(2):
                group = jnp.minimum(g, GROUPS - 1)
                xi, yi, zi, wi = own_ref[0, group], own_ref[1, group], own_ref[2, group], own_ref[3, group]
                own_w[half] = jnp.concatenate([wi, wi], axis=0).astype(BF16)
                for t in range(TILES):
                    row = table_sm[g, TILES * b + t]
                    dx = xi - rows_ref[row, 0:1, :]
                    dy = yi - rows_ref[row, 1:2, :]
                    dz = zi - rows_ref[row, 2:3, :]
                    far_w[half, t] = jnp.broadcast_to(rows_ref[row, 3:4, :].astype(BF16), (16, 128))
                    dx2 = dx * dx
                    q = dx2 + dy * dy + dz * dz
                    s = jnp.floor(jnp.log2(q + 0.48) * LOG_SCALE + LOG_BASE)
                    near = jnp.floor(jnp.abs(dx) * lax.rsqrt(q) * float(MU_BINS) + 0.5)
                    mu = jnp.where(near * near * q > dx2 * float(MU_BINS * MU_BINS), near - 1.0, near)
                    c = s * float(MU_BINS) + jnp.minimum(mu, MU_BINS - 1.0)
                    u = jnp.floor(c * (1.0 / LEVELS_V) + 0.01)
                    v = c - u * float(LEVELS_V)
                    bin_u[half, t] = jnp.concatenate([u, u - 1.0], axis=0).astype(BF16)
                    bin_v[half, t] = jnp.concatenate([v, v - 1.0], axis=0).astype(BF16)
                b = b + 1
                over = b >= table_sm[g, 255]
                g = jnp.where(over, g + 1, g)
                g = jnp.where(g >= stop, GROUPS, g)
                b = jnp.where(over, 0, b)
            return g, b

        def fill(half):
            w_own = own_w[half]
            for t in range(TILES):
                u2, v2, w_far = bin_u[half, t], bin_v[half, t], far_w[half, t]
                lanes = slice(128 * t, 128 * t + 128)
                for k in range(LEVELS_U // 2):
                    hot_u[half, 16 * k : 16 * k + 16, lanes] = jnp.where(u2 == jnp.bfloat16(2 * k), w_far, zero)
                for k in range(V_ROWS // 16):
                    hot_v[half, 16 * k : 16 * k + 16, lanes] = jnp.where(v2 == jnp.bfloat16(2 * k), w_own, zero)

        def push(half):
            for mxu in range(2):
                pltpu.matmul_push_rhs(hot_u[half, :, 256 * mxu : 256 * mxu + 256], staging_register=half, mxu_index=mxu, transpose=True)

        def multiply(half, accs):
            for mxu in range(2):
                pltpu.matmul_acc_lhs(accs[mxu], hot_v[half, :, 256 * mxu : 256 * mxu + 256], load_staged_rhs=half)

        state = (jnp.where(stop > 0, 0, GROUPS).astype(jnp.int32), jnp.int32(0))
        state = index(state)
        for half in range(2):
            fill(half)
            push(half)
        state = index(state)
        sub = lax.broadcasted_iota(jnp.int32, (8, 256), 0)
        diagonal = sub == (lax.broadcasted_iota(jnp.int32, (8, 256), 1) & 7)

        def drain(r):
            accs = sets[r % 2]
            both = pltpu.matmul_pop(accs[0]) + pltpu.matmul_pop(accs[1])
            for v in range(V_ROWS // 8):
                out_ref[r, v : v + 1, :] = jnp.sum(jnp.where(diagonal, both[8 * v : 8 * v + 8], 0.0), axis=0, keepdims=True)
            out_ref[r, V_ROWS // 8 :, :] = jnp.zeros((32 - V_ROWS // 8, 256), F32)

        for r in range(SUBREGIONS):
            accs = sets[r % 2]

            def trip(_, state):
                for half in range(2):
                    multiply(half, accs)
                for half in range(2):
                    fill(half)
                    push(half)
                return index(state)

            state = lax.fori_loop(0, trips[r], trip, state)
            if r > 0:
                drain(r - 1)
        for half in range(2):
            multiply(half, sets[(SUBREGIONS - 1) % 2])
        drain(SUBREGIONS - 1)

    pl.run_scoped(
        body,
        pltpu.ACC(0)((V_ROWS, 256), F32),
        pltpu.ACC(1)((V_ROWS, 256), F32),
        pltpu.ACC(0)((V_ROWS, 256), F32),
        pltpu.ACC(1)((V_ROWS, 256), F32),
        pltpu.VMEM((2, 256, 128 * TILES), BF16),
        pltpu.VMEM((2, V_ROWS, 128 * TILES), BF16),
        pltpu.VMEM((2, TILES, 16, 128), BF16),
        pltpu.VMEM((2, TILES, 16, 128), BF16),
        pltpu.VMEM((2, TILES, 16, 128), BF16),
        pltpu.VMEM((2, 16, 128), BF16),
    )


def count_call(start, lists, got, own):
    vmem = pl.BlockSpec(memory_space=pltpu.VMEM)
    return pl.pallas_call(
        count_kernel,
        out_shape=jax.ShapeDtypeStruct((SUBREGIONS, 32, 256), F32),
        in_specs=[pl.BlockSpec(memory_space=pltpu.SMEM), vmem, vmem, vmem],
        out_specs=vmem,
        scratch_shapes=[
            pltpu.VMEM((DUMMY + 1, 8, 128), F32),
            pltpu.VMEM((32, 256), jnp.int32),
            pltpu.SMEM((32, 256), jnp.int32),
            pltpu.SemaphoreType.DMA,
        ],
        compiler_params=pltpu.CompilerParams(vmem_limit_bytes=8 << 20),
    )(start, lists, got, own)


MESH = pl.DeviceIdType.MESH


def halo_kernel(lists_ref, got_ref, send_sem, recv_sem):
    shell, sky = lax.axis_index("shell"), lax.axis_index("sky")
    shells, skies = lax.axis_size("shell"), lax.axis_size("sky")
    barrier = pltpu.get_barrier_semaphore()

    def present(da, db):
        a, b = shell + da, sky + db
        return (a >= 0) & (a < shells) & (b >= 0) & (b < skies)

    for da, db in DIRS:

        @pl.when(present(da, db))
        def _():
            pl.semaphore_signal(barrier, inc=1, device_id=(shell + da, sky + db), device_id_type=MESH)

    for d, (da, db) in enumerate(DIRS):

        @pl.when(jnp.logical_not(present(da, db)))
        def _():
            got_ref[d] = jnp.zeros((4, PART_DEV), F32)

    beside_shell = 1 + (shell > 0).astype(jnp.int32) + (shell < shells - 1).astype(jnp.int32)
    beside_sky = 1 + (sky > 0).astype(jnp.int32) + (sky < skies - 1).astype(jnp.int32)
    pl.semaphore_wait(barrier, beside_shell * beside_sky - 1)

    def copy(d):
        da, db = DIRS[d]
        return pltpu.make_async_remote_copy(
            src_ref=lists_ref.at[d],
            dst_ref=got_ref.at[7 - d],
            send_sem=send_sem.at[d],
            recv_sem=recv_sem.at[7 - d],
            device_id=(shell + da, sky + db),
            device_id_type=MESH,
        )

    for d, (da, db) in enumerate(DIRS):

        @pl.when(present(da, db))
        def _():
            copy(d).start()

    for d, (da, db) in enumerate(DIRS):

        @pl.when(present(da, db))
        def _():
            copy(d).wait_send()

        @pl.when(present(-da, -db))
        def _():
            copy(d).wait_recv()


def halo_call(lists):
    return pl.pallas_call(
        halo_kernel,
        out_shape=jax.ShapeDtypeStruct((8, 4, PART_DEV), F32),
        in_specs=[pl.BlockSpec(memory_space=pltpu.VMEM)],
        out_specs=pl.BlockSpec(memory_space=pltpu.VMEM),
        scratch_shapes=[pltpu.SemaphoreType.DMA((8,)), pltpu.SemaphoreType.DMA((8,))],
        compiler_params=pltpu.CompilerParams(collective_id=0, has_side_effects=True, vmem_limit_bytes=4 << 20),
    )(lists)


def total_kernel(skies, counts_ref, own_ref, total_ref, sent_ref, land_ref, send_sem, recv_sem):
    shell, sky = lax.axis_index("shell"), lax.axis_index("sky")
    barrier = pltpu.get_barrier_semaphore()
    for k in range(1, skies):
        pl.semaphore_signal(barrier, inc=1, device_id=(shell, lax.rem(sky + k, skies)), device_id_type=MESH)
    lane_in = lax.broadcasted_iota(jnp.int32, (256, 128), 0)
    lane_out = lax.broadcasted_iota(jnp.int32, (256, 128), 1)
    packed = jnp.zeros((8 * SUBREGIONS, 128), F32)
    for k in range(4):
        rows = jnp.concatenate([counts_ref[r, 8 * k : 8 * k + 8, :] for r in range(SUBREGIONS)], axis=0)
        pick = jnp.where((lane_in >> 3) + 32 * k == lane_out, 1.0, 0.0)
        packed = packed + jnp.dot(rows, pick, precision=lax.Precision.HIGHEST, preferred_element_type=F32)
    own_ref[...] = packed
    mine = packed[0:8]
    for r in range(1, SUBREGIONS):
        mine = mine + packed[8 * r : 8 * r + 8]
    sent_ref[...] = mine
    pl.semaphore_wait(barrier, skies - 1)

    def copy(k):
        return pltpu.make_async_remote_copy(
            src_ref=sent_ref,
            dst_ref=land_ref.at[k - 1],
            send_sem=send_sem.at[k - 1],
            recv_sem=recv_sem.at[k - 1],
            device_id=(shell, lax.rem(sky + k, skies)),
            device_id_type=MESH,
        )

    for k in range(1, skies):
        copy(k).start()
    total = mine
    for k in range(1, skies):
        copy(k).wait_recv()
        total = total + land_ref[k - 1]
    total_ref[...] = total
    for k in range(1, skies):
        copy(k).wait_send()


def total_call(counts):
    skies = lax.axis_size("sky")
    vmem = pl.BlockSpec(memory_space=pltpu.VMEM)
    return pl.pallas_call(
        functools.partial(total_kernel, skies),
        out_shape=(jax.ShapeDtypeStruct((8 * SUBREGIONS, 128), F32), jax.ShapeDtypeStruct((8, 128), F32)),
        in_specs=[vmem],
        out_specs=(vmem, vmem),
        scratch_shapes=[
            pltpu.VMEM((8, 128), F32),
            pltpu.VMEM((skies - 1, 8, 128), F32),
            pltpu.SemaphoreType.DMA((skies - 1,)),
            pltpu.SemaphoreType.DMA((skies - 1,)),
        ],
        compiler_params=pltpu.CompilerParams(collective_id=1, has_side_effects=True, vmem_limit_bytes=4 << 20),
    )(counts)


def edge_values():
    return [int(4.0 * 10.0 ** (4.0 * level / S_BINS) + 0.5) for level in range(S_BINS + 1)]


def bin_scale(patches):
    edges = edge_values()
    factor = SIDE_CELLS * SIDE_CELLS * SPAN_CELLS / (patches * PART_DEV * PART_DEV)
    values = []
    for level in range(S_BINS):
        volume = 4.0 * math.pi / 3.0 * (edges[level + 1] ** 1.5 - edges[level] ** 1.5) / MU_BINS
        values = values + [factor / volume] * MU_BINS
    return jnp.asarray(values, dtype=F32)


def unpacked(x):
    x = x.reshape(-1, 8, 4, 32).transpose(0, 3, 2, 1).reshape(-1, 32, 32)
    return x[:, :LEVELS_U, :LEVELS_V].reshape(-1, S_BINS * MU_BINS)


def local(coords, weights, live):
    lists, own, start = sort_call(coords, weights, live)
    counts = count_call(start, lists, halo_call(lists), own)
    packed, total = total_call(counts)
    leave = total[None] - packed.reshape(SUBREGIONS, 8, 128)
    return (unpacked(leave) * bin_scale(lax.axis_size("sky"))[None, :])[None]


def solution(mesh):
    in_specs = (P(None, "shell", "sky", None), P("shell", "sky", None), P("shell", "sky"))
    out_specs = P("shell", "sky", None)
    return jax.shard_map(local, mesh=mesh, in_specs=in_specs, out_specs=out_specs, check_vma=False)
```

```python
import functools, math
import jax, jax.numpy as jnp
from jax import lax
from jax.experimental import pallas as pl
from jax.experimental.pallas import tpu as pltpu
from jax.sharding import PartitionSpec as P

PART_DEV = 512
SIDE_CELLS = 256
SPAN_CELLS = 1024
SUBREGIONS = 8
S_BINS = 30
MU_BINS = 20
REACH = 199
GROUPS = 24
STEP = 16
ROWS = PART_DEV // STEP
DUMMY = 9 * ROWS
TILES = 4
DIRS = tuple((da, db) for da in (-1, 0, 1) for db in (-1, 0, 1) if (da, db) != (0, 0))
MESH = pl.DeviceIdType.MESH
F32 = jnp.float32
BF16 = jnp.bfloat16


def send_kernel(coords_hbm, weight_hbm, live_hbm, table_ref, rows_ref, own_ref, coords_ref, weight_ref, live_ref, lists_ref, got_ref, load_sem, send_sem, recv_sem):
    shell, sky = lax.axis_index("shell"), lax.axis_index("sky")
    shells, skies = lax.axis_size("shell"), lax.axis_size("sky")
    barrier = pltpu.get_barrier_semaphore()
    loads = [
        pltpu.make_async_copy(src, dst, load_sem.at[k])
        for k, (src, dst) in enumerate(((coords_hbm, coords_ref), (weight_hbm, weight_ref), (live_hbm, live_ref)))
    ]
    for load in loads:
        load.start()

    def present(da, db):
        a, b = shell + da, sky + db
        return (a >= 0) & (a < shells) & (b >= 0) & (b < skies)

    for da, db in DIRS:

        @pl.when(present(da, db))
        def _():
            pl.semaphore_signal(barrier, inc=1, device_id=(shell + da, sky + db), device_id_type=MESH)

    for d, (da, db) in enumerate(DIRS):

        @pl.when(jnp.logical_not(present(da, db)))
        def _():
            got_ref[d] = jnp.zeros((4, PART_DEV), F32)

    def copy(d):
        da, db = DIRS[d]
        return pltpu.make_async_remote_copy(
            src_ref=lists_ref.at[d],
            dst_ref=got_ref.at[7 - d],
            send_sem=send_sem.at[d],
            recv_sem=recv_sem.at[7 - d],
            device_id=(shell + da, sky + db),
            device_id_type=MESH,
        )

    def body(acc0, acc1, acc2, acc3, tall0, tall1):
        for acc in (acc0, acc1, acc2, acc3, tall0, tall1):
            pltpu.matmul_pop(acc)
        for load in loads:
            load.wait()
        n = PART_DEV
        x = (coords_ref[0, 0] & (SIDE_CELLS - 1)).astype(F32)
        y = (coords_ref[1, 0] & (SIDE_CELLS - 1)).astype(F32)
        zi = coords_ref[2, 0]
        region = zi >> 7
        z_high = region.astype(F32)
        z_low = (zi & 127).astype(F32)
        slot = lax.broadcasted_iota(jnp.int32, (1, n), 1)
        alive = slot < live_ref[...]
        w = jnp.where(alive, weight_ref[0].astype(F32), 0.0)
        key = (jnp.where(alive, zi * n, SPAN_CELLS * n) + slot).astype(F32)
        key_column = jnp.transpose(jnp.broadcast_to(key, (128, n)))[:, 0:1]
        before = jnp.where(key_column < key, 1.0, 0.0).astype(BF16)
        valid = []
        for da, db in DIRS:
            ok = alive
            if da > 0:
                ok = ok & (x >= SIDE_CELLS - REACH)
            if da < 0:
                ok = ok & (x <= REACH - 1)
            if db > 0:
                ok = ok & (y >= SIDE_CELLS - REACH)
            if db < 0:
                ok = ok & (y <= REACH - 1)
            valid.append(ok)
        valid.append(alive)
        ones = [jnp.where(ok, 1.0, 0.0) for ok in valid]
        flags = jnp.concatenate(ones + [jnp.zeros((7, n), F32)], axis=0).astype(BF16)
        for half in range(2):
            rows = slice(256 * half, 256 * half + 256)
            pltpu.matmul_push_rhs(before[rows, 0:256], staging_register=0, mxu_index=0)
            pltpu.matmul_acc_lhs(acc0, flags[:, rows], load_staged_rhs=0)
            pltpu.matmul_push_rhs(before[rows, 256:512], staging_register=0, mxu_index=1)
            pltpu.matmul_acc_lhs(acc1, flags[:, rows], load_staged_rhs=0)
        rank = jnp.concatenate([pltpu.matmul_pop(acc0), pltpu.matmul_pop(acc1)], axis=1)
        attrs = jnp.concatenate([x, y, z_high, z_low, w, jnp.zeros((11, n), F32)], axis=0).astype(BF16)
        place = lax.broadcasted_iota(jnp.int32, (n, 1), 0).astype(F32)
        accs = ((acc0, acc1), (acc2, acc3))
        for d in range(9):
            target = jnp.where(valid[d], rank[d : d + 1, :], -1.0)
            hot = jnp.where(place == target, 1.0, 0.0).astype(BF16)
            pair = accs[d % 2]
            for half in range(2):
                cols = slice(256 * half, 256 * half + 256)
                for mxu in range(2):
                    pltpu.matmul_push_rhs(hot[256 * mxu : 256 * mxu + 256, cols], staging_register=0, mxu_index=mxu, transpose=True)
                    pltpu.matmul_acc_lhs(pair[mxu], attrs[:, cols], load_staged_rhs=0)
            da, db = DIRS[d] if d < 8 else (0, 0)
            for mxu in range(2):
                got = pltpu.matmul_pop(pair[mxu])
                lanes = slice(256 * mxu, 256 * mxu + 256)
                lists_ref[d, 0:1, lanes] = got[0:1] - float(SIDE_CELLS * da)
                lists_ref[d, 1:2, lanes] = got[1:2] - float(SIDE_CELLS * db)
                lists_ref[d, 2:3, lanes] = got[2:3] * 128.0 + got[3:4]
                lists_ref[d, 3:4, lanes] = got[4:5]

        beside_shell = 1 + (shell > 0).astype(jnp.int32) + (shell < shells - 1).astype(jnp.int32)
        beside_sky = 1 + (sky > 0).astype(jnp.int32) + (sky < skies - 1).astype(jnp.int32)
        pl.semaphore_wait(barrier, beside_shell * beside_sky - 1)
        for d, (da, db) in enumerate(DIRS):

            @pl.when(present(da, db))
            def _():
                copy(d).start()

        shift = jnp.zeros((1, n), F32)
        first = jnp.zeros((1, 1), F32)
        group = jnp.zeros((1, 1), F32)
        starts = []
        for r in range(SUBREGIONS):
            here = alive & (region == r)
            starts.append(group)
            shift = jnp.where(here, 32.0 * group - first, shift)
            count = jnp.sum(jnp.where(here, 1.0, 0.0), axis=1, keepdims=True)
            first = first + count
            group = group + jnp.floor((count + 31.0) * (1.0 / 32.0))
        starts = starts + [group]
        lane_row = lax.broadcasted_iota(jnp.int32, (1, 128), 1)
        begin, end = jnp.zeros((1, 128), F32), jnp.zeros((1, 128), F32)
        for r in range(SUBREGIONS):
            begin = jnp.where(lane_row == r, starts[r], begin)
            end = jnp.where(lane_row == r, starts[r + 1], end)
        target = jnp.where(alive, rank[8:9, :] + shift, -1.0)
        wide = lax.broadcasted_iota(jnp.int32, (GROUPS * 32, 1), 0).astype(F32)
        hot = jnp.where(wide == target, 1.0, 0.0).astype(BF16)
        rhs = jnp.concatenate([attrs, jnp.zeros((240, n), BF16)], axis=0)
        half_rows = GROUPS * 16
        for half in range(2):
            cols = slice(256 * half, 256 * half + 256)
            for mxu, acc in ((0, tall0), (1, tall1)):
                pltpu.matmul_push_rhs(rhs[:, cols], staging_register=0, mxu_index=mxu, transpose=True)
                pltpu.matmul_acc_lhs(acc, hot[half_rows * mxu : half_rows * mxu + half_rows, cols], load_staged_rhs=0)
        quarter = lax.broadcasted_iota(jnp.int32, (8, 128), 1) // 32
        for mxu, acc in ((0, tall0), (1, tall1)):
            got = pltpu.matmul_pop(acc)[:, 0:128]
            for g in range(GROUPS // 2):
                parts = []
                for q in range(4):
                    block = got[32 * g + 8 * q : 32 * g + 8 * q + 8]
                    deep = block[:, 2:3] * 128.0 + block[:, 3:4]
                    parts.append([jnp.broadcast_to(v, (8, 128)) for v in (block[:, 0:1], block[:, 1:2], deep, block[:, 4:5])])
                for k in range(4):
                    value = parts[0][k]
                    for q in range(1, 4):
                        value = jnp.where(quarter == q, parts[q][k], value)
                    own_ref[k, mxu * (GROUPS // 2) + g] = value

        zs, ws = own_ref[2], own_ref[3]
        z_min = jnp.min(jnp.min(jnp.where(ws > 0.0, zs, 1e6), axis=1), axis=1, keepdims=True)
        z_max = jnp.max(jnp.max(jnp.where(ws > 0.0, zs, -1e6), axis=1), axis=1, keepdims=True)
        lane = lax.broadcasted_iota(jnp.int32, (GROUPS, 128), 1)
        chunk = lane.astype(F32) * 2.0
        even = jnp.full((GROUPS, 128), float(DUMMY), F32)
        odd = even
        total = jnp.zeros((GROUPS, 1), F32)
        lane8 = lax.broadcasted_iota(jnp.int32, (8, 128), 1)
        rows_ref[DUMMY] = jnp.zeros((8, 128), F32)
        for d in (8, 3, 4, 1, 6, 0, 2, 5, 7):
            if d < 8:

                @pl.when(present(*DIRS[d]))
                def _():
                    copy(7 - d).wait_recv()

            src = lists_ref.at[8] if d == 8 else got_ref.at[d]
            z_row = jnp.where(src[3:4, :] > 0.0, src[2:3, :], 2e6)
            low = jnp.sum(jnp.where(z_row < z_min - float(REACH), 1.0, 0.0), axis=1, keepdims=True)
            high = jnp.sum(jnp.where(z_row <= z_max + float(REACH), 1.0, 0.0), axis=1, keepdims=True)
            first = jnp.floor(low * (1.0 / STEP))
            count = jnp.where(high > low, jnp.floor((high - STEP * first + 31.0) * (1.0 / 32.0)), 0.0)
            at = chunk - total
            even = jnp.where((at >= 0.0) & (at < count), at * 2.0 + (first + float(ROWS * d)), even)
            at = at + 1.0
            odd = jnp.where((at >= 0.0) & (at < count), at * 2.0 + (first + float(ROWS * d)), odd)
            total = total + count
            parts = []
            for t in range(4):
                block = src[:, 128 * t : 128 * t + 128]
                block = jnp.concatenate([block, block], axis=0)
                for k in range(4):
                    part = block if k == 0 else pltpu.roll(block, 128 - 32 * k, 1)
                    part = jnp.where(lane8 < 32, part, pltpu.roll(part, 32, 1))
                    part = jnp.where(lane8 < 64, part, pltpu.roll(part, 64, 1))
                    parts.append(part)
            turned = [pltpu.roll(part, 16, 1) for part in parts] + [jnp.zeros((8, 128), F32)]
            for k in range(16):
                rows_ref[ROWS * d + 2 * k] = parts[k]
                rows_ref[ROWS * d + 2 * k + 1] = jnp.where((lane8 & 31) < 16, turned[k], turned[k + 1])
        batches = jnp.floor((total + (TILES - 1.0)) * (1.0 / TILES))
        name = lax.broadcasted_iota(jnp.int32, (GROUPS, 128), 0).astype(F32)
        number = jnp.sum(jnp.where((name >= begin) & (name < end), batches, 0.0), axis=0, keepdims=True)
        extra = number - 2.0 * jnp.floor(number * 0.5)
        batches = batches + jnp.sum(jnp.where(name == end - 1.0, extra, 0.0), axis=1, keepdims=True)
        table = jnp.where(lane == 127, batches, even + 512.0 * odd)
        table_ref[0:GROUPS, :] = table.astype(jnp.int32)
        idle = jnp.where(lane_row == 127, float(1 << 20), float(DUMMY * 513))
        trips = jnp.where(lane_row == SUBREGIONS, starts[SUBREGIONS], (number + extra) * 0.5)
        tail = jnp.concatenate([idle, trips, jnp.zeros((6, 128), F32)], axis=0)
        table_ref[GROUPS : GROUPS + 8, :] = tail.astype(jnp.int32)
        for d, (da, db) in enumerate(DIRS):

            @pl.when(present(da, db))
            def _():
                copy(d).wait_send()

    pl.run_scoped(
        body,
        pltpu.ACC(0)((16, 256), F32),
        pltpu.ACC(1)((16, 256), F32),
        pltpu.ACC(0)((16, 256), F32),
        pltpu.ACC(1)((16, 256), F32),
        pltpu.ACC(0)((GROUPS * 16, 256), F32),
        pltpu.ACC(1)((GROUPS * 16, 256), F32),
    )


def send_call(coords, weights, live):
    far = pl.BlockSpec(memory_space=pltpu.HBM)
    return pl.pallas_call(
        send_kernel,
        out_shape=(
            jax.ShapeDtypeStruct((GROUPS + 8, 128), jnp.int32),
            jax.ShapeDtypeStruct((DUMMY + 1, 8, 128), F32),
            jax.ShapeDtypeStruct((4, GROUPS, 8, 128), F32),
        ),
        in_specs=[far] * 3,
        out_specs=[pl.BlockSpec(memory_space=pltpu.VMEM)] * 3,
        scratch_shapes=[
            pltpu.VMEM((3, 1, 1, PART_DEV), jnp.int32),
            pltpu.VMEM((1, 1, PART_DEV), BF16),
            pltpu.VMEM((1, 1), jnp.int32),
            pltpu.VMEM((9, 4, PART_DEV), F32),
            pltpu.VMEM((8, 4, PART_DEV), F32),
            pltpu.SemaphoreType.DMA((3,)),
            pltpu.SemaphoreType.DMA((8,)),
            pltpu.SemaphoreType.DMA((8,)),
        ],
        compiler_params=pltpu.CompilerParams(collective_id=0, has_side_effects=True, vmem_limit_bytes=12 << 20),
    )(coords, weights, live)


LOG_SCALE = (S_BINS / 4.0) / math.log2(10.0)
LOG_BASE = -4.515457845
LEVELS_U = 24
LEVELS_V = 25
V_ROWS = 208


def count_kernel(table_ref, rows_ref, own_ref, out_ref, table_sm, sem):
    def body(a0, a1, b0, b1, hot_u, hot_v, bin_u, bin_v, far_w, own_w):
        sets = ((a0, a1), (b0, b1))
        copy = pltpu.make_async_copy(table_ref, table_sm, sem)
        copy.start()
        for acc in (a0, a1, b0, b1):
            pltpu.matmul_pop(acc)
        for half in range(2):
            hot_u[half, 8 * LEVELS_U :, :] = jnp.zeros((256 - 8 * LEVELS_U, 128 * TILES), BF16)
        copy.wait()
        trips = [table_sm[GROUPS + 1, r] for r in range(SUBREGIONS)]
        stop = table_sm[GROUPS + 1, SUBREGIONS]
        zero = jnp.zeros((16, 128), BF16)

        def index(state):
            g, b = state
            for half in range(2):
                group = jnp.minimum(g, GROUPS - 1)
                xi, yi, zi, wi = own_ref[0, group], own_ref[1, group], own_ref[2, group], own_ref[3, group]
                own_w[half] = jnp.concatenate([wi, wi], axis=0).astype(BF16)
                for t in range(TILES):
                    pair = table_sm[g, TILES // 2 * b + t // 2]
                    row = pair & 511 if t % 2 == 0 else pair >> 9
                    dx = xi - rows_ref[row, 0:1, :]
                    dy = yi - rows_ref[row, 1:2, :]
                    dz = zi - rows_ref[row, 2:3, :]
                    far_w[half, t] = jnp.broadcast_to(rows_ref[row, 3:4, :].astype(BF16), (16, 128))
                    dx2 = dx * dx
                    q = dx2 + dy * dy + dz * dz
                    s = jnp.floor(jnp.log2(q + 0.48) * LOG_SCALE + LOG_BASE)
                    near = jnp.floor(jnp.abs(dx) * lax.rsqrt(q) * float(MU_BINS) + 0.5)
                    mu = jnp.where(near * near * q > dx2 * float(MU_BINS * MU_BINS), near - 1.0, near)
                    c = s * float(MU_BINS) + jnp.minimum(mu, MU_BINS - 1.0)
                    u = jnp.floor(c * (1.0 / LEVELS_V) + 0.01)
                    v = c - u * float(LEVELS_V)
                    bin_u[half, t] = jnp.concatenate([u, u - 1.0], axis=0).astype(BF16)
                    bin_v[half, t] = jnp.concatenate([v, v - 1.0], axis=0).astype(BF16)
                b = b + 1
                over = b >= table_sm[g, 127]
                g = jnp.where(over, g + 1, g)
                g = jnp.where(g >= stop, GROUPS, g)
                b = jnp.where(over, 0, b)
            return g, b

        def fill(half):
            w_own = own_w[half]
            for t in range(TILES):
                u2, v2, w_far = bin_u[half, t], bin_v[half, t], far_w[half, t]
                lanes = slice(128 * t, 128 * t + 128)
                for k in range(LEVELS_U // 2):
                    hot_u[half, 16 * k : 16 * k + 16, lanes] = jnp.where(u2 == jnp.bfloat16(2 * k), w_far, zero)
                for k in range(V_ROWS // 16):
                    hot_v[half, 16 * k : 16 * k + 16, lanes] = jnp.where(v2 == jnp.bfloat16(2 * k), w_own, zero)

        def push(half):
            for mxu in range(2):
                pltpu.matmul_push_rhs(hot_u[half, :, 256 * mxu : 256 * mxu + 256], staging_register=half, mxu_index=mxu, transpose=True)

        def multiply(half, accs):
            for mxu in range(2):
                pltpu.matmul_acc_lhs(accs[mxu], hot_v[half, :, 256 * mxu : 256 * mxu + 256], load_staged_rhs=half)

        state = (jnp.where(stop > 0, 0, GROUPS).astype(jnp.int32), jnp.int32(0))
        state = index(state)
        for half in range(2):
            fill(half)
            push(half)
        state = index(state)
        sub = lax.broadcasted_iota(jnp.int32, (8, 256), 0)
        diagonal = sub == (lax.broadcasted_iota(jnp.int32, (8, 256), 1) & 7)

        def drain(r):
            accs = sets[r % 2]
            both = pltpu.matmul_pop(accs[0]) + pltpu.matmul_pop(accs[1])
            for v in range(V_ROWS // 8):
                out_ref[r, v : v + 1, :] = jnp.sum(jnp.where(diagonal, both[8 * v : 8 * v + 8], 0.0), axis=0, keepdims=True)
            out_ref[r, V_ROWS // 8 :, :] = jnp.zeros((32 - V_ROWS // 8, 256), F32)

        for r in range(SUBREGIONS):
            accs = sets[r % 2]

            def trip(_, state):
                for half in range(2):
                    multiply(half, accs)
                for half in range(2):
                    fill(half)
                    push(half)
                return index(state)

            state = lax.fori_loop(0, trips[r], trip, state)
            if r > 0:
                drain(r - 1)
        for half in range(2):
            multiply(half, sets[(SUBREGIONS - 1) % 2])
        drain(SUBREGIONS - 1)

    pl.run_scoped(
        body,
        pltpu.ACC(0)((V_ROWS, 256), F32),
        pltpu.ACC(1)((V_ROWS, 256), F32),
        pltpu.ACC(0)((V_ROWS, 256), F32),
        pltpu.ACC(1)((V_ROWS, 256), F32),
        pltpu.VMEM((2, 256, 128 * TILES), BF16),
        pltpu.VMEM((2, V_ROWS, 128 * TILES), BF16),
        pltpu.VMEM((2, TILES, 16, 128), BF16),
        pltpu.VMEM((2, TILES, 16, 128), BF16),
        pltpu.VMEM((2, TILES, 16, 128), BF16),
        pltpu.VMEM((2, 16, 128), BF16),
    )


def count_call(table, rows, own):
    vmem = pl.BlockSpec(memory_space=pltpu.VMEM)
    return pl.pallas_call(
        count_kernel,
        out_shape=jax.ShapeDtypeStruct((SUBREGIONS, 32, 256), F32),
        in_specs=[vmem, vmem, vmem],
        out_specs=vmem,
        scratch_shapes=[pltpu.SMEM((GROUPS + 8, 128), jnp.int32), pltpu.SemaphoreType.DMA],
        compiler_params=pltpu.CompilerParams(vmem_limit_bytes=6 << 20),
    )(table, rows, own)


def total_kernel(skies, counts_ref, own_ref, total_ref, sent_ref, land_ref, send_sem, recv_sem):
    shell, sky = lax.axis_index("shell"), lax.axis_index("sky")
    barrier = pltpu.get_barrier_semaphore()
    for k in range(1, skies):
        pl.semaphore_signal(barrier, inc=1, device_id=(shell, lax.rem(sky + k, skies)), device_id_type=MESH)
    lane_in = lax.broadcasted_iota(jnp.int32, (256, 128), 0)
    lane_out = lax.broadcasted_iota(jnp.int32, (256, 128), 1)
    every = counts_ref[0]
    for r in range(1, SUBREGIONS):
        every = every + counts_ref[r]
    picks = [jnp.where((lane_in >> 3) + 32 * k == lane_out, 1.0, 0.0) for k in range(4)]

    def pack(rows):
        packed = jnp.dot(rows[0], picks[0], precision=lax.Precision.HIGHEST, preferred_element_type=F32)
        for k in range(1, 4):
            packed = packed + jnp.dot(rows[k], picks[k], precision=lax.Precision.HIGHEST, preferred_element_type=F32)
        return packed

    mine = pack([every[8 * k : 8 * k + 8] for k in range(4)])
    sent_ref[...] = mine
    pl.semaphore_wait(barrier, skies - 1)

    def copy(k):
        return pltpu.make_async_remote_copy(
            src_ref=sent_ref,
            dst_ref=land_ref.at[k - 1],
            send_sem=send_sem.at[k - 1],
            recv_sem=recv_sem.at[k - 1],
            device_id=(shell, lax.rem(sky + k, skies)),
            device_id_type=MESH,
        )

    for k in range(1, skies):
        copy(k).start()
    own_ref[...] = pack([jnp.concatenate([counts_ref[r, 8 * k : 8 * k + 8, :] for r in range(SUBREGIONS)], axis=0) for k in range(4)])
    total = mine
    for k in range(1, skies):
        copy(k).wait_recv()
        total = total + land_ref[k - 1]
    total_ref[...] = total
    for k in range(1, skies):
        copy(k).wait_send()


def total_call(counts):
    skies = lax.axis_size("sky")
    vmem = pl.BlockSpec(memory_space=pltpu.VMEM)
    return pl.pallas_call(
        functools.partial(total_kernel, skies),
        out_shape=(jax.ShapeDtypeStruct((8 * SUBREGIONS, 128), F32), jax.ShapeDtypeStruct((8, 128), F32)),
        in_specs=[vmem],
        out_specs=(vmem, vmem),
        scratch_shapes=[
            pltpu.VMEM((8, 128), F32),
            pltpu.VMEM((skies - 1, 8, 128), F32),
            pltpu.SemaphoreType.DMA((skies - 1,)),
            pltpu.SemaphoreType.DMA((skies - 1,)),
        ],
        compiler_params=pltpu.CompilerParams(collective_id=1, has_side_effects=True, vmem_limit_bytes=4 << 20),
    )(counts)


def edge_values():
    return [int(4.0 * 10.0 ** (4.0 * level / S_BINS) + 0.5) for level in range(S_BINS + 1)]


def bin_scale(patches):
    edges = edge_values()
    factor = SIDE_CELLS * SIDE_CELLS * SPAN_CELLS / (patches * PART_DEV * PART_DEV)
    values = []
    for level in range(S_BINS):
        volume = 4.0 * math.pi / 3.0 * (edges[level + 1] ** 1.5 - edges[level] ** 1.5) / MU_BINS
        values = values + [factor / volume] * MU_BINS
    return jnp.asarray(values, dtype=F32)


def unpacked(x):
    x = x.reshape(-1, 8, 4, 32).transpose(0, 3, 2, 1).reshape(-1, 32, 32)
    return x[:, :LEVELS_U, :LEVELS_V].reshape(-1, S_BINS * MU_BINS)


def local(coords, weights, live):
    counts = count_call(*send_call(coords, weights, live))
    packed, total = total_call(counts)
    leave = total[None] - packed.reshape(SUBREGIONS, 8, 128)
    return (unpacked(leave) * bin_scale(lax.axis_size("sky"))[None, :])[None]


def solution(mesh):
    in_specs = (P(None, "shell", "sky", None), P("shell", "sky", None), P("shell", "sky"))
    out_specs = P("shell", "sky", None)
    return jax.shard_map(local, mesh=mesh, in_specs=in_specs, out_specs=out_specs, check_vma=False)
```

```python
import functools, math
import jax, jax.numpy as jnp
from jax import lax
from jax.experimental import pallas as pl
from jax.experimental.pallas import tpu as pltpu
from jax.sharding import PartitionSpec as P

PART_DEV = 512
SIDE_CELLS = 256
SPAN_CELLS = 1024
SUBREGIONS = 8
S_BINS = 30
MU_BINS = 20
REACH = 199
GROUPS = 24
STEP = 16
ROWS = PART_DEV // STEP
DUMMY = 9 * ROWS
TILES = 4
DIRS = tuple((da, db) for da in (-1, 0, 1) for db in (-1, 0, 1) if (da, db) != (0, 0))
MESH = pl.DeviceIdType.MESH
F32 = jnp.float32
BF16 = jnp.bfloat16


def send_kernel(coords_hbm, weight_hbm, live_hbm, table_ref, rows_ref, own_ref, coords_ref, weight_ref, live_ref, lists_ref, got_ref, load_sem, send_sem, recv_sem):
    shell, sky = lax.axis_index("shell"), lax.axis_index("sky")
    shells, skies = lax.axis_size("shell"), lax.axis_size("sky")
    barrier = pltpu.get_barrier_semaphore()
    loads = [
        pltpu.make_async_copy(src, dst, load_sem.at[k])
        for k, (src, dst) in enumerate(((coords_hbm, coords_ref), (weight_hbm, weight_ref), (live_hbm, live_ref)))
    ]
    for load in loads:
        load.start()

    def present(da, db):
        a, b = shell + da, sky + db
        return (a >= 0) & (a < shells) & (b >= 0) & (b < skies)

    for da, db in DIRS:

        @pl.when(present(da, db))
        def _():
            pl.semaphore_signal(barrier, inc=1, device_id=(shell + da, sky + db), device_id_type=MESH)

    for d, (da, db) in enumerate(DIRS):

        @pl.when(jnp.logical_not(present(da, db)))
        def _():
            got_ref[d] = jnp.zeros((4, PART_DEV), F32)

    def copy(d):
        da, db = DIRS[d]
        return pltpu.make_async_remote_copy(
            src_ref=lists_ref.at[d],
            dst_ref=got_ref.at[7 - d],
            send_sem=send_sem.at[d],
            recv_sem=recv_sem.at[7 - d],
            device_id=(shell + da, sky + db),
            device_id_type=MESH,
        )

    def body(acc0, acc1, acc2, acc3, tall0, tall1):
        for acc in (acc0, acc1, acc2, acc3, tall0, tall1):
            pltpu.matmul_pop(acc)
        for load in loads:
            load.wait()
        n = PART_DEV
        x = (coords_ref[0, 0] & (SIDE_CELLS - 1)).astype(F32)
        y = (coords_ref[1, 0] & (SIDE_CELLS - 1)).astype(F32)
        zi = coords_ref[2, 0]
        region = zi >> 7
        z_high = region.astype(F32)
        z_low = (zi & 127).astype(F32)
        slot = lax.broadcasted_iota(jnp.int32, (1, n), 1)
        alive = slot < live_ref[...]
        w = jnp.where(alive, weight_ref[0].astype(F32), 0.0)
        key = (jnp.where(alive, zi * n, SPAN_CELLS * n) + slot).astype(F32)
        key_column = jnp.transpose(jnp.broadcast_to(key, (128, n)))[:, 0:1]
        before = jnp.where(key_column < key, 1.0, 0.0).astype(BF16)
        valid = []
        for da, db in DIRS:
            ok = alive
            if da > 0:
                ok = ok & (x >= SIDE_CELLS - REACH)
            if da < 0:
                ok = ok & (x <= REACH - 1)
            if db > 0:
                ok = ok & (y >= SIDE_CELLS - REACH)
            if db < 0:
                ok = ok & (y <= REACH - 1)
            valid.append(ok)
        valid.append(alive)
        ones = [jnp.where(ok, 1.0, 0.0) for ok in valid]
        flags = jnp.concatenate(ones + [jnp.zeros((7, n), F32)], axis=0).astype(BF16)
        for half in range(2):
            rows = slice(256 * half, 256 * half + 256)
            pltpu.matmul_push_rhs(before[rows, 0:256], staging_register=0, mxu_index=0)
            pltpu.matmul_acc_lhs(acc0, flags[:, rows], load_staged_rhs=0)
            pltpu.matmul_push_rhs(before[rows, 256:512], staging_register=0, mxu_index=1)
            pltpu.matmul_acc_lhs(acc1, flags[:, rows], load_staged_rhs=0)
        rank = jnp.concatenate([pltpu.matmul_pop(acc0), pltpu.matmul_pop(acc1)], axis=1)
        attrs = jnp.concatenate([x, y, z_high, z_low, w, jnp.zeros((11, n), F32)], axis=0).astype(BF16)
        place = lax.broadcasted_iota(jnp.int32, (n, 1), 0).astype(F32)
        accs = ((acc0, acc1), (acc2, acc3))
        for d in range(9):
            target = jnp.where(valid[d], rank[d : d + 1, :], -1.0)
            hot = jnp.where(place == target, 1.0, 0.0).astype(BF16)
            pair = accs[d % 2]
            for half in range(2):
                cols = slice(256 * half, 256 * half + 256)
                for mxu in range(2):
                    pltpu.matmul_push_rhs(hot[256 * mxu : 256 * mxu + 256, cols], staging_register=0, mxu_index=mxu, transpose=True)
                    pltpu.matmul_acc_lhs(pair[mxu], attrs[:, cols], load_staged_rhs=0)
            da, db = DIRS[d] if d < 8 else (0, 0)
            for mxu in range(2):
                got = pltpu.matmul_pop(pair[mxu])
                lanes = slice(256 * mxu, 256 * mxu + 256)
                lists_ref[d, 0:1, lanes] = got[0:1] - float(SIDE_CELLS * da)
                lists_ref[d, 1:2, lanes] = got[1:2] - float(SIDE_CELLS * db)
                lists_ref[d, 2:3, lanes] = got[2:3] * 128.0 + got[3:4]
                lists_ref[d, 3:4, lanes] = got[4:5]

        beside_shell = 1 + (shell > 0).astype(jnp.int32) + (shell < shells - 1).astype(jnp.int32)
        beside_sky = 1 + (sky > 0).astype(jnp.int32) + (sky < skies - 1).astype(jnp.int32)
        pl.semaphore_wait(barrier, beside_shell * beside_sky - 1)
        for d, (da, db) in enumerate(DIRS):

            @pl.when(present(da, db))
            def _():
                copy(d).start()

        shift = jnp.zeros((1, n), F32)
        first = jnp.zeros((1, 1), F32)
        group = jnp.zeros((1, 1), F32)
        starts = []
        for r in range(SUBREGIONS):
            here = alive & (region == r)
            starts.append(group)
            shift = jnp.where(here, 32.0 * group - first, shift)
            count = jnp.sum(jnp.where(here, 1.0, 0.0), axis=1, keepdims=True)
            first = first + count
            group = group + jnp.floor((count + 31.0) * (1.0 / 32.0))
        starts = starts + [group]
        lane_row = lax.broadcasted_iota(jnp.int32, (1, 128), 1)
        begin, end = jnp.zeros((1, 128), F32), jnp.zeros((1, 128), F32)
        for r in range(SUBREGIONS):
            begin = jnp.where(lane_row == r, starts[r], begin)
            end = jnp.where(lane_row == r, starts[r + 1], end)
        target = jnp.where(alive, rank[8:9, :] + shift, -1.0)
        wide = lax.broadcasted_iota(jnp.int32, (GROUPS * 32, 1), 0).astype(F32)
        hot = jnp.where(wide == target, 1.0, 0.0).astype(BF16)
        rhs = jnp.concatenate([attrs, jnp.zeros((240, n), BF16)], axis=0)
        half_rows = GROUPS * 16
        for half in range(2):
            cols = slice(256 * half, 256 * half + 256)
            for mxu, acc in ((0, tall0), (1, tall1)):
                pltpu.matmul_push_rhs(rhs[:, cols], staging_register=0, mxu_index=mxu, transpose=True)
                pltpu.matmul_acc_lhs(acc, hot[half_rows * mxu : half_rows * mxu + half_rows, cols], load_staged_rhs=0)
        quarter = lax.broadcasted_iota(jnp.int32, (8, 128), 1) // 32
        for mxu, acc in ((0, tall0), (1, tall1)):
            got = pltpu.matmul_pop(acc)[:, 0:128]
            for g in range(GROUPS // 2):
                parts = []
                for q in range(4):
                    block = got[32 * g + 8 * q : 32 * g + 8 * q + 8]
                    deep = block[:, 2:3] * 128.0 + block[:, 3:4]
                    parts.append([jnp.broadcast_to(v, (8, 128)) for v in (block[:, 0:1], block[:, 1:2], deep, block[:, 4:5])])
                for k in range(4):
                    value = parts[0][k]
                    for q in range(1, 4):
                        value = jnp.where(quarter == q, parts[q][k], value)
                    own_ref[k, mxu * (GROUPS // 2) + g] = value

        zs, ws = own_ref[2], own_ref[3]
        z_min = jnp.min(jnp.min(jnp.where(ws > 0.0, zs, 1e6), axis=1), axis=1, keepdims=True)
        z_max = jnp.max(jnp.max(jnp.where(ws > 0.0, zs, -1e6), axis=1), axis=1, keepdims=True)
        lane = lax.broadcasted_iota(jnp.int32, (GROUPS, 128), 1)
        chunk = lane.astype(F32) * 2.0
        even = jnp.full((GROUPS, 128), float(DUMMY), F32)
        odd = even
        total = jnp.zeros((GROUPS, 1), F32)
        lane8 = lax.broadcasted_iota(jnp.int32, (8, 128), 1)
        rows_ref[DUMMY] = jnp.zeros((8, 128), F32)
        for d in (8, 3, 4, 1, 6, 0, 2, 5, 7):
            if d < 8:

                @pl.when(present(*DIRS[d]))
                def _():
                    copy(7 - d).wait_recv()

            src = lists_ref.at[8] if d == 8 else got_ref.at[d]
            z_row = jnp.where(src[3:4, :] > 0.0, src[2:3, :], 2e6)
            low = jnp.sum(jnp.where(z_row < z_min - float(REACH), 1.0, 0.0), axis=1, keepdims=True)
            high = jnp.sum(jnp.where(z_row <= z_max + float(REACH), 1.0, 0.0), axis=1, keepdims=True)
            first = jnp.floor(low * (1.0 / STEP))
            count = jnp.where(high > low, jnp.floor((high - STEP * first + 31.0) * (1.0 / 32.0)), 0.0)
            at = chunk - total
            even = jnp.where((at >= 0.0) & (at < count), at * 2.0 + (first + float(ROWS * d)), even)
            at = at + 1.0
            odd = jnp.where((at >= 0.0) & (at < count), at * 2.0 + (first + float(ROWS * d)), odd)
            total = total + count
            parts = []
            for t in range(4):
                block = src[:, 128 * t : 128 * t + 128]
                block = jnp.concatenate([block, block], axis=0)
                for k in range(4):
                    part = block if k == 0 else pltpu.roll(block, 128 - 32 * k, 1)
                    part = jnp.where(lane8 < 32, part, pltpu.roll(part, 32, 1))
                    part = jnp.where(lane8 < 64, part, pltpu.roll(part, 64, 1))
                    parts.append(part)
            turned = [pltpu.roll(part, 16, 1) for part in parts] + [jnp.zeros((8, 128), F32)]
            for k in range(16):
                rows_ref[ROWS * d + 2 * k] = parts[k]
                rows_ref[ROWS * d + 2 * k + 1] = jnp.where((lane8 & 31) < 16, turned[k], turned[k + 1])
        units = jnp.floor((total + 1.0) * 0.5)
        name = lax.broadcasted_iota(jnp.int32, (GROUPS, 128), 0).astype(F32)
        number = jnp.sum(jnp.where((name >= begin) & (name < end), units, 0.0), axis=0, keepdims=True)
        turns = jnp.floor((number + 3.0) * 0.25)
        extra = 4.0 * turns - number
        units = units + jnp.sum(jnp.where(name == end - 1.0, extra, 0.0), axis=1, keepdims=True)
        table = jnp.where(lane == 127, units, even + 512.0 * odd)
        table_ref[0:GROUPS, :] = table.astype(jnp.int32)
        idle = jnp.where(lane_row == 127, float(1 << 20), float(DUMMY * 513))
        trips = jnp.where(lane_row == SUBREGIONS, starts[SUBREGIONS], turns)
        tail = jnp.concatenate([idle, trips, jnp.zeros((6, 128), F32)], axis=0)
        table_ref[GROUPS : GROUPS + 8, :] = tail.astype(jnp.int32)
        for d, (da, db) in enumerate(DIRS):

            @pl.when(present(da, db))
            def _():
                copy(d).wait_send()

    pl.run_scoped(
        body,
        pltpu.ACC(0)((16, 256), F32),
        pltpu.ACC(1)((16, 256), F32),
        pltpu.ACC(0)((16, 256), F32),
        pltpu.ACC(1)((16, 256), F32),
        pltpu.ACC(0)((GROUPS * 16, 256), F32),
        pltpu.ACC(1)((GROUPS * 16, 256), F32),
    )


def send_call(coords, weights, live):
    far = pl.BlockSpec(memory_space=pltpu.HBM)
    return pl.pallas_call(
        send_kernel,
        out_shape=(
            jax.ShapeDtypeStruct((GROUPS + 8, 128), jnp.int32),
            jax.ShapeDtypeStruct((DUMMY + 1, 8, 128), F32),
            jax.ShapeDtypeStruct((4, GROUPS, 8, 128), F32),
        ),
        in_specs=[far] * 3,
        out_specs=[pl.BlockSpec(memory_space=pltpu.VMEM)] * 3,
        scratch_shapes=[
            pltpu.VMEM((3, 1, 1, PART_DEV), jnp.int32),
            pltpu.VMEM((1, 1, PART_DEV), BF16),
            pltpu.VMEM((1, 1), jnp.int32),
            pltpu.VMEM((9, 4, PART_DEV), F32),
            pltpu.VMEM((8, 4, PART_DEV), F32),
            pltpu.SemaphoreType.DMA((3,)),
            pltpu.SemaphoreType.DMA((8,)),
            pltpu.SemaphoreType.DMA((8,)),
        ],
        compiler_params=pltpu.CompilerParams(collective_id=0, has_side_effects=True, vmem_limit_bytes=12 << 20),
    )(*[pltpu.with_memory_space_constraint(v, pltpu.HBM) for v in (coords, weights)], live)


LOG_SCALE = (S_BINS / 4.0) / math.log2(10.0)
LOG_BASE = -4.515457845
LEVELS_U = 24
LEVELS_V = 25
V_ROWS = 208


def count_kernel(table_ref, rows_ref, own_ref, out_ref, table_sm, sem):
    def body(a0, a1, b0, b1, hot_u, hot_v, bin_u, bin_v, far_w, own_w):
        sets = ((a0, a1), (b0, b1))
        copy = pltpu.make_async_copy(table_ref, table_sm, sem)
        copy.start()
        for acc in (a0, a1, b0, b1):
            pltpu.matmul_pop(acc)
        for half in range(2):
            hot_u[half, 8 * LEVELS_U :, :] = jnp.zeros((256 - 8 * LEVELS_U, 128 * TILES), BF16)
        copy.wait()
        trips = [table_sm[GROUPS + 1, r] for r in range(SUBREGIONS)]
        stop = table_sm[GROUPS + 1, SUBREGIONS]
        zero = jnp.zeros((16, 128), BF16)

        def index(state):
            g, b = state
            for half in range(2):
                for mxu in range(2):
                    group = jnp.minimum(g, GROUPS - 1)
                    xi, yi, zi, wi = own_ref[0, group], own_ref[1, group], own_ref[2, group], own_ref[3, group]
                    own_w[half, mxu] = jnp.concatenate([wi, wi], axis=0).astype(BF16)
                    pair = table_sm[g, b]
                    for t, row in ((2 * mxu, pair & 511), (2 * mxu + 1, pair >> 9)):
                        dx = xi - rows_ref[row, 0:1, :]
                        dy = yi - rows_ref[row, 1:2, :]
                        dz = zi - rows_ref[row, 2:3, :]
                        far_w[half, t] = jnp.broadcast_to(rows_ref[row, 3:4, :].astype(BF16), (16, 128))
                        dx2 = dx * dx
                        q = dx2 + dy * dy + dz * dz
                        s = jnp.floor(jnp.log2(q + 0.48) * LOG_SCALE + LOG_BASE)
                        near = jnp.floor(jnp.abs(dx) * lax.rsqrt(q) * float(MU_BINS) + 0.5)
                        mu = jnp.where(near * near * q > dx2 * float(MU_BINS * MU_BINS), near - 1.0, near)
                        c = s * float(MU_BINS) + jnp.minimum(mu, MU_BINS - 1.0)
                        u = jnp.floor(c * (1.0 / LEVELS_V) + 0.01)
                        v = c - u * float(LEVELS_V)
                        bin_u[half, t] = jnp.concatenate([u, u - 1.0], axis=0).astype(BF16)
                        bin_v[half, t] = jnp.concatenate([v, v - 1.0], axis=0).astype(BF16)
                    b = b + 1
                    over = b >= table_sm[g, 127]
                    g = jnp.where(over, g + 1, g)
                    g = jnp.where(g >= stop, GROUPS, g)
                    b = jnp.where(over, 0, b)
            return g, b

        def fill(half):
            for t in range(TILES):
                w_own = own_w[half, t // 2]
                u2, v2, w_far = bin_u[half, t], bin_v[half, t], far_w[half, t]
                lanes = slice(128 * t, 128 * t + 128)
                for k in range(LEVELS_U // 2):
                    hot_u[half, 16 * k : 16 * k + 16, lanes] = jnp.where(u2 == jnp.bfloat16(2 * k), w_far, zero)
                for k in range(V_ROWS // 16):
                    hot_v[half, 16 * k : 16 * k + 16, lanes] = jnp.where(v2 == jnp.bfloat16(2 * k), w_own, zero)

        def push(half):
            for mxu in range(2):
                pltpu.matmul_push_rhs(hot_u[half, :, 256 * mxu : 256 * mxu + 256], staging_register=half, mxu_index=mxu, transpose=True)

        def multiply(half, accs):
            for mxu in range(2):
                pltpu.matmul_acc_lhs(accs[mxu], hot_v[half, :, 256 * mxu : 256 * mxu + 256], load_staged_rhs=half)

        state = (jnp.where(stop > 0, 0, GROUPS).astype(jnp.int32), jnp.int32(0))
        state = index(state)
        for half in range(2):
            fill(half)
            push(half)
        state = index(state)
        def drain(r):
            accs = sets[r % 2]
            out_ref[r] = pltpu.matmul_pop(accs[0]) + pltpu.matmul_pop(accs[1])

        for r in range(SUBREGIONS):
            accs = sets[r % 2]

            def trip(_, state):
                for half in range(2):
                    multiply(half, accs)
                for half in range(2):
                    fill(half)
                    push(half)
                return index(state)

            state = lax.fori_loop(0, trips[r], trip, state)
            if r > 0:
                drain(r - 1)
        for half in range(2):
            multiply(half, sets[(SUBREGIONS - 1) % 2])
        drain(SUBREGIONS - 1)

    pl.run_scoped(
        body,
        pltpu.ACC(0)((V_ROWS, 256), F32),
        pltpu.ACC(1)((V_ROWS, 256), F32),
        pltpu.ACC(0)((V_ROWS, 256), F32),
        pltpu.ACC(1)((V_ROWS, 256), F32),
        pltpu.VMEM((2, 256, 128 * TILES), BF16),
        pltpu.VMEM((2, V_ROWS, 128 * TILES), BF16),
        pltpu.VMEM((2, TILES, 16, 128), BF16),
        pltpu.VMEM((2, TILES, 16, 128), BF16),
        pltpu.VMEM((2, TILES, 16, 128), BF16),
        pltpu.VMEM((2, 2, 16, 128), BF16),
    )


def count_call(table, rows, own):
    vmem = pl.BlockSpec(memory_space=pltpu.VMEM)
    return pl.pallas_call(
        count_kernel,
        out_shape=jax.ShapeDtypeStruct((SUBREGIONS, V_ROWS, 256), F32),
        in_specs=[vmem, vmem, vmem],
        out_specs=vmem,
        scratch_shapes=[pltpu.SMEM((GROUPS + 8, 128), jnp.int32), pltpu.SemaphoreType.DMA],
        compiler_params=pltpu.CompilerParams(vmem_limit_bytes=6 << 20),
    )(table, rows, own)


def total_kernel(skies, counts_ref, own_ref, total_ref, sent_ref, land_ref, send_sem, recv_sem):
    shell, sky = lax.axis_index("shell"), lax.axis_index("sky")
    barrier = pltpu.get_barrier_semaphore()
    for k in range(1, skies):
        pl.semaphore_signal(barrier, inc=1, device_id=(shell, lax.rem(sky + k, skies)), device_id_type=MESH)
    lane_in = lax.broadcasted_iota(jnp.int32, (256, 128), 0)
    lane_out = lax.broadcasted_iota(jnp.int32, (256, 128), 1)
    picks = [jnp.where((lane_in >> 3) + 32 * k == lane_out, 1.0, 0.0) for k in range(4)]
    diagonal = lax.broadcasted_iota(jnp.int32, (V_ROWS, 256), 0) & 7 == lax.broadcasted_iota(jnp.int32, (V_ROWS, 256), 1) & 7

    def folded(block):
        block = jnp.where(diagonal, block, 0.0).reshape(V_ROWS // 8, 8, 256)
        return jnp.concatenate([jnp.sum(block, axis=1), jnp.zeros((32 - V_ROWS // 8, 256), F32)], axis=0)

    def pack(rows):
        packed = jnp.dot(rows[0], picks[0], precision=lax.Precision.HIGHEST, preferred_element_type=F32)
        for k in range(1, 4):
            packed = packed + jnp.dot(rows[k], picks[k], precision=lax.Precision.HIGHEST, preferred_element_type=F32)
        return packed

    every = counts_ref[0]
    for r in range(1, SUBREGIONS):
        every = every + counts_ref[r]
    every = folded(every)
    mine = pack([every[8 * k : 8 * k + 8] for k in range(4)])
    sent_ref[...] = mine
    pl.semaphore_wait(barrier, skies - 1)

    def copy(k):
        return pltpu.make_async_remote_copy(
            src_ref=sent_ref,
            dst_ref=land_ref.at[k - 1],
            send_sem=send_sem.at[k - 1],
            recv_sem=recv_sem.at[k - 1],
            device_id=(shell, lax.rem(sky + k, skies)),
            device_id_type=MESH,
        )

    for k in range(1, skies):
        copy(k).start()
    each = [folded(counts_ref[r]) for r in range(SUBREGIONS)]
    own_ref[...] = pack([jnp.concatenate([block[8 * k : 8 * k + 8] for block in each], axis=0) for k in range(4)])
    total = mine
    for k in range(1, skies):
        copy(k).wait_recv()
        total = total + land_ref[k - 1]
    total_ref[...] = total
    for k in range(1, skies):
        copy(k).wait_send()


def total_call(counts):
    skies = lax.axis_size("sky")
    vmem = pl.BlockSpec(memory_space=pltpu.VMEM)
    return pl.pallas_call(
        functools.partial(total_kernel, skies),
        out_shape=(jax.ShapeDtypeStruct((8 * SUBREGIONS, 128), F32), jax.ShapeDtypeStruct((8, 128), F32)),
        in_specs=[vmem],
        out_specs=(vmem, vmem),
        scratch_shapes=[
            pltpu.VMEM((8, 128), F32),
            pltpu.VMEM((skies - 1, 8, 128), F32),
            pltpu.SemaphoreType.DMA((skies - 1,)),
            pltpu.SemaphoreType.DMA((skies - 1,)),
        ],
        compiler_params=pltpu.CompilerParams(collective_id=1, has_side_effects=True, vmem_limit_bytes=4 << 20),
    )(counts)


def edge_values():
    return [int(4.0 * 10.0 ** (4.0 * level / S_BINS) + 0.5) for level in range(S_BINS + 1)]


def bin_scale(patches):
    edges = edge_values()
    factor = SIDE_CELLS * SIDE_CELLS * SPAN_CELLS / (patches * PART_DEV * PART_DEV)
    values = []
    for level in range(S_BINS):
        volume = 4.0 * math.pi / 3.0 * (edges[level + 1] ** 1.5 - edges[level] ** 1.5) / MU_BINS
        values = values + [factor / volume] * MU_BINS
    return jnp.asarray(values, dtype=F32)


def unpacked(x):
    x = x.reshape(-1, 8, 4, 32).transpose(0, 3, 2, 1).reshape(-1, 32, 32)
    return x[:, :LEVELS_U, :LEVELS_V].reshape(-1, S_BINS * MU_BINS)


def local(coords, weights, live):
    counts = count_call(*send_call(coords, weights, live))
    packed, total = total_call(counts)
    leave = total[None] - packed.reshape(SUBREGIONS, 8, 128)
    return (unpacked(leave) * bin_scale(lax.axis_size("sky"))[None, :])[None]


def solution(mesh):
    in_specs = (P(None, "shell", "sky", None), P("shell", "sky", None), P("shell", "sky"))
    out_specs = P("shell", "sky", None)
    return jax.shard_map(local, mesh=mesh, in_specs=in_specs, out_specs=out_specs, check_vma=False)
```

```python
import functools, math
import jax, jax.numpy as jnp
from jax import lax
from jax.experimental import pallas as pl
from jax.experimental.pallas import tpu as pltpu
from jax.sharding import PartitionSpec as P

PART_DEV = 512
SIDE_CELLS = 256
SPAN_CELLS = 1024
SUBREGIONS = 8
S_BINS = 30
MU_BINS = 20
REACH = 199
CLOSE = 43
GROUPS = 24
STEP = 16
ROWS = PART_DEV // STEP
DUMMY = 9 * ROWS
TILES = 4
DIRS = tuple((da, db) for da in (-1, 0, 1) for db in (-1, 0, 1) if (da, db) != (0, 0))
MESH = pl.DeviceIdType.MESH
F32 = jnp.float32
BF16 = jnp.bfloat16


def send_kernel(coords_hbm, weight_hbm, live_hbm, table_ref, rows_ref, own_ref, coords_ref, weight_ref, live_ref, lists_ref, got_ref, load_sem, send_sem, recv_sem):
    shell, sky = lax.axis_index("shell"), lax.axis_index("sky")
    shells, skies = lax.axis_size("shell"), lax.axis_size("sky")
    barrier = pltpu.get_barrier_semaphore()
    loads = [
        pltpu.make_async_copy(src, dst, load_sem.at[k])
        for k, (src, dst) in enumerate(((coords_hbm, coords_ref), (weight_hbm, weight_ref), (live_hbm, live_ref)))
    ]
    for load in loads:
        load.start()

    def present(da, db):
        a, b = shell + da, sky + db
        return (a >= 0) & (a < shells) & (b >= 0) & (b < skies)

    for da, db in DIRS:

        @pl.when(present(da, db))
        def _():
            pl.semaphore_signal(barrier, inc=1, device_id=(shell + da, sky + db), device_id_type=MESH)

    for d, (da, db) in enumerate(DIRS):

        @pl.when(jnp.logical_not(present(da, db)))
        def _():
            got_ref[d] = jnp.zeros((4, PART_DEV), F32)

    def copy(d):
        da, db = DIRS[d]
        return pltpu.make_async_remote_copy(
            src_ref=lists_ref.at[d],
            dst_ref=got_ref.at[7 - d],
            send_sem=send_sem.at[d],
            recv_sem=recv_sem.at[7 - d],
            device_id=(shell + da, sky + db),
            device_id_type=MESH,
        )

    def body(acc0, acc1, acc2, acc3, tall0, tall1):
        for acc in (acc0, acc1, acc2, acc3, tall0, tall1):
            pltpu.matmul_pop(acc)
        for load in loads:
            load.wait()
        n = PART_DEV
        x = (coords_ref[0, 0] & (SIDE_CELLS - 1)).astype(F32)
        y = (coords_ref[1, 0] & (SIDE_CELLS - 1)).astype(F32)
        zi = coords_ref[2, 0]
        region = zi >> 7
        z_high = region.astype(F32)
        z_low = (zi & 127).astype(F32)
        slot = lax.broadcasted_iota(jnp.int32, (1, n), 1)
        alive = slot < live_ref[...]
        w = jnp.where(alive, weight_ref[0].astype(F32), 0.0)
        key = (jnp.where(alive, zi * n, SPAN_CELLS * n) + slot).astype(F32)
        key_column = jnp.transpose(jnp.broadcast_to(key, (128, n)))[:, 0:1]
        before = jnp.where(key_column < key, 1.0, 0.0).astype(BF16)
        valid = []
        for da, db in DIRS:
            ok = alive
            if da > 0:
                ok = ok & (x >= SIDE_CELLS - REACH)
            if da < 0:
                ok = ok & (x <= REACH - 1)
            if db > 0:
                ok = ok & (y >= SIDE_CELLS - REACH)
            if db < 0:
                ok = ok & (y <= REACH - 1)
            valid.append(ok)
        valid.append(alive)
        ones = [jnp.where(ok, 1.0, 0.0) for ok in valid]
        flags = jnp.concatenate(ones + [jnp.zeros((7, n), F32)], axis=0).astype(BF16)
        for half in range(2):
            rows = slice(256 * half, 256 * half + 256)
            pltpu.matmul_push_rhs(before[rows, 0:256], staging_register=0, mxu_index=0)
            pltpu.matmul_acc_lhs(acc0, flags[:, rows], load_staged_rhs=0)
            pltpu.matmul_push_rhs(before[rows, 256:512], staging_register=0, mxu_index=1)
            pltpu.matmul_acc_lhs(acc1, flags[:, rows], load_staged_rhs=0)
        rank = jnp.concatenate([pltpu.matmul_pop(acc0), pltpu.matmul_pop(acc1)], axis=1)
        attrs = jnp.concatenate([x, y, z_high, z_low, w, jnp.zeros((11, n), F32)], axis=0).astype(BF16)
        place = lax.broadcasted_iota(jnp.int32, (256, n), 0).astype(F32).astype(BF16)
        one, zero = jnp.ones((256, n), BF16), jnp.zeros((256, n), BF16)
        accs = ((acc0, acc1), (acc2, acc3))
        beside_shell = 1 + (shell > 0).astype(jnp.int32) + (shell < shells - 1).astype(jnp.int32)
        beside_sky = 1 + (sky > 0).astype(jnp.int32) + (sky < skies - 1).astype(jnp.int32)

        def build(d):
            target = jnp.where(valid[d], rank[d : d + 1, :], -1.0)
            pair = accs[d % 2]
            for mxu in range(2):
                near = jnp.broadcast_to((target - 256.0 * mxu).astype(BF16), (256, n))
                hot = jnp.where(place == near, one, zero)
                for half in range(2):
                    cols = slice(256 * half, 256 * half + 256)
                    pltpu.matmul_push_rhs(hot[:, cols], staging_register=0, mxu_index=mxu, transpose=True)
                    pltpu.matmul_acc_lhs(pair[mxu], attrs[:, cols], load_staged_rhs=0)
            da, db = DIRS[d] if d < 8 else (0, 0)
            for mxu in range(2):
                got = pltpu.matmul_pop(pair[mxu])
                lanes = slice(256 * mxu, 256 * mxu + 256)
                lists_ref[d, 0:1, lanes] = got[0:1] - float(SIDE_CELLS * da)
                lists_ref[d, 1:2, lanes] = got[1:2] - float(SIDE_CELLS * db)
                lists_ref[d, 2:3, lanes] = got[2:3] * 128.0 + got[3:4]
                lists_ref[d, 3:4, lanes] = got[4:5]

        for d in range(9):
            build(d)
        pl.semaphore_wait(barrier, beside_shell * beside_sky - 1)
        for d in (0, 2, 5, 7, 3, 4, 1, 6):

            @pl.when(present(*DIRS[d]))
            def _():
                copy(d).start()

        shift = jnp.zeros((1, n), F32)
        first = jnp.zeros((1, 1), F32)
        group = jnp.zeros((1, 1), F32)
        starts = []
        for r in range(SUBREGIONS):
            here = alive & (region == r)
            starts.append(group)
            shift = jnp.where(here, 32.0 * group - first, shift)
            count = jnp.sum(jnp.where(here, 1.0, 0.0), axis=1, keepdims=True)
            first = first + count
            group = group + jnp.floor((count + 31.0) * (1.0 / 32.0))
        starts = starts + [group]
        lane_row = lax.broadcasted_iota(jnp.int32, (1, 128), 1)
        begin, end = jnp.zeros((1, 128), F32), jnp.zeros((1, 128), F32)
        for r in range(SUBREGIONS):
            begin = jnp.where(lane_row == r, starts[r], begin)
            end = jnp.where(lane_row == r, starts[r + 1], end)
        target = jnp.where(alive, rank[8:9, :] + shift, -1.0)
        wide = lax.broadcasted_iota(jnp.int32, (GROUPS * 32, 1), 0).astype(F32)
        hot = jnp.where(wide == target, 1.0, 0.0).astype(BF16)
        rhs = jnp.concatenate([attrs, jnp.zeros((240, n), BF16)], axis=0)
        half_rows = GROUPS * 16
        for half in range(2):
            cols = slice(256 * half, 256 * half + 256)
            for mxu, acc in ((0, tall0), (1, tall1)):
                pltpu.matmul_push_rhs(rhs[:, cols], staging_register=0, mxu_index=mxu, transpose=True)
                pltpu.matmul_acc_lhs(acc, hot[half_rows * mxu : half_rows * mxu + half_rows, cols], load_staged_rhs=0)
        quarter = lax.broadcasted_iota(jnp.int32, (8, 128), 1) // 32
        for mxu, acc in ((0, tall0), (1, tall1)):
            got = pltpu.matmul_pop(acc)[:, 0:128]
            for g in range(GROUPS // 2):
                parts = []
                for q in range(4):
                    block = got[32 * g + 8 * q : 32 * g + 8 * q + 8]
                    deep = block[:, 2:3] * 128.0 + block[:, 3:4]
                    parts.append([jnp.broadcast_to(v, (8, 128)) for v in (block[:, 0:1], block[:, 1:2], deep, block[:, 4:5])])
                for k in range(4):
                    value = parts[0][k]
                    for q in range(1, 4):
                        value = jnp.where(quarter == q, parts[q][k], value)
                    own_ref[k, mxu * (GROUPS // 2) + g] = value

        zs, ws = own_ref[2], own_ref[3]
        z_min = jnp.min(jnp.min(jnp.where(ws > 0.0, zs, 1e6), axis=1), axis=1, keepdims=True)
        z_max = jnp.max(jnp.max(jnp.where(ws > 0.0, zs, -1e6), axis=1), axis=1, keepdims=True)
        lane = lax.broadcasted_iota(jnp.int32, (GROUPS, 128), 1)
        chunk = lane.astype(F32) * 2.0
        near_even = near_odd = far_even = far_odd = jnp.full((GROUPS, 128), float(DUMMY), F32)
        near_total = far_total = jnp.zeros((GROUPS, 1), F32)
        lane8 = lax.broadcasted_iota(jnp.int32, (8, 128), 1)
        rows_ref[DUMMY] = jnp.zeros((8, 128), F32)
        for d in (8, 3, 4, 1, 6, 0, 2, 5, 7):
            if d < 8:

                @pl.when(present(*DIRS[d]))
                def _():
                    copy(7 - d).wait_recv()

            src = lists_ref.at[8] if d == 8 else got_ref.at[d]
            z_row = jnp.where(src[3:4, :] > 0.0, src[2:3, :], 2e6)
            below = lambda edge: jnp.sum(jnp.where(z_row < edge, 1.0, 0.0), axis=1, keepdims=True)
            low, high = below(z_min - float(REACH)), below(z_max + float(REACH + 1))
            first = jnp.floor(low * (1.0 / STEP))
            base = STEP * first
            count = jnp.where(high > low, jnp.floor((high - base + 31.0) * (1.0 / 32.0)), 0.0)
            head = jnp.floor((below(z_min - float(CLOSE)) - base) * (1.0 / 32.0))
            head = jnp.minimum(jnp.maximum(head, 0.0), count)
            rest = jnp.floor((below(z_max + float(CLOSE + 1)) - base + 31.0) * (1.0 / 32.0))
            rest = jnp.minimum(jnp.maximum(rest, head), count)
            middle = rest - head
            start = first + float(ROWS * d)

            def near_put(at, table):
                return jnp.where((at >= 0.0) & (at < middle), (at + head) * 2.0 + start, table)

            def far_put(at, table):
                return jnp.where((at >= 0.0) & (at < count - middle), (at + jnp.where(at >= head, middle, 0.0)) * 2.0 + start, table)

            near_even = near_put(chunk - near_total, near_even)
            near_odd = near_put(chunk + 1.0 - near_total, near_odd)
            far_even = far_put(chunk - far_total, far_even)
            far_odd = far_put(chunk + 1.0 - far_total, far_odd)
            near_total = near_total + middle
            far_total = far_total + (count - middle)
            parts = []
            for t in range(4):
                block = src[:, 128 * t : 128 * t + 128]
                block = jnp.concatenate([block, block], axis=0)
                for k in range(4):
                    part = block if k == 0 else pltpu.roll(block, 128 - 32 * k, 1)
                    part = jnp.where(lane8 < 32, part, pltpu.roll(part, 32, 1))
                    part = jnp.where(lane8 < 64, part, pltpu.roll(part, 64, 1))
                    parts.append(part)
            turned = [pltpu.roll(part, 16, 1) for part in parts] + [jnp.zeros((8, 128), F32)]
            for k in range(16):
                rows_ref[ROWS * d + 2 * k] = parts[k]
                rows_ref[ROWS * d + 2 * k + 1] = jnp.where((lane8 & 31) < 16, turned[k], turned[k + 1])
        name = lax.broadcasted_iota(jnp.int32, (GROUPS, 128), 0).astype(F32)
        idle = jnp.where(lane_row == 127, float(1 << 20), float(DUMMY * 513))

        def finish(units, even, odd):
            number = jnp.sum(jnp.where((name >= begin) & (name < end), units, 0.0), axis=0, keepdims=True)
            turns = jnp.floor((number + 3.0) * 0.25)
            extra = 4.0 * turns - number
            units = units + jnp.sum(jnp.where(name == end - 1.0, extra, 0.0), axis=1, keepdims=True)
            return jnp.where(lane == 127, units, even + 512.0 * odd), turns

        near_table, near_turns = finish(jnp.floor((near_total + 1.0) * 0.5), near_even, near_odd)
        far_table, far_turns = finish(jnp.maximum(jnp.floor((far_total + 3.0) * 0.25), 1.0), far_even, far_odd)
        far_turns = jnp.where(lane_row == SUBREGIONS, starts[SUBREGIONS], far_turns)
        pad = jnp.zeros((6, 128), F32)
        table_ref[...] = jnp.concatenate([near_table, idle, near_turns, pad, far_table, idle, far_turns, pad], axis=0).astype(jnp.int32)
        for d, (da, db) in enumerate(DIRS):

            @pl.when(present(da, db))
            def _():
                copy(d).wait_send()

    pl.run_scoped(
        body,
        pltpu.ACC(0)((16, 256), F32),
        pltpu.ACC(1)((16, 256), F32),
        pltpu.ACC(0)((16, 256), F32),
        pltpu.ACC(1)((16, 256), F32),
        pltpu.ACC(0)((GROUPS * 16, 256), F32),
        pltpu.ACC(1)((GROUPS * 16, 256), F32),
    )


def send_call(coords, weights, live):
    far = pl.BlockSpec(memory_space=pltpu.HBM)
    return pl.pallas_call(
        send_kernel,
        out_shape=(
            jax.ShapeDtypeStruct((2 * GROUPS + 16, 128), jnp.int32),
            jax.ShapeDtypeStruct((DUMMY + 1, 8, 128), F32),
            jax.ShapeDtypeStruct((4, GROUPS, 8, 128), F32),
        ),
        in_specs=[far] * 3,
        out_specs=[pl.BlockSpec(memory_space=pltpu.VMEM)] * 3,
        scratch_shapes=[
            pltpu.VMEM((3, 1, 1, PART_DEV), jnp.int32),
            pltpu.VMEM((1, 1, PART_DEV), BF16),
            pltpu.VMEM((1, 1), jnp.int32),
            pltpu.VMEM((9, 4, PART_DEV), F32),
            pltpu.VMEM((8, 4, PART_DEV), F32),
            pltpu.SemaphoreType.DMA((3,)),
            pltpu.SemaphoreType.DMA((8,)),
            pltpu.SemaphoreType.DMA((8,)),
        ],
        compiler_params=pltpu.CompilerParams(collective_id=0, has_side_effects=True, vmem_limit_bytes=12 << 20),
    )(*[pltpu.with_memory_space_constraint(v, pltpu.HBM) for v in (coords, weights)], live)


LOG_SCALE = (S_BINS / 4.0) / math.log2(10.0)
LOG_BASE = -4.515457845
LEVELS_U = 24
LEVELS_V = 25
FAR_FIRST = 400
FAR_U = 16
FAR_V = 13
V_ROWS = 208


def count_kernel(table_ref, rows_ref, own_ref, out_ref, table_sm, sem):
    def body(a0, a1, b0, b1, hot_u, hot_v, bin_u, bin_v, far_w, own_w):
        sets = ((a0, a1), (b0, b1))
        copy = pltpu.make_async_copy(table_ref, table_sm, sem)
        copy.start()
        for acc in (a0, a1, b0, b1):
            pltpu.matmul_pop(acc)
        for half in range(2):
            hot_u[half, 8 * LEVELS_U :, :] = jnp.zeros((256 - 8 * LEVELS_U, 128 * TILES), BF16)
        copy.wait()
        stop = table_sm[2 * GROUPS + 9, SUBREGIONS]
        zero = jnp.zeros((16, 128), BF16)

        def combined(own, row):
            dx = own[0] - rows_ref[row, 0:1, :]
            dy = own[1] - rows_ref[row, 1:2, :]
            dz = own[2] - rows_ref[row, 2:3, :]
            dx2 = dx * dx
            q = dx2 + dy * dy + dz * dz
            s = jnp.floor(jnp.log2(q + 0.48) * LOG_SCALE + LOG_BASE)
            near = jnp.floor(jnp.abs(dx) * lax.rsqrt(q) * float(MU_BINS) + 0.5)
            mu = jnp.where(near * near * q > dx2 * float(MU_BINS * MU_BINS), near - 1.0, near)
            return s * float(MU_BINS) + jnp.minimum(mu, MU_BINS - 1.0)

        def near_unit(own, g, b, half, mxu):
            pair = table_sm[g, b]
            for t, row in ((2 * mxu, pair & 511), (2 * mxu + 1, pair >> 9)):
                far_w[half, t] = jnp.broadcast_to(rows_ref[row, 3:4, :].astype(BF16), (16, 128))
                c = combined(own, row)
                u = jnp.floor(c * (1.0 / LEVELS_V) + 0.01)
                v = c - u * float(LEVELS_V)
                bin_u[half, t] = jnp.concatenate([u, u - 1.0], axis=0).astype(BF16)
                bin_v[half, t] = jnp.concatenate([v, v - 1.0], axis=0).astype(BF16)

        def far_unit(own, g, b, half, mxu):
            for k in range(2):
                pair = table_sm[GROUPS + 8 + g, 2 * b + k]
                rows = (pair & 511, pair >> 9)
                t = 2 * mxu + k
                far_w[half, t] = jnp.concatenate([jnp.broadcast_to(rows_ref[row, 3:4, :], (8, 128)) for row in rows], axis=0).astype(BF16)
                us, vs = [], []
                for row in rows:
                    c = combined(own, row) - float(FAR_FIRST)
                    u = jnp.floor(c * (1.0 / FAR_V) + 0.01)
                    us.append(u)
                    vs.append(c - u * float(FAR_V))
                bin_u[half, t] = jnp.concatenate(us, axis=0).astype(BF16)
                bin_v[half, t] = jnp.concatenate(vs, axis=0).astype(BF16)

        def near_fill(half):
            for t in range(TILES):
                u2, v2, w_far, w_own = bin_u[half, t], bin_v[half, t], far_w[half, t], own_w[half, t // 2]
                lanes = slice(128 * t, 128 * t + 128)
                for k in range(LEVELS_U // 2):
                    hot_u[half, 16 * k : 16 * k + 16, lanes] = jnp.where(u2 == jnp.bfloat16(2 * k), w_far, zero)
                for k in range(V_ROWS // 16):
                    hot_v[half, 16 * k : 16 * k + 16, lanes] = jnp.where(v2 == jnp.bfloat16(2 * k), w_own, zero)

        def far_fill(half):
            for t in range(TILES):
                u2, v2, w_far, w_own = bin_u[half, t], bin_v[half, t], far_w[half, t], own_w[half, t // 2]
                lanes = slice(128 * t, 128 * t + 128)
                for k in range(FAR_U):
                    hot_u[half, 16 * k : 16 * k + 16, lanes] = jnp.where(u2 == jnp.bfloat16(k), w_far, zero)
                for k in range(FAR_V):
                    hot_v[half, 16 * k : 16 * k + 16, lanes] = jnp.where(v2 == jnp.bfloat16(k), w_own, zero)

        def push(half):
            for mxu in range(2):
                pltpu.matmul_push_rhs(hot_u[half, :, 256 * mxu : 256 * mxu + 256], staging_register=half, mxu_index=mxu, transpose=True)

        def multiply(half, accs):
            for mxu in range(2):
                pltpu.matmul_acc_lhs(accs[mxu], hot_v[half, :, 256 * mxu : 256 * mxu + 256], load_staged_rhs=half)

        def phase(unit, fill, first_row, out):
            def index(state):
                g, b = state
                for half in range(2):
                    for mxu in range(2):
                        group = jnp.minimum(g, GROUPS - 1)
                        own = (own_ref[0, group], own_ref[1, group], own_ref[2, group])
                        wi = own_ref[3, group]
                        own_w[half, mxu] = jnp.concatenate([wi, wi], axis=0).astype(BF16)
                        unit(own, g, b, half, mxu)
                        b = b + 1
                        over = b >= table_sm[first_row + g, 127]
                        g = jnp.where(over, g + 1, g)
                        g = jnp.where(g >= stop, GROUPS, g)
                        b = jnp.where(over, 0, b)
                return g, b

            def drain(r):
                accs = sets[r % 2]
                out_ref[out + r] = pltpu.matmul_pop(accs[0]) + pltpu.matmul_pop(accs[1])

            state = index((jnp.where(stop > 0, 0, GROUPS).astype(jnp.int32), jnp.int32(0)))
            for half in range(2):
                fill(half)
                push(half)
            state = index(state)
            for r in range(SUBREGIONS):
                accs = sets[r % 2]

                def trip(_, state):
                    for half in range(2):
                        multiply(half, accs)
                    for half in range(2):
                        fill(half)
                        push(half)
                    return index(state)

                state = lax.fori_loop(0, table_sm[first_row + GROUPS + 1, r], trip, state)
                if r > 0:
                    drain(r - 1)
            for half in range(2):
                multiply(half, sets[(SUBREGIONS - 1) % 2])
            drain(SUBREGIONS - 1)

        phase(near_unit, near_fill, 0, 0)
        phase(far_unit, far_fill, GROUPS + 8, SUBREGIONS)

    pl.run_scoped(
        body,
        pltpu.ACC(0)((V_ROWS, 256), F32),
        pltpu.ACC(1)((V_ROWS, 256), F32),
        pltpu.ACC(0)((V_ROWS, 256), F32),
        pltpu.ACC(1)((V_ROWS, 256), F32),
        pltpu.VMEM((2, 256, 128 * TILES), BF16),
        pltpu.VMEM((2, V_ROWS, 128 * TILES), BF16),
        pltpu.VMEM((2, TILES, 16, 128), BF16),
        pltpu.VMEM((2, TILES, 16, 128), BF16),
        pltpu.VMEM((2, TILES, 16, 128), BF16),
        pltpu.VMEM((2, 2, 16, 128), BF16),
    )


def count_call(table, rows, own):
    vmem = pl.BlockSpec(memory_space=pltpu.VMEM)
    return pl.pallas_call(
        count_kernel,
        out_shape=jax.ShapeDtypeStruct((2 * SUBREGIONS, V_ROWS, 256), F32),
        in_specs=[vmem, vmem, vmem],
        out_specs=vmem,
        scratch_shapes=[pltpu.SMEM((2 * GROUPS + 16, 128), jnp.int32), pltpu.SemaphoreType.DMA],
        compiler_params=pltpu.CompilerParams(vmem_limit_bytes=8 << 20),
    )(table, rows, own)


def total_kernel(skies, counts_ref, own_ref, total_ref, sent_ref, land_ref, send_sem, recv_sem):
    shell, sky = lax.axis_index("shell"), lax.axis_index("sky")
    barrier = pltpu.get_barrier_semaphore()
    for k in range(1, skies):
        pl.semaphore_signal(barrier, inc=1, device_id=(shell, lax.rem(sky + k, skies)), device_id_type=MESH)
    lane_in = lax.broadcasted_iota(jnp.int32, (256, 128), 0)
    lane_out = lax.broadcasted_iota(jnp.int32, (256, 128), 1)
    picks = [jnp.where((lane_in >> 3) + 32 * k == lane_out, 1.0, 0.0) for k in range(4)]
    level = lane_in >> 4
    for k in range(2):
        spot = 32 * (2 * k + (level >> 3)) + LEVELS_U + (level & 7)
        picks.append(jnp.where(spot == lane_out, 1.0, 0.0))

    def folded(block, size):
        rows = lax.broadcasted_iota(jnp.int32, (V_ROWS, 256), 0)
        lanes = lax.broadcasted_iota(jnp.int32, (V_ROWS, 256), 1)
        block = jnp.where((rows & (size - 1)) == (lanes & (size - 1)), block, 0.0)
        block = jnp.sum(block.reshape(V_ROWS // size, size, 256), axis=1)
        full = 32 * 8 // size
        return jnp.concatenate([block, jnp.zeros((full - V_ROWS // size, 256), F32)], axis=0)

    def pack(pairs):
        packed = None
        for k in range(6):
            rows = [pair[k // 4][8 * (k % 4) : 8 * (k % 4) + 8] for pair in pairs]
            rows = rows[0] if len(rows) == 1 else jnp.concatenate(rows, axis=0)
            part = jnp.dot(rows, picks[k], precision=lax.Precision.HIGHEST, preferred_element_type=F32)
            packed = part if packed is None else packed + part
        return packed

    every = []
    for out, size in ((0, 8), (SUBREGIONS, 16)):
        block = counts_ref[out]
        for r in range(1, SUBREGIONS):
            block = block + counts_ref[out + r]
        every.append(folded(block, size))
    mine = pack([every])
    sent_ref[...] = mine
    pl.semaphore_wait(barrier, skies - 1)

    def copy(k):
        return pltpu.make_async_remote_copy(
            src_ref=sent_ref,
            dst_ref=land_ref.at[k - 1],
            send_sem=send_sem.at[k - 1],
            recv_sem=recv_sem.at[k - 1],
            device_id=(shell, lax.rem(sky + k, skies)),
            device_id_type=MESH,
        )

    for k in range(1, skies):
        copy(k).start()
    own_ref[...] = pack([(folded(counts_ref[r], 8), folded(counts_ref[SUBREGIONS + r], 16)) for r in range(SUBREGIONS)])
    total = mine
    for k in range(1, skies):
        copy(k).wait_recv()
        total = total + land_ref[k - 1]
    total_ref[...] = total
    for k in range(1, skies):
        copy(k).wait_send()


def total_call(counts):
    skies = lax.axis_size("sky")
    vmem = pl.BlockSpec(memory_space=pltpu.VMEM)
    return pl.pallas_call(
        functools.partial(total_kernel, skies),
        out_shape=(jax.ShapeDtypeStruct((8 * SUBREGIONS, 128), F32), jax.ShapeDtypeStruct((8, 128), F32)),
        in_specs=[vmem],
        out_specs=(vmem, vmem),
        scratch_shapes=[
            pltpu.VMEM((8, 128), F32),
            pltpu.VMEM((skies - 1, 8, 128), F32),
            pltpu.SemaphoreType.DMA((skies - 1,)),
            pltpu.SemaphoreType.DMA((skies - 1,)),
        ],
        compiler_params=pltpu.CompilerParams(collective_id=1, has_side_effects=True, vmem_limit_bytes=4 << 20),
    )(counts)


def edge_values():
    return [int(4.0 * 10.0 ** (4.0 * level / S_BINS) + 0.5) for level in range(S_BINS + 1)]


def bin_scale(patches):
    edges = edge_values()
    factor = SIDE_CELLS * SIDE_CELLS * SPAN_CELLS / (patches * PART_DEV * PART_DEV)
    values = []
    for level in range(S_BINS):
        volume = 4.0 * math.pi / 3.0 * (edges[level + 1] ** 1.5 - edges[level] ** 1.5) / MU_BINS
        values = values + [factor / volume] * MU_BINS
    return jnp.asarray(values, dtype=F32)


def unpacked(x):
    x = x.reshape(-1, 8, 4, 32)
    near = x[..., :LEVELS_U].transpose(0, 3, 2, 1).reshape(-1, LEVELS_U, 32)
    near = near[:, :, :LEVELS_V].reshape(-1, S_BINS * MU_BINS)
    far = x[..., LEVELS_U:].reshape(-1, 8, 2, 2, 8).transpose(0, 3, 4, 2, 1).reshape(-1, FAR_U, 16)
    far = far[:, :, :FAR_V].reshape(-1, FAR_U * FAR_V)[:, : S_BINS * MU_BINS - FAR_FIRST]
    return near + jnp.pad(far, ((0, 0), (FAR_FIRST, 0)))


def local(coords, weights, live):
    counts = count_call(*send_call(coords, weights, live))
    packed, total = total_call(counts)
    leave = total[None] - packed.reshape(SUBREGIONS, 8, 128)
    return (unpacked(leave) * bin_scale(lax.axis_size("sky"))[None, :])[None]


def solution(mesh):
    in_specs = (P(None, "shell", "sky", None), P("shell", "sky", None), P("shell", "sky"))
    out_specs = P("shell", "sky", None)
    return jax.shard_map(local, mesh=mesh, in_specs=in_specs, out_specs=out_specs, check_vma=False)
```

```python
import functools, math
import jax, jax.numpy as jnp
from jax import lax
from jax.experimental import pallas as pl
from jax.experimental.pallas import tpu as pltpu
from jax.sharding import PartitionSpec as P

PART_DEV = 512
SIDE_CELLS = 256
SPAN_CELLS = 1024
SUBREGIONS = 8
S_BINS = 30
MU_BINS = 20
REACH = 199
EARLY = 3
GROUPS = 24
STEP = 16
ROWS = PART_DEV // STEP
DUMMY = 9 * ROWS
TILES = 4
DIRS = tuple((da, db) for da in (-1, 0, 1) for db in (-1, 0, 1) if (da, db) != (0, 0))
MESH = pl.DeviceIdType.MESH
F32 = jnp.float32
BF16 = jnp.bfloat16


def send_kernel(coords_hbm, weight_hbm, live_hbm, table_ref, rows_ref, own_ref, coords_ref, weight_ref, live_ref, lists_ref, got_ref, load_sem, send_sem, recv_sem):
    shell, sky = lax.axis_index("shell"), lax.axis_index("sky")
    shells, skies = lax.axis_size("shell"), lax.axis_size("sky")
    barrier = pltpu.get_barrier_semaphore()
    loads = [
        pltpu.make_async_copy(src, dst, load_sem.at[k])
        for k, (src, dst) in enumerate(((coords_hbm, coords_ref), (weight_hbm, weight_ref), (live_hbm, live_ref)))
    ]
    for load in loads:
        load.start()

    def present(da, db):
        a, b = shell + da, sky + db
        return (a >= 0) & (a < shells) & (b >= 0) & (b < skies)

    for da, db in DIRS:

        @pl.when(present(da, db))
        def _():
            pl.semaphore_signal(barrier, inc=1, device_id=(shell + da, sky + db), device_id_type=MESH)

    for d, (da, db) in enumerate(DIRS):

        @pl.when(jnp.logical_not(present(da, db)))
        def _():
            got_ref[d] = jnp.zeros((4, PART_DEV), F32)

    def copy(d):
        da, db = DIRS[d]
        return pltpu.make_async_remote_copy(
            src_ref=lists_ref.at[d],
            dst_ref=got_ref.at[7 - d],
            send_sem=send_sem.at[d],
            recv_sem=recv_sem.at[7 - d],
            device_id=(shell + da, sky + db),
            device_id_type=MESH,
        )

    def body(acc0, acc1, acc2, acc3, tall0, tall1):
        for acc in (acc0, acc1, acc2, acc3, tall0, tall1):
            pltpu.matmul_pop(acc)
        for load in loads:
            load.wait()
        n = PART_DEV
        x = (coords_ref[0, 0] & (SIDE_CELLS - 1)).astype(F32)
        y = (coords_ref[1, 0] & (SIDE_CELLS - 1)).astype(F32)
        zi = coords_ref[2, 0]
        region = zi >> 7
        z_high = region.astype(F32)
        z_low = (zi & 127).astype(F32)
        slot = lax.broadcasted_iota(jnp.int32, (1, n), 1)
        alive = slot < live_ref[...]
        w = jnp.where(alive, weight_ref[0].astype(F32), 0.0)
        key = (jnp.where(alive, zi * n, SPAN_CELLS * n) + slot).astype(F32)
        key_column = jnp.transpose(jnp.broadcast_to(key, (128, n)))[:, 0:1]
        before = jnp.where(key_column < key, 1.0, 0.0).astype(BF16)
        valid = []
        for da, db in DIRS:
            ok = alive
            if da > 0:
                ok = ok & (x >= SIDE_CELLS - REACH)
            if da < 0:
                ok = ok & (x <= REACH - 1)
            if db > 0:
                ok = ok & (y >= SIDE_CELLS - REACH)
            if db < 0:
                ok = ok & (y <= REACH - 1)
            valid.append(ok)
        valid.append(alive)
        ones = [jnp.where(ok, 1.0, 0.0) for ok in valid]
        flags = jnp.concatenate(ones + [jnp.zeros((7, n), F32)], axis=0).astype(BF16)
        for half in range(2):
            rows = slice(256 * half, 256 * half + 256)
            pltpu.matmul_push_rhs(before[rows, 0:256], staging_register=0, mxu_index=0)
            pltpu.matmul_acc_lhs(acc0, flags[:, rows], load_staged_rhs=0)
            pltpu.matmul_push_rhs(before[rows, 256:512], staging_register=0, mxu_index=1)
            pltpu.matmul_acc_lhs(acc1, flags[:, rows], load_staged_rhs=0)
        rank = jnp.concatenate([pltpu.matmul_pop(acc0), pltpu.matmul_pop(acc1)], axis=1)
        attrs = jnp.concatenate([x, y, z_high, z_low, w, jnp.zeros((11, n), F32)], axis=0).astype(BF16)
        place = lax.broadcasted_iota(jnp.int32, (256, n), 0).astype(F32).astype(BF16)
        one, zero = jnp.ones((256, n), BF16), jnp.zeros((256, n), BF16)
        accs = ((acc0, acc1), (acc2, acc3))
        beside_shell = 1 + (shell > 0).astype(jnp.int32) + (shell < shells - 1).astype(jnp.int32)
        beside_sky = 1 + (sky > 0).astype(jnp.int32) + (sky < skies - 1).astype(jnp.int32)

        def build(d):
            target = jnp.where(valid[d], rank[d : d + 1, :], -1.0)
            pair = accs[d % 2]
            for mxu in range(2):
                near = jnp.broadcast_to((target - 256.0 * mxu).astype(BF16), (256, n))
                hot = jnp.where(place == near, one, zero)
                for half in range(2):
                    cols = slice(256 * half, 256 * half + 256)
                    pltpu.matmul_push_rhs(hot[:, cols], staging_register=0, mxu_index=mxu, transpose=True)
                    pltpu.matmul_acc_lhs(pair[mxu], attrs[:, cols], load_staged_rhs=0)
            da, db = DIRS[d] if d < 8 else (0, 0)
            for mxu in range(2):
                got = pltpu.matmul_pop(pair[mxu])
                lanes = slice(256 * mxu, 256 * mxu + 256)
                lists_ref[d, 0:1, lanes] = got[0:1] - float(SIDE_CELLS * da)
                lists_ref[d, 1:2, lanes] = got[1:2] - float(SIDE_CELLS * db)
                lists_ref[d, 2:3, lanes] = got[2:3] * 128.0 + got[3:4]
                lists_ref[d, 3:4, lanes] = got[4:5]

        for d in range(9):
            build(d)
        pl.semaphore_wait(barrier, beside_shell * beside_sky - 1)
        for d in (0, 2, 5, 7, 3, 4, 1, 6):

            @pl.when(present(*DIRS[d]))
            def _():
                copy(d).start()

        shift = jnp.zeros((1, n), F32)
        first = jnp.zeros((1, 1), F32)
        group = jnp.zeros((1, 1), F32)
        starts = []
        for r in range(SUBREGIONS):
            here = alive & (region == r)
            starts.append(group)
            shift = jnp.where(here, 32.0 * group - first, shift)
            count = jnp.sum(jnp.where(here, 1.0, 0.0), axis=1, keepdims=True)
            first = first + count
            group = group + jnp.floor((count + 31.0) * (1.0 / 32.0))
        starts = starts + [group]
        lane_row = lax.broadcasted_iota(jnp.int32, (1, 128), 1)
        begin, end = jnp.zeros((1, 128), F32), jnp.zeros((1, 128), F32)
        for r in range(SUBREGIONS):
            begin = jnp.where(lane_row == r, starts[r], begin)
            end = jnp.where(lane_row == r, starts[r + 1], end)
        target = jnp.where(alive, rank[8:9, :] + shift, -1.0)
        wide = lax.broadcasted_iota(jnp.int32, (GROUPS * 32, 1), 0).astype(F32)
        hot = jnp.where(wide == target, 1.0, 0.0).astype(BF16)
        rhs = jnp.concatenate([attrs, jnp.zeros((240, n), BF16)], axis=0)
        half_rows = GROUPS * 16
        for half in range(2):
            cols = slice(256 * half, 256 * half + 256)
            for mxu, acc in ((0, tall0), (1, tall1)):
                pltpu.matmul_push_rhs(rhs[:, cols], staging_register=0, mxu_index=mxu, transpose=True)
                pltpu.matmul_acc_lhs(acc, hot[half_rows * mxu : half_rows * mxu + half_rows, cols], load_staged_rhs=0)
        quarter = lax.broadcasted_iota(jnp.int32, (8, 128), 1) // 32
        for mxu, acc in ((0, tall0), (1, tall1)):
            got = pltpu.matmul_pop(acc)[:, 0:128]
            for g in range(GROUPS // 2):
                parts = []
                for q in range(4):
                    block = got[32 * g + 8 * q : 32 * g + 8 * q + 8]
                    deep = block[:, 2:3] * 128.0 + block[:, 3:4]
                    parts.append([jnp.broadcast_to(v, (8, 128)) for v in (block[:, 0:1], block[:, 1:2], deep, block[:, 4:5])])
                for k in range(4):
                    value = parts[0][k]
                    for q in range(1, 4):
                        value = jnp.where(quarter == q, parts[q][k], value)
                    own_ref[k, mxu * (GROUPS // 2) + g] = value

        zs, ws = own_ref[2], own_ref[3]
        z_min = jnp.min(jnp.min(jnp.where(ws > 0.0, zs, 1e6), axis=1), axis=1, keepdims=True)
        z_max = jnp.max(jnp.max(jnp.where(ws > 0.0, zs, -1e6), axis=1), axis=1, keepdims=True)
        lane = lax.broadcasted_iota(jnp.int32, (GROUPS, 128), 1)
        chunk = lane.astype(F32) * 2.0
        even = jnp.full((GROUPS, 128), float(DUMMY), F32)
        odd = even
        total = jnp.zeros((GROUPS, 1), F32)
        lane8 = lax.broadcasted_iota(jnp.int32, (8, 128), 1)
        rows_ref[DUMMY] = jnp.zeros((8, 128), F32)
        for d in (8, 3, 4, 1, 6, 0, 2, 5, 7):
            if d < 8:

                @pl.when(present(*DIRS[d]))
                def _():
                    copy(7 - d).wait_recv()

            src = lists_ref.at[8] if d == 8 else got_ref.at[d]
            z_row = jnp.where(src[3:4, :] > 0.0, src[2:3, :], 2e6)
            low = jnp.sum(jnp.where(z_row < z_min - float(REACH), 1.0, 0.0), axis=1, keepdims=True)
            high = jnp.sum(jnp.where(z_row <= z_max + float(REACH), 1.0, 0.0), axis=1, keepdims=True)
            first = jnp.floor(low * (1.0 / STEP))
            count = jnp.where(high > low, jnp.floor((high - STEP * first + 31.0) * (1.0 / 32.0)), 0.0)
            at = chunk - total
            even = jnp.where((at >= 0.0) & (at < count), at * 2.0 + (first + float(ROWS * d)), even)
            at = at + 1.0
            odd = jnp.where((at >= 0.0) & (at < count), at * 2.0 + (first + float(ROWS * d)), odd)
            total = total + count
            parts = []
            for t in range(4):
                block = src[:, 128 * t : 128 * t + 128]
                block = jnp.concatenate([block, block], axis=0)
                for k in range(4):
                    part = block if k == 0 else pltpu.roll(block, 128 - 32 * k, 1)
                    part = jnp.where(lane8 < 32, part, pltpu.roll(part, 32, 1))
                    part = jnp.where(lane8 < 64, part, pltpu.roll(part, 64, 1))
                    parts.append(part)
            turned = [pltpu.roll(part, 16, 1) for part in parts] + [jnp.zeros((8, 128), F32)]
            for k in range(16):
                rows_ref[ROWS * d + 2 * k] = parts[k]
                rows_ref[ROWS * d + 2 * k + 1] = jnp.where((lane8 & 31) < 16, turned[k], turned[k + 1])
        units = jnp.floor((total + 1.0) * 0.5)
        name = lax.broadcasted_iota(jnp.int32, (GROUPS, 128), 0).astype(F32)
        number = jnp.sum(jnp.where((name >= begin) & (name < end), units, 0.0), axis=0, keepdims=True)
        turns = jnp.floor((number + 3.0) * 0.25)
        extra = 4.0 * turns - number
        units = units + jnp.sum(jnp.where(name == end - 1.0, extra, 0.0), axis=1, keepdims=True)
        skip = 4.0 * EARLY
        other = lane.astype(F32)
        units_row = jnp.sum(jnp.where(name == other, units, 0.0), axis=0, keepdims=True)
        origin = jnp.zeros((GROUPS, 1), F32)
        for r in range(SUBREGIONS):
            origin = jnp.where(name[:, 0:1] >= starts[r], starts[r], origin)
        passed = jnp.sum(jnp.where((other < name) & (other >= origin), units_row, 0.0), axis=1, keepdims=True)
        hit = (name >= begin) & (name < end) & (passed <= skip) & (skip < passed + units)
        found = jnp.sum(jnp.where(hit, 1.0, 0.0), axis=0, keepdims=True)
        start_g = jnp.sum(jnp.where(hit, name, 0.0), axis=0, keepdims=True)
        start_b = jnp.sum(jnp.where(hit, skip - passed, 0.0), axis=0, keepdims=True)
        real = lane_row < SUBREGIONS
        late = jnp.where(real, jnp.maximum(turns - EARLY, 1.0), float(1 << 18))
        start_g = jnp.where(found > 0.0, start_g, float(GROUPS))
        open_g = jnp.where(real & (begin < end), begin, float(GROUPS))
        table = jnp.where(lane == 127, units, even + 512.0 * odd)
        idle = jnp.where(lane_row == 127, float(1 << 20), float(DUMMY * 513))
        tail = [idle, late, start_g, start_b, open_g, end, jnp.zeros((2, 128), F32)]
        table_ref[...] = jnp.concatenate([table] + tail, axis=0).astype(jnp.int32)
        for d, (da, db) in enumerate(DIRS):

            @pl.when(present(da, db))
            def _():
                copy(d).wait_send()

    pl.run_scoped(
        body,
        pltpu.ACC(0)((16, 256), F32),
        pltpu.ACC(1)((16, 256), F32),
        pltpu.ACC(0)((16, 256), F32),
        pltpu.ACC(1)((16, 256), F32),
        pltpu.ACC(0)((GROUPS * 16, 256), F32),
        pltpu.ACC(1)((GROUPS * 16, 256), F32),
    )


def send_call(coords, weights, live):
    far = pl.BlockSpec(memory_space=pltpu.HBM)
    return pl.pallas_call(
        send_kernel,
        out_shape=(
            jax.ShapeDtypeStruct((GROUPS + 8, 128), jnp.int32),
            jax.ShapeDtypeStruct((DUMMY + 1, 8, 128), F32),
            jax.ShapeDtypeStruct((4, GROUPS, 8, 128), F32),
        ),
        in_specs=[far] * 3,
        out_specs=[pl.BlockSpec(memory_space=pltpu.VMEM)] * 3,
        scratch_shapes=[
            pltpu.VMEM((3, 1, 1, PART_DEV), jnp.int32),
            pltpu.VMEM((1, 1, PART_DEV), BF16),
            pltpu.VMEM((1, 1), jnp.int32),
            pltpu.VMEM((9, 4, PART_DEV), F32),
            pltpu.VMEM((8, 4, PART_DEV), F32),
            pltpu.SemaphoreType.DMA((3,)),
            pltpu.SemaphoreType.DMA((8,)),
            pltpu.SemaphoreType.DMA((8,)),
        ],
        compiler_params=pltpu.CompilerParams(collective_id=0, has_side_effects=True, vmem_limit_bytes=12 << 20),
    )(*[pltpu.with_memory_space_constraint(v, pltpu.HBM) for v in (coords, weights)], live)


LOG_SCALE = (S_BINS / 4.0) / math.log2(10.0)
LOG_BASE = -4.515457845
LEVELS_U = 24
LEVELS_V = 25
V_ROWS = 208
BINS = (2, TILES, 16, 128)
ENGINE = (
    ((2, 256, 128 * TILES), BF16),
    ((2, V_ROWS, 128 * TILES), BF16),
    (BINS, BF16),
    (BINS, BF16),
    (BINS, BF16),
    ((2, 2, 16, 128), BF16),
)


def engine(table_sm, rows_ref, own_ref, hot_u, hot_v, bin_u, bin_v, far_w, own_w):
    zero = jnp.zeros((16, 128), BF16)
    for half in range(2):
        hot_u[half, 8 * LEVELS_U :, :] = jnp.zeros((256 - 8 * LEVELS_U, 128 * TILES), BF16)

    def index(state, advance):
        for half in range(2):
            for mxu in range(2):
                g, b = state[0], state[1]
                group = jnp.minimum(g, GROUPS - 1)
                xi, yi, zi, wi = own_ref[0, group], own_ref[1, group], own_ref[2, group], own_ref[3, group]
                own_w[half, mxu] = jnp.concatenate([wi, wi], axis=0).astype(BF16)
                pair = table_sm[g, b]
                for t, row in ((2 * mxu, pair & 511), (2 * mxu + 1, pair >> 9)):
                    dx = xi - rows_ref[row, 0:1, :]
                    dy = yi - rows_ref[row, 1:2, :]
                    dz = zi - rows_ref[row, 2:3, :]
                    far_w[half, t] = jnp.broadcast_to(rows_ref[row, 3:4, :].astype(BF16), (16, 128))
                    dx2 = dx * dx
                    q = dx2 + dy * dy + dz * dz
                    s = jnp.floor(jnp.log2(q + 0.48) * LOG_SCALE + LOG_BASE)
                    near = jnp.floor(jnp.abs(dx) * lax.rsqrt(q) * float(MU_BINS) + 0.5)
                    mu = jnp.where(near * near * q > dx2 * float(MU_BINS * MU_BINS), near - 1.0, near)
                    c = s * float(MU_BINS) + jnp.minimum(mu, MU_BINS - 1.0)
                    u = jnp.floor(c * (1.0 / LEVELS_V) + 0.01)
                    v = c - u * float(LEVELS_V)
                    bin_u[half, t] = jnp.concatenate([u, u - 1.0], axis=0).astype(BF16)
                    bin_v[half, t] = jnp.concatenate([v, v - 1.0], axis=0).astype(BF16)
                state = advance(*state)
        return state

    def fill(half):
        for t in range(TILES):
            u2, v2, w_far, w_own = bin_u[half, t], bin_v[half, t], far_w[half, t], own_w[half, t // 2]
            lanes = slice(128 * t, 128 * t + 128)
            for k in range(LEVELS_U // 2):
                hot_u[half, 16 * k : 16 * k + 16, lanes] = jnp.where(u2 == jnp.bfloat16(2 * k), w_far, zero)
            for k in range(V_ROWS // 16):
                hot_v[half, 16 * k : 16 * k + 16, lanes] = jnp.where(v2 == jnp.bfloat16(2 * k), w_own, zero)

    def push(half):
        for mxu in range(2):
            pltpu.matmul_push_rhs(hot_u[half, :, 256 * mxu : 256 * mxu + 256], staging_register=half, mxu_index=mxu, transpose=True)

    def multiply(half, accs):
        for mxu in range(2):
            pltpu.matmul_acc_lhs(accs[mxu], hot_v[half, :, 256 * mxu : 256 * mxu + 256], load_staged_rhs=half)

    def run(state, advance, trips, sets, drain):
        state = index(state, advance)
        for half in range(2):
            fill(half)
            push(half)
        state = index(state, advance)
        for r in range(SUBREGIONS):

            def trip(_, state):
                for half in range(2):
                    multiply(half, sets[r % 2])
                for half in range(2):
                    fill(half)
                    push(half)
                return index(state, advance)

            state = lax.fori_loop(0, trips(r), trip, state)
            if r > 0:
                drain(r - 1, sets[(r - 1) % 2])
        last = sets[(SUBREGIONS - 1) % 2]
        for half in range(2):
            multiply(half, last)
        drain(SUBREGIONS - 1, last)

    return run


def count_kernel(table_ref, rows_ref, own_ref, out_ref, table_sm, sem):
    def body(a0, a1, b0, b1, *buffers):
        copy = pltpu.make_async_copy(table_ref, table_sm, sem)
        copy.start()
        for acc in (a0, a1, b0, b1):
            pltpu.matmul_pop(acc)
        run = engine(table_sm, rows_ref, own_ref, *buffers)
        copy.wait()

        def advance(g, b, left, region):
            over = b + 1 >= table_sm[g, 127]
            left = left - 1
            done = left <= 0
            region = jnp.where(done, jnp.minimum(region + 1, SUBREGIONS), region)
            b = jnp.where(done, table_sm[GROUPS + 3, region], jnp.where(over, 0, b + 1))
            g = jnp.where(done, table_sm[GROUPS + 2, region], jnp.where(over, g + 1, g))
            return g, b, jnp.where(done, 4 * table_sm[GROUPS + 1, region], left), region

        def drain(r, accs):
            out_ref[r] = pltpu.matmul_pop(accs[0]) + pltpu.matmul_pop(accs[1])

        state = (table_sm[GROUPS + 2, 0], table_sm[GROUPS + 3, 0], 4 * table_sm[GROUPS + 1, 0], jnp.int32(0))
        run(state, advance, lambda r: table_sm[GROUPS + 1, r], ((a0, a1), (b0, b1)), drain)

    pl.run_scoped(
        body,
        pltpu.ACC(0)((V_ROWS, 256), F32),
        pltpu.ACC(1)((V_ROWS, 256), F32),
        pltpu.ACC(0)((V_ROWS, 256), F32),
        pltpu.ACC(1)((V_ROWS, 256), F32),
        *(pltpu.VMEM(shape, dtype) for shape, dtype in ENGINE),
    )


def count_call(table, rows, own):
    vmem = pl.BlockSpec(memory_space=pltpu.VMEM)
    return pl.pallas_call(
        count_kernel,
        out_shape=jax.ShapeDtypeStruct((SUBREGIONS, V_ROWS, 256), F32),
        in_specs=[vmem, vmem, vmem],
        out_specs=vmem,
        scratch_shapes=[pltpu.SMEM((GROUPS + 8, 128), jnp.int32), pltpu.SemaphoreType.DMA],
        compiler_params=pltpu.CompilerParams(vmem_limit_bytes=6 << 20),
    )(table, rows, own)


def total_kernel(skies, counts_ref, table_ref, rows_ref, own_ref, packed_ref, total_ref, sum_ref, sent_ref, land_ref, table_sm, sem, send_sem, recv_sem):
    shell, sky = lax.axis_index("shell"), lax.axis_index("sky")
    barrier = pltpu.get_barrier_semaphore()
    load = pltpu.make_async_copy(table_ref, table_sm, sem)
    load.start()
    for k in range(1, skies):
        pl.semaphore_signal(barrier, inc=1, device_id=(shell, lax.rem(sky + k, skies)), device_id_type=MESH)

    def copy(k):
        return pltpu.make_async_remote_copy(
            src_ref=sent_ref,
            dst_ref=land_ref.at[k - 1],
            send_sem=send_sem.at[k - 1],
            recv_sem=recv_sem.at[k - 1],
            device_id=(shell, lax.rem(sky + k, skies)),
            device_id_type=MESH,
        )

    def body(a0, a1, b0, b1, small, large, *buffers):
        for acc in (a0, a1, b0, b1, small, large):
            pltpu.matmul_pop(acc)
        run = engine(table_sm, rows_ref, own_ref, *buffers)
        load.wait()

        def advance(g, b, left, region):
            over = b + 1 >= table_sm[g, 127]
            b = jnp.where(over, 0, b + 1)
            g = jnp.where(over, g + 1, g)
            g = jnp.where(g >= table_sm[GROUPS + 5, region], GROUPS, g)
            left = left - 1
            done = left <= 0
            region = jnp.where(done, jnp.minimum(region + 1, SUBREGIONS), region)
            g = jnp.where(done, table_sm[GROUPS + 4, region], g)
            return g, jnp.where(done, 0, b), jnp.where(done, 4 * EARLY, left), region

        def drain(r, accs):
            sum_ref[r] = counts_ref[r] + (pltpu.matmul_pop(accs[0]) + pltpu.matmul_pop(accs[1]))

        state = (table_sm[GROUPS + 4, 0], jnp.int32(0), jnp.int32(4 * EARLY), jnp.int32(0))
        run(state, advance, lambda r: EARLY, ((a0, a1), (b0, b1)), drain)

        lane_in = lax.broadcasted_iota(jnp.int32, (256, 256), 0) >> 3
        lane_out = lax.broadcasted_iota(jnp.int32, (256, 256), 1)
        diagonal = lax.broadcasted_iota(jnp.int32, (V_ROWS, 256), 0) & 7 == lax.broadcasted_iota(jnp.int32, (V_ROWS, 256), 1) & 7

        def folded(block):
            block = jnp.where(diagonal, block, 0.0).reshape(V_ROWS // 8, 8, 256)
            return jnp.concatenate([jnp.sum(block, axis=1), jnp.zeros((32 - V_ROWS // 8, 256), F32)], axis=0)

        def pack(blocks, acc):
            size = 8 * len(blocks)
            for k in range(4):
                rows = jnp.concatenate([block[8 * k : 8 * k + 8] for block in blocks], axis=0)
                high = rows.astype(BF16)
                rest = rows - high.astype(F32)
                middle = rest.astype(BF16)
                low = (rest - middle.astype(F32)).astype(BF16)
                parts = [high.astype(F32), middle.astype(F32), low.astype(F32)]
                if size == 8:
                    parts.append(jnp.zeros((8, 256), F32))
                pick = jnp.where(lane_in + 32 * k == lane_out, 1.0, 0.0).astype(BF16)
                pltpu.matmul_push_rhs(pick, staging_register=0, mxu_index=0)
                pltpu.matmul_acc_lhs(acc, jnp.concatenate(parts, axis=0).astype(BF16), load_staged_rhs=0)
            got = pltpu.matmul_pop(acc)
            return (got[0:size] + got[size : 2 * size] + got[2 * size : 3 * size])[:, 0:128]

        every = sum_ref[0]
        for r in range(1, SUBREGIONS):
            every = every + sum_ref[r]
        mine = pack([folded(every)], small)
        sent_ref[...] = mine
        pl.semaphore_wait(barrier, skies - 1)
        for k in range(1, skies):
            copy(k).start()
        packed_ref[...] = pack([folded(sum_ref[r]) for r in range(SUBREGIONS)], large)
        total = mine
        for k in range(1, skies):
            copy(k).wait_recv()
            total = total + land_ref[k - 1]
        total_ref[...] = total
        for k in range(1, skies):
            copy(k).wait_send()

    pl.run_scoped(
        body,
        pltpu.ACC(0)((V_ROWS, 256), F32),
        pltpu.ACC(1)((V_ROWS, 256), F32),
        pltpu.ACC(0)((V_ROWS, 256), F32),
        pltpu.ACC(1)((V_ROWS, 256), F32),
        pltpu.ACC(0)((32, 256), F32),
        pltpu.ACC(0)((24 * SUBREGIONS, 256), F32),
        *(pltpu.VMEM(shape, dtype) for shape, dtype in ENGINE),
    )


def total_call(counts, table, rows, own):
    skies = lax.axis_size("sky")
    vmem = pl.BlockSpec(memory_space=pltpu.VMEM)
    return pl.pallas_call(
        functools.partial(total_kernel, skies),
        out_shape=(jax.ShapeDtypeStruct((8 * SUBREGIONS, 128), F32), jax.ShapeDtypeStruct((8, 128), F32)),
        in_specs=[vmem] * 4,
        out_specs=(vmem, vmem),
        scratch_shapes=[
            pltpu.VMEM((SUBREGIONS, V_ROWS, 256), F32),
            pltpu.VMEM((8, 128), F32),
            pltpu.VMEM((skies - 1, 8, 128), F32),
            pltpu.SMEM((GROUPS + 8, 128), jnp.int32),
            pltpu.SemaphoreType.DMA,
            pltpu.SemaphoreType.DMA((skies - 1,)),
            pltpu.SemaphoreType.DMA((skies - 1,)),
        ],
        compiler_params=pltpu.CompilerParams(collective_id=1, has_side_effects=True, vmem_limit_bytes=10 << 20),
    )(counts, table, rows, own)


def edge_values():
    return [int(4.0 * 10.0 ** (4.0 * level / S_BINS) + 0.5) for level in range(S_BINS + 1)]


def bin_scale(patches):
    edges = edge_values()
    factor = SIDE_CELLS * SIDE_CELLS * SPAN_CELLS / (patches * PART_DEV * PART_DEV)
    values = []
    for level in range(S_BINS):
        volume = 4.0 * math.pi / 3.0 * (edges[level + 1] ** 1.5 - edges[level] ** 1.5) / MU_BINS
        values = values + [factor / volume] * MU_BINS
    return jnp.asarray(values, dtype=F32)


def unpacked(x):
    x = x.reshape(-1, 8, 4, 32).transpose(0, 3, 2, 1).reshape(-1, 32, 32)
    return x[:, :LEVELS_U, :LEVELS_V].reshape(-1, S_BINS * MU_BINS)


def local(coords, weights, live):
    tables = send_call(coords, weights, live)
    packed, total = total_call(count_call(*tables), *tables)
    leave = total[None] - packed.reshape(SUBREGIONS, 8, 128)
    return (unpacked(leave) * bin_scale(lax.axis_size("sky"))[None, :])[None]


def solution(mesh):
    in_specs = (P(None, "shell", "sky", None), P("shell", "sky", None), P("shell", "sky"))
    out_specs = P("shell", "sky", None)
    return jax.shard_map(local, mesh=mesh, in_specs=in_specs, out_specs=out_specs, check_vma=False)
```

```python
import functools, math
import jax, jax.numpy as jnp
from jax import lax
from jax.experimental import pallas as pl
from jax.experimental.pallas import tpu as pltpu
from jax.sharding import PartitionSpec as P

PART_DEV = 512
SIDE_CELLS = 256
SPAN_CELLS = 1024
SUBREGIONS = 8
S_BINS = 30
MU_BINS = 20
REACH = 199
EARLY = 3
GROUPS = 24
STEP = 16
ROWS = PART_DEV // STEP
DUMMY = 9 * ROWS
TILES = 4
DIRS = tuple((da, db) for da in (-1, 0, 1) for db in (-1, 0, 1) if (da, db) != (0, 0))
ORDER = (0, 2, 5, 7, 3, 4, 1, 6)
MESH = pl.DeviceIdType.MESH
F32 = jnp.float32
BF16 = jnp.bfloat16


def send_kernel(coords_hbm, weight_hbm, live_hbm, table_ref, rows_ref, own_ref, coords_ref, weight_ref, live_ref, lists_ref, got_ref, load_sem, send_sem, recv_sem):
    shell, sky = lax.axis_index("shell"), lax.axis_index("sky")
    shells, skies = lax.axis_size("shell"), lax.axis_size("sky")
    barrier = pltpu.get_barrier_semaphore()
    loads = [
        pltpu.make_async_copy(src, dst, load_sem.at[k])
        for k, (src, dst) in enumerate(((coords_hbm, coords_ref), (weight_hbm, weight_ref), (live_hbm, live_ref)))
    ]
    for load in loads:
        load.start()

    def present(da, db):
        a, b = shell + da, sky + db
        return (a >= 0) & (a < shells) & (b >= 0) & (b < skies)

    for da, db in DIRS:

        @pl.when(present(da, db))
        def _():
            pl.semaphore_signal(barrier, inc=1, device_id=(shell + da, sky + db), device_id_type=MESH)

    for d, (da, db) in enumerate(DIRS):

        @pl.when(jnp.logical_not(present(da, db)))
        def _():
            got_ref[d] = jnp.zeros((4, PART_DEV), F32)

    def copy(d):
        da, db = DIRS[d]
        return pltpu.make_async_remote_copy(
            src_ref=lists_ref.at[d],
            dst_ref=got_ref.at[7 - d],
            send_sem=send_sem.at[d],
            recv_sem=recv_sem.at[7 - d],
            device_id=(shell + da, sky + db),
            device_id_type=MESH,
        )

    def body(acc0, acc1, acc2, acc3, tall0, tall1):
        for acc in (acc0, acc1, acc2, acc3, tall0, tall1):
            pltpu.matmul_pop(acc)
        for load in loads:
            load.wait()
        n = PART_DEV
        x = (coords_ref[0, 0] & (SIDE_CELLS - 1)).astype(F32)
        y = (coords_ref[1, 0] & (SIDE_CELLS - 1)).astype(F32)
        zi = coords_ref[2, 0]
        region = zi >> 7
        z_high = region.astype(F32)
        z_low = (zi & 127).astype(F32)
        slot = lax.broadcasted_iota(jnp.int32, (1, n), 1)
        alive = slot < live_ref[...]
        w = jnp.where(alive, weight_ref[0].astype(F32), 0.0)
        key = (jnp.where(alive, zi * n, SPAN_CELLS * n) + slot).astype(F32)
        key_column = jnp.transpose(jnp.broadcast_to(key, (128, n)))[:, 0:1]
        before = jnp.where(key_column < key, 1.0, 0.0).astype(BF16)
        valid = []
        for da, db in DIRS:
            ok = alive
            if da > 0:
                ok = ok & (x >= SIDE_CELLS - REACH)
            if da < 0:
                ok = ok & (x <= REACH - 1)
            if db > 0:
                ok = ok & (y >= SIDE_CELLS - REACH)
            if db < 0:
                ok = ok & (y <= REACH - 1)
            valid.append(ok)
        valid.append(alive)
        ones = [jnp.where(ok, 1.0, 0.0) for ok in valid]
        flags = jnp.concatenate(ones + [jnp.zeros((7, n), F32)], axis=0).astype(BF16)
        for half in range(2):
            rows = slice(256 * half, 256 * half + 256)
            pltpu.matmul_push_rhs(before[rows, 0:256], staging_register=0, mxu_index=0)
            pltpu.matmul_acc_lhs(acc0, flags[:, rows], load_staged_rhs=0)
            pltpu.matmul_push_rhs(before[rows, 256:512], staging_register=0, mxu_index=1)
            pltpu.matmul_acc_lhs(acc1, flags[:, rows], load_staged_rhs=0)
        rank = jnp.concatenate([pltpu.matmul_pop(acc0), pltpu.matmul_pop(acc1)], axis=1)
        attrs = jnp.concatenate([x, y, z_high, z_low, w, jnp.zeros((11, n), F32)], axis=0).astype(BF16)
        place = lax.broadcasted_iota(jnp.int32, (256, n), 0).astype(F32).astype(BF16)
        one, zero = jnp.ones((256, n), BF16), jnp.zeros((256, n), BF16)
        accs = ((acc0, acc1), (acc2, acc3))
        beside_shell = 1 + (shell > 0).astype(jnp.int32) + (shell < shells - 1).astype(jnp.int32)
        beside_sky = 1 + (sky > 0).astype(jnp.int32) + (sky < skies - 1).astype(jnp.int32)

        def build(d, slot):
            target = jnp.where(valid[d], rank[d : d + 1, :], -1.0)
            pair = accs[slot % 2]
            for mxu in range(2):
                near = jnp.broadcast_to((target - 256.0 * mxu).astype(BF16), (256, n))
                hot = jnp.where(place == near, one, zero)
                for half in range(2):
                    cols = slice(256 * half, 256 * half + 256)
                    pltpu.matmul_push_rhs(hot[:, cols], staging_register=0, mxu_index=mxu, transpose=True)
                    pltpu.matmul_acc_lhs(pair[mxu], attrs[:, cols], load_staged_rhs=0)
            da, db = DIRS[d] if d < 8 else (0, 0)
            for mxu in range(2):
                got = pltpu.matmul_pop(pair[mxu])
                lanes = slice(256 * mxu, 256 * mxu + 256)
                lists_ref[d, 0:1, lanes] = got[0:1] - float(SIDE_CELLS * da)
                lists_ref[d, 1:2, lanes] = got[1:2] - float(SIDE_CELLS * db)
                lists_ref[d, 2:3, lanes] = got[2:3] * 128.0 + got[3:4]
                lists_ref[d, 3:4, lanes] = got[4:5]

        for slot, d in enumerate(ORDER):
            build(d, slot)
        pl.semaphore_wait(barrier, beside_shell * beside_sky - 1)
        for d in ORDER:

            @pl.when(present(*DIRS[d]))
            def _():
                copy(d).start()

        build(8, 0)
        shift = jnp.zeros((1, n), F32)
        first = jnp.zeros((1, 1), F32)
        group = jnp.zeros((1, 1), F32)
        starts = []
        for r in range(SUBREGIONS):
            here = alive & (region == r)
            starts.append(group)
            shift = jnp.where(here, 32.0 * group - first, shift)
            count = jnp.sum(jnp.where(here, 1.0, 0.0), axis=1, keepdims=True)
            first = first + count
            group = group + jnp.floor((count + 31.0) * (1.0 / 32.0))
        starts = starts + [group]
        lane_row = lax.broadcasted_iota(jnp.int32, (1, 128), 1)
        begin, end = jnp.zeros((1, 128), F32), jnp.zeros((1, 128), F32)
        for r in range(SUBREGIONS):
            begin = jnp.where(lane_row == r, starts[r], begin)
            end = jnp.where(lane_row == r, starts[r + 1], end)
        target = jnp.where(alive, rank[8:9, :] + shift, -1.0)
        wide = lax.broadcasted_iota(jnp.int32, (GROUPS * 32, 1), 0).astype(F32)
        hot = jnp.where(wide == target, 1.0, 0.0).astype(BF16)
        rhs = jnp.concatenate([attrs, jnp.zeros((240, n), BF16)], axis=0)
        half_rows = GROUPS * 16
        for half in range(2):
            cols = slice(256 * half, 256 * half + 256)
            for mxu, acc in ((0, tall0), (1, tall1)):
                pltpu.matmul_push_rhs(rhs[:, cols], staging_register=0, mxu_index=mxu, transpose=True)
                pltpu.matmul_acc_lhs(acc, hot[half_rows * mxu : half_rows * mxu + half_rows, cols], load_staged_rhs=0)
        quarter = lax.broadcasted_iota(jnp.int32, (8, 128), 1) // 32
        for mxu, acc in ((0, tall0), (1, tall1)):
            got = pltpu.matmul_pop(acc)[:, 0:128]
            for g in range(GROUPS // 2):
                parts = []
                for q in range(4):
                    block = got[32 * g + 8 * q : 32 * g + 8 * q + 8]
                    deep = block[:, 2:3] * 128.0 + block[:, 3:4]
                    parts.append([jnp.broadcast_to(v, (8, 128)) for v in (block[:, 0:1], block[:, 1:2], deep, block[:, 4:5])])
                for k in range(4):
                    value = parts[0][k]
                    for q in range(1, 4):
                        value = jnp.where(quarter == q, parts[q][k], value)
                    own_ref[k, mxu * (GROUPS // 2) + g] = value

        zs, ws = own_ref[2], own_ref[3]
        z_min = jnp.min(jnp.min(jnp.where(ws > 0.0, zs, 1e6), axis=1), axis=1, keepdims=True)
        z_max = jnp.max(jnp.max(jnp.where(ws > 0.0, zs, -1e6), axis=1), axis=1, keepdims=True)
        lane = lax.broadcasted_iota(jnp.int32, (GROUPS, 128), 1)
        chunk = lane.astype(F32) * 2.0
        even = jnp.full((GROUPS, 128), float(DUMMY), F32)
        odd = even
        total = jnp.zeros((GROUPS, 1), F32)
        lane8 = lax.broadcasted_iota(jnp.int32, (8, 128), 1)
        rows_ref[DUMMY] = jnp.zeros((8, 128), F32)
        for d in (8, 1, 6, 3, 4, 0, 2, 5, 7):
            if d < 8:

                @pl.when(present(*DIRS[d]))
                def _():
                    copy(7 - d).wait_recv()

            src = lists_ref.at[8] if d == 8 else got_ref.at[d]
            z_row = jnp.where(src[3:4, :] > 0.0, src[2:3, :], 2e6)
            low = jnp.sum(jnp.where(z_row < z_min - float(REACH), 1.0, 0.0), axis=1, keepdims=True)
            high = jnp.sum(jnp.where(z_row <= z_max + float(REACH), 1.0, 0.0), axis=1, keepdims=True)
            first = jnp.floor(low * (1.0 / STEP))
            count = jnp.where(high > low, jnp.floor((high - STEP * first + 31.0) * (1.0 / 32.0)), 0.0)
            at = chunk - total
            even = jnp.where((at >= 0.0) & (at < count), at * 2.0 + (first + float(ROWS * d)), even)
            at = at + 1.0
            odd = jnp.where((at >= 0.0) & (at < count), at * 2.0 + (first + float(ROWS * d)), odd)
            total = total + count
            parts = []
            for t in range(4):
                block = src[:, 128 * t : 128 * t + 128]
                block = jnp.concatenate([block, block], axis=0)
                for k in range(4):
                    part = block if k == 0 else pltpu.roll(block, 128 - 32 * k, 1)
                    part = jnp.where(lane8 < 32, part, pltpu.roll(part, 32, 1))
                    part = jnp.where(lane8 < 64, part, pltpu.roll(part, 64, 1))
                    parts.append(part)
            turned = [pltpu.roll(part, 16, 1) for part in parts] + [jnp.zeros((8, 128), F32)]
            for k in range(16):
                rows_ref[ROWS * d + 2 * k] = parts[k]
                rows_ref[ROWS * d + 2 * k + 1] = jnp.where((lane8 & 31) < 16, turned[k], turned[k + 1])
        units = jnp.floor((total + 1.0) * 0.5)
        name = lax.broadcasted_iota(jnp.int32, (GROUPS, 128), 0).astype(F32)
        number = jnp.sum(jnp.where((name >= begin) & (name < end), units, 0.0), axis=0, keepdims=True)
        turns = jnp.floor((number + 3.0) * 0.25)
        extra = 4.0 * turns - number
        units = units + jnp.sum(jnp.where(name == end - 1.0, extra, 0.0), axis=1, keepdims=True)
        skip = 4.0 * EARLY
        other = lane.astype(F32)
        units_row = jnp.sum(jnp.where(name == other, units, 0.0), axis=0, keepdims=True)
        origin = jnp.zeros((GROUPS, 1), F32)
        for r in range(SUBREGIONS):
            origin = jnp.where(name[:, 0:1] >= starts[r], starts[r], origin)
        passed = jnp.sum(jnp.where((other < name) & (other >= origin), units_row, 0.0), axis=1, keepdims=True)
        hit = (name >= begin) & (name < end) & (passed <= skip) & (skip < passed + units)
        found = jnp.sum(jnp.where(hit, 1.0, 0.0), axis=0, keepdims=True)
        start_g = jnp.sum(jnp.where(hit, name, 0.0), axis=0, keepdims=True)
        start_b = jnp.sum(jnp.where(hit, skip - passed, 0.0), axis=0, keepdims=True)
        real = lane_row < SUBREGIONS
        late = jnp.where(real, jnp.maximum(turns - EARLY, 1.0), float(1 << 18))
        start_g = jnp.where(found > 0.0, start_g, float(GROUPS))
        open_g = jnp.where(real & (begin < end), begin, float(GROUPS))
        table = jnp.where(lane == 127, units, even + 512.0 * odd)
        idle = jnp.where(lane_row == 127, float(1 << 20), float(DUMMY * 513))
        tail = [idle, late, start_g, start_b, open_g, end, jnp.zeros((2, 128), F32)]
        table_ref[...] = jnp.concatenate([table] + tail, axis=0).astype(jnp.int32)
        for d, (da, db) in enumerate(DIRS):

            @pl.when(present(da, db))
            def _():
                copy(d).wait_send()

    pl.run_scoped(
        body,
        pltpu.ACC(0)((16, 256), F32),
        pltpu.ACC(1)((16, 256), F32),
        pltpu.ACC(0)((16, 256), F32),
        pltpu.ACC(1)((16, 256), F32),
        pltpu.ACC(0)((GROUPS * 16, 256), F32),
        pltpu.ACC(1)((GROUPS * 16, 256), F32),
    )


def send_call(coords, weights, live):
    far = pl.BlockSpec(memory_space=pltpu.HBM)
    return pl.pallas_call(
        send_kernel,
        out_shape=(
            jax.ShapeDtypeStruct((GROUPS + 8, 128), jnp.int32),
            jax.ShapeDtypeStruct((DUMMY + 1, 8, 128), F32),
            jax.ShapeDtypeStruct((4, GROUPS, 8, 128), F32),
        ),
        in_specs=[far] * 3,
        out_specs=[pl.BlockSpec(memory_space=pltpu.VMEM)] * 3,
        scratch_shapes=[
            pltpu.VMEM((3, 1, 1, PART_DEV), jnp.int32),
            pltpu.VMEM((1, 1, PART_DEV), BF16),
            pltpu.VMEM((1, 1), jnp.int32),
            pltpu.VMEM((9, 4, PART_DEV), F32),
            pltpu.VMEM((8, 4, PART_DEV), F32),
            pltpu.SemaphoreType.DMA((3,)),
            pltpu.SemaphoreType.DMA((8,)),
            pltpu.SemaphoreType.DMA((8,)),
        ],
        compiler_params=pltpu.CompilerParams(collective_id=0, has_side_effects=True, vmem_limit_bytes=12 << 20),
    )(*[pltpu.with_memory_space_constraint(v, pltpu.HBM) for v in (coords, weights)], live)


LOG_SCALE = (S_BINS / 4.0) / math.log2(10.0)
LOG_BASE = -4.515457845
LEVELS_U = 24
LEVELS_V = 25
V_ROWS = 208
BINS = (2, TILES, 16, 128)
ENGINE = (
    ((2, 256, 128 * TILES), BF16),
    ((2, V_ROWS, 128 * TILES), BF16),
    (BINS, BF16),
    (BINS, BF16),
    (BINS, BF16),
    ((2, 2, 16, 128), BF16),
)


def engine(table_sm, rows_ref, own_ref, hot_u, hot_v, bin_u, bin_v, far_w, own_w):
    zero = jnp.zeros((16, 128), BF16)
    for half in range(2):
        hot_u[half, 8 * LEVELS_U :, :] = jnp.zeros((256 - 8 * LEVELS_U, 128 * TILES), BF16)

    def index(state, advance):
        for half in range(2):
            for mxu in range(2):
                g, b = state[0], state[1]
                group = jnp.minimum(g, GROUPS - 1)
                xi, yi, zi, wi = own_ref[0, group], own_ref[1, group], own_ref[2, group], own_ref[3, group]
                own_w[half, mxu] = jnp.concatenate([wi, wi], axis=0).astype(BF16)
                pair = table_sm[g, b]
                for t, row in ((2 * mxu, pair & 511), (2 * mxu + 1, pair >> 9)):
                    dx = xi - rows_ref[row, 0:1, :]
                    dy = yi - rows_ref[row, 1:2, :]
                    dz = zi - rows_ref[row, 2:3, :]
                    far_w[half, t] = jnp.broadcast_to(rows_ref[row, 3:4, :].astype(BF16), (16, 128))
                    dx2 = dx * dx
                    q = dx2 + dy * dy + dz * dz
                    s = jnp.floor(jnp.log2(q + 0.48) * LOG_SCALE + LOG_BASE)
                    near = jnp.floor(jnp.abs(dx) * lax.rsqrt(q) * float(MU_BINS) + 0.5)
                    mu = jnp.where(near * near * q > dx2 * float(MU_BINS * MU_BINS), near - 1.0, near)
                    c = s * float(MU_BINS) + jnp.minimum(mu, MU_BINS - 1.0)
                    u = jnp.floor(c * (1.0 / LEVELS_V) + 0.01)
                    v = c - u * float(LEVELS_V)
                    bin_u[half, t] = jnp.concatenate([u, u - 1.0], axis=0).astype(BF16)
                    bin_v[half, t] = jnp.concatenate([v, v - 1.0], axis=0).astype(BF16)
                state = advance(*state)
        return state

    def fill(half):
        for t in range(TILES):
            u2, v2, w_far, w_own = bin_u[half, t], bin_v[half, t], far_w[half, t], own_w[half, t // 2]
            lanes = slice(128 * t, 128 * t + 128)
            for k in range(LEVELS_U // 2):
                hot_u[half, 16 * k : 16 * k + 16, lanes] = jnp.where(u2 == jnp.bfloat16(2 * k), w_far, zero)
            for k in range(V_ROWS // 16):
                hot_v[half, 16 * k : 16 * k + 16, lanes] = jnp.where(v2 == jnp.bfloat16(2 * k), w_own, zero)

    def push(half):
        for mxu in range(2):
            pltpu.matmul_push_rhs(hot_u[half, :, 256 * mxu : 256 * mxu + 256], staging_register=half, mxu_index=mxu, transpose=True)

    def multiply(half, accs):
        for mxu in range(2):
            pltpu.matmul_acc_lhs(accs[mxu], hot_v[half, :, 256 * mxu : 256 * mxu + 256], load_staged_rhs=half)

    def run(state, advance, trips, sets, drain):
        state = index(state, advance)
        for half in range(2):
            fill(half)
            push(half)
        state = index(state, advance)
        for r in range(SUBREGIONS):

            def trip(_, state):
                for half in range(2):
                    multiply(half, sets[r % 2])
                for half in range(2):
                    fill(half)
                    push(half)
                return index(state, advance)

            state = lax.fori_loop(0, trips(r), trip, state)
            if r > 0:
                drain(r - 1, sets[(r - 1) % 2])
        last = sets[(SUBREGIONS - 1) % 2]
        for half in range(2):
            multiply(half, last)
        drain(SUBREGIONS - 1, last)

    return run


def count_kernel(table_ref, rows_ref, own_ref, out_ref, table_sm, sem):
    def body(a0, a1, b0, b1, *buffers):
        copy = pltpu.make_async_copy(table_ref, table_sm, sem)
        copy.start()
        for acc in (a0, a1, b0, b1):
            pltpu.matmul_pop(acc)
        run = engine(table_sm, rows_ref, own_ref, *buffers)
        copy.wait()

        def advance(g, b, left, region):
            over = b + 1 >= table_sm[g, 127]
            left = left - 1
            done = left <= 0
            region = jnp.where(done, jnp.minimum(region + 1, SUBREGIONS), region)
            b = jnp.where(done, table_sm[GROUPS + 3, region], jnp.where(over, 0, b + 1))
            g = jnp.where(done, table_sm[GROUPS + 2, region], jnp.where(over, g + 1, g))
            return g, b, jnp.where(done, 4 * table_sm[GROUPS + 1, region], left), region

        def drain(r, accs):
            out_ref[r] = pltpu.matmul_pop(accs[0]) + pltpu.matmul_pop(accs[1])

        state = (table_sm[GROUPS + 2, 0], table_sm[GROUPS + 3, 0], 4 * table_sm[GROUPS + 1, 0], jnp.int32(0))
        run(state, advance, lambda r: table_sm[GROUPS + 1, r], ((a0, a1), (b0, b1)), drain)

    pl.run_scoped(
        body,
        pltpu.ACC(0)((V_ROWS, 256), F32),
        pltpu.ACC(1)((V_ROWS, 256), F32),
        pltpu.ACC(0)((V_ROWS, 256), F32),
        pltpu.ACC(1)((V_ROWS, 256), F32),
        *(pltpu.VMEM(shape, dtype) for shape, dtype in ENGINE),
    )


def count_call(table, rows, own):
    vmem = pl.BlockSpec(memory_space=pltpu.VMEM)
    return pl.pallas_call(
        count_kernel,
        out_shape=jax.ShapeDtypeStruct((SUBREGIONS, V_ROWS, 256), F32),
        in_specs=[vmem, vmem, vmem],
        out_specs=vmem,
        scratch_shapes=[pltpu.SMEM((GROUPS + 8, 128), jnp.int32), pltpu.SemaphoreType.DMA],
        compiler_params=pltpu.CompilerParams(vmem_limit_bytes=6 << 20),
    )(table, rows, own)


def total_kernel(skies, counts_ref, table_ref, rows_ref, own_ref, packed_ref, total_ref, sum_ref, sent_ref, land_ref, table_sm, sem, send_sem, recv_sem):
    shell, sky = lax.axis_index("shell"), lax.axis_index("sky")
    barrier = pltpu.get_barrier_semaphore()
    load = pltpu.make_async_copy(table_ref, table_sm, sem)
    load.start()
    for k in range(1, skies):
        pl.semaphore_signal(barrier, inc=1, device_id=(shell, lax.rem(sky + k, skies)), device_id_type=MESH)

    def copy(k):
        return pltpu.make_async_remote_copy(
            src_ref=sent_ref,
            dst_ref=land_ref.at[k - 1],
            send_sem=send_sem.at[k - 1],
            recv_sem=recv_sem.at[k - 1],
            device_id=(shell, lax.rem(sky + k, skies)),
            device_id_type=MESH,
        )

    def body(a0, a1, b0, b1, small, large, *buffers):
        for acc in (a0, a1, b0, b1, small, large):
            pltpu.matmul_pop(acc)
        run = engine(table_sm, rows_ref, own_ref, *buffers)
        load.wait()

        def advance(g, b, left, region):
            over = b + 1 >= table_sm[g, 127]
            b = jnp.where(over, 0, b + 1)
            g = jnp.where(over, g + 1, g)
            g = jnp.where(g >= table_sm[GROUPS + 5, region], GROUPS, g)
            left = left - 1
            done = left <= 0
            region = jnp.where(done, jnp.minimum(region + 1, SUBREGIONS), region)
            g = jnp.where(done, table_sm[GROUPS + 4, region], g)
            return g, jnp.where(done, 0, b), jnp.where(done, 4 * EARLY, left), region

        def drain(r, accs):
            sum_ref[r] = counts_ref[r] + (pltpu.matmul_pop(accs[0]) + pltpu.matmul_pop(accs[1]))

        state = (table_sm[GROUPS + 4, 0], jnp.int32(0), jnp.int32(4 * EARLY), jnp.int32(0))
        run(state, advance, lambda r: EARLY, ((a0, a1), (b0, b1)), drain)

        lane_in = lax.broadcasted_iota(jnp.int32, (256, 256), 0) >> 3
        lane_out = lax.broadcasted_iota(jnp.int32, (256, 256), 1)
        diagonal = lax.broadcasted_iota(jnp.int32, (V_ROWS, 256), 0) & 7 == lax.broadcasted_iota(jnp.int32, (V_ROWS, 256), 1) & 7

        def folded(block):
            block = jnp.where(diagonal, block, 0.0).reshape(V_ROWS // 8, 8, 256)
            return jnp.concatenate([jnp.sum(block, axis=1), jnp.zeros((32 - V_ROWS // 8, 256), F32)], axis=0)

        def pack(blocks, acc):
            size = 8 * len(blocks)
            for k in range(4):
                rows = jnp.concatenate([block[8 * k : 8 * k + 8] for block in blocks], axis=0)
                high = rows.astype(BF16)
                rest = rows - high.astype(F32)
                middle = rest.astype(BF16)
                low = (rest - middle.astype(F32)).astype(BF16)
                parts = [high.astype(F32), middle.astype(F32), low.astype(F32)]
                if size == 8:
                    parts.append(jnp.zeros((8, 256), F32))
                pick = jnp.where(lane_in + 32 * k == lane_out, 1.0, 0.0).astype(BF16)
                pltpu.matmul_push_rhs(pick, staging_register=0, mxu_index=0)
                pltpu.matmul_acc_lhs(acc, jnp.concatenate(parts, axis=0).astype(BF16), load_staged_rhs=0)
            got = pltpu.matmul_pop(acc)
            return (got[0:size] + got[size : 2 * size] + got[2 * size : 3 * size])[:, 0:128]

        every = sum_ref[0]
        for r in range(1, SUBREGIONS):
            every = every + sum_ref[r]
        mine = pack([folded(every)], small)
        sent_ref[...] = mine
        pl.semaphore_wait(barrier, skies - 1)
        for k in range(1, skies):
            copy(k).start()
        packed_ref[...] = pack([folded(sum_ref[r]) for r in range(SUBREGIONS)], large)
        total = mine
        for k in range(1, skies):
            copy(k).wait_recv()
            total = total + land_ref[k - 1]
        total_ref[...] = total
        for k in range(1, skies):
            copy(k).wait_send()

    pl.run_scoped(
        body,
        pltpu.ACC(0)((V_ROWS, 256), F32),
        pltpu.ACC(1)((V_ROWS, 256), F32),
        pltpu.ACC(0)((V_ROWS, 256), F32),
        pltpu.ACC(1)((V_ROWS, 256), F32),
        pltpu.ACC(0)((32, 256), F32),
        pltpu.ACC(0)((24 * SUBREGIONS, 256), F32),
        *(pltpu.VMEM(shape, dtype) for shape, dtype in ENGINE),
    )


def total_call(counts, table, rows, own):
    skies = lax.axis_size("sky")
    vmem = pl.BlockSpec(memory_space=pltpu.VMEM)
    return pl.pallas_call(
        functools.partial(total_kernel, skies),
        out_shape=(jax.ShapeDtypeStruct((8 * SUBREGIONS, 128), F32), jax.ShapeDtypeStruct((8, 128), F32)),
        in_specs=[vmem] * 4,
        out_specs=(vmem, vmem),
        scratch_shapes=[
            pltpu.VMEM((SUBREGIONS, V_ROWS, 256), F32),
            pltpu.VMEM((8, 128), F32),
            pltpu.VMEM((skies - 1, 8, 128), F32),
            pltpu.SMEM((GROUPS + 8, 128), jnp.int32),
            pltpu.SemaphoreType.DMA,
            pltpu.SemaphoreType.DMA((skies - 1,)),
            pltpu.SemaphoreType.DMA((skies - 1,)),
        ],
        compiler_params=pltpu.CompilerParams(collective_id=1, has_side_effects=True, vmem_limit_bytes=10 << 20),
    )(counts, table, rows, own)


def edge_values():
    return [int(4.0 * 10.0 ** (4.0 * level / S_BINS) + 0.5) for level in range(S_BINS + 1)]


def bin_scale(patches):
    edges = edge_values()
    factor = SIDE_CELLS * SIDE_CELLS * SPAN_CELLS / (patches * PART_DEV * PART_DEV)
    values = []
    for level in range(S_BINS):
        volume = 4.0 * math.pi / 3.0 * (edges[level + 1] ** 1.5 - edges[level] ** 1.5) / MU_BINS
        values = values + [factor / volume] * MU_BINS
    return jnp.asarray(values, dtype=F32)


def unpacked(x):
    x = x.reshape(-1, 8, 4, 32).transpose(0, 3, 2, 1).reshape(-1, 32, 32)
    return x[:, :LEVELS_U, :LEVELS_V].reshape(-1, S_BINS * MU_BINS)


def local(coords, weights, live):
    tables = send_call(coords, weights, live)
    packed, total = total_call(count_call(*tables), *tables)
    leave = total[None] - packed.reshape(SUBREGIONS, 8, 128)
    return (unpacked(leave) * bin_scale(lax.axis_size("sky"))[None, :])[None]


def solution(mesh):
    in_specs = (P(None, "shell", "sky", None), P("shell", "sky", None), P("shell", "sky"))
    out_specs = P("shell", "sky", None)
    return jax.shard_map(local, mesh=mesh, in_specs=in_specs, out_specs=out_specs, check_vma=False)
```

```python
import functools, math
import jax, jax.numpy as jnp
from jax import lax
from jax.experimental import pallas as pl
from jax.experimental.pallas import tpu as pltpu
from jax.sharding import PartitionSpec as P

PART_DEV = 512
SIDE_CELLS = 256
SPAN_CELLS = 1024
SUBREGIONS = 8
S_BINS = 30
MU_BINS = 20
REACH = 199
EARLY = 4
GROUPS = 24
STEP = 16
ROWS = PART_DEV // STEP
DUMMY = 9 * ROWS
TILES = 4
DIRS = tuple((da, db) for da in (-1, 0, 1) for db in (-1, 0, 1) if (da, db) != (0, 0))
ORDER = (0, 2, 5, 7, 3, 4, 1, 6)
MESH = pl.DeviceIdType.MESH
F32 = jnp.float32
BF16 = jnp.bfloat16


def send_kernel(coords_hbm, weight_hbm, live_hbm, table_ref, rows_ref, own_ref, coords_ref, weight_ref, live_ref, lists_ref, got_ref, load_sem, send_sem, recv_sem):
    shell, sky = lax.axis_index("shell"), lax.axis_index("sky")
    shells, skies = lax.axis_size("shell"), lax.axis_size("sky")
    barrier = pltpu.get_barrier_semaphore()
    loads = [
        pltpu.make_async_copy(src, dst, load_sem.at[k])
        for k, (src, dst) in enumerate(((coords_hbm, coords_ref), (weight_hbm, weight_ref), (live_hbm, live_ref)))
    ]
    for load in loads:
        load.start()

    def present(da, db):
        a, b = shell + da, sky + db
        return (a >= 0) & (a < shells) & (b >= 0) & (b < skies)

    for da, db in DIRS:

        @pl.when(present(da, db))
        def _():
            pl.semaphore_signal(barrier, inc=1, device_id=(shell + da, sky + db), device_id_type=MESH)

    for d, (da, db) in enumerate(DIRS):

        @pl.when(jnp.logical_not(present(da, db)))
        def _():
            got_ref[d] = jnp.zeros((4, PART_DEV), F32)

    def copy(d):
        da, db = DIRS[d]
        return pltpu.make_async_remote_copy(
            src_ref=lists_ref.at[d],
            dst_ref=got_ref.at[7 - d],
            send_sem=send_sem.at[d],
            recv_sem=recv_sem.at[7 - d],
            device_id=(shell + da, sky + db),
            device_id_type=MESH,
        )

    def body(acc0, acc1, acc2, acc3, tall0, tall1):
        for acc in (acc0, acc1, acc2, acc3, tall0, tall1):
            pltpu.matmul_pop(acc)
        for load in loads:
            load.wait()
        n = PART_DEV
        x = (coords_ref[0, 0] & (SIDE_CELLS - 1)).astype(F32)
        y = (coords_ref[1, 0] & (SIDE_CELLS - 1)).astype(F32)
        zi = coords_ref[2, 0]
        region = zi >> 7
        z_high = region.astype(F32)
        z_low = (zi & 127).astype(F32)
        slot = lax.broadcasted_iota(jnp.int32, (1, n), 1)
        alive = slot < live_ref[...]
        w = jnp.where(alive, weight_ref[0].astype(F32), 0.0)
        key = (jnp.where(alive, zi * n, SPAN_CELLS * n) + slot).astype(F32)
        key_column = jnp.transpose(jnp.broadcast_to(key, (128, n)))[:, 0:1]
        before = jnp.where(key_column < key, 1.0, 0.0).astype(BF16)
        valid = []
        for da, db in DIRS:
            ok = alive
            if da > 0:
                ok = ok & (x >= SIDE_CELLS - REACH)
            if da < 0:
                ok = ok & (x <= REACH - 1)
            if db > 0:
                ok = ok & (y >= SIDE_CELLS - REACH)
            if db < 0:
                ok = ok & (y <= REACH - 1)
            valid.append(ok)
        valid.append(alive)
        ones = [jnp.where(ok, 1.0, 0.0) for ok in valid]
        flags = jnp.concatenate(ones + [jnp.zeros((7, n), F32)], axis=0).astype(BF16)
        for half in range(2):
            rows = slice(256 * half, 256 * half + 256)
            pltpu.matmul_push_rhs(before[rows, 0:256], staging_register=0, mxu_index=0)
            pltpu.matmul_acc_lhs(acc0, flags[:, rows], load_staged_rhs=0)
            pltpu.matmul_push_rhs(before[rows, 256:512], staging_register=0, mxu_index=1)
            pltpu.matmul_acc_lhs(acc1, flags[:, rows], load_staged_rhs=0)
        rank = jnp.concatenate([pltpu.matmul_pop(acc0), pltpu.matmul_pop(acc1)], axis=1)
        attrs = jnp.concatenate([x, y, z_high, z_low, w, jnp.zeros((11, n), F32)], axis=0).astype(BF16)
        place = lax.broadcasted_iota(jnp.int32, (256, n), 0).astype(F32).astype(BF16)
        one, zero = jnp.ones((256, n), BF16), jnp.zeros((256, n), BF16)
        accs = ((acc0, acc1), (acc2, acc3))
        beside_shell = 1 + (shell > 0).astype(jnp.int32) + (shell < shells - 1).astype(jnp.int32)
        beside_sky = 1 + (sky > 0).astype(jnp.int32) + (sky < skies - 1).astype(jnp.int32)

        def build(d, slot):
            target = jnp.where(valid[d], rank[d : d + 1, :], -1.0)
            pair = accs[slot % 2]
            for mxu in range(2):
                near = jnp.broadcast_to((target - 256.0 * mxu).astype(BF16), (256, n))
                hot = jnp.where(place == near, one, zero)
                for half in range(2):
                    cols = slice(256 * half, 256 * half + 256)
                    pltpu.matmul_push_rhs(hot[:, cols], staging_register=0, mxu_index=mxu, transpose=True)
                    pltpu.matmul_acc_lhs(pair[mxu], attrs[:, cols], load_staged_rhs=0)
            da, db = DIRS[d] if d < 8 else (0, 0)
            for mxu in range(2):
                got = pltpu.matmul_pop(pair[mxu])
                lanes = slice(256 * mxu, 256 * mxu + 256)
                lists_ref[d, 0:1, lanes] = got[0:1] - float(SIDE_CELLS * da)
                lists_ref[d, 1:2, lanes] = got[1:2] - float(SIDE_CELLS * db)
                lists_ref[d, 2:3, lanes] = got[2:3] * 128.0 + got[3:4]
                lists_ref[d, 3:4, lanes] = got[4:5]

        for slot, d in enumerate(ORDER):
            build(d, slot)
        pl.semaphore_wait(barrier, beside_shell * beside_sky - 1)
        for d in ORDER:

            @pl.when(present(*DIRS[d]))
            def _():
                copy(d).start()

        build(8, 0)
        shift = jnp.zeros((1, n), F32)
        first = jnp.zeros((1, 1), F32)
        group = jnp.zeros((1, 1), F32)
        starts = []
        for r in range(SUBREGIONS):
            here = alive & (region == r)
            starts.append(group)
            shift = jnp.where(here, 32.0 * group - first, shift)
            count = jnp.sum(jnp.where(here, 1.0, 0.0), axis=1, keepdims=True)
            first = first + count
            group = group + jnp.floor((count + 31.0) * (1.0 / 32.0))
        starts = starts + [group]
        lane_row = lax.broadcasted_iota(jnp.int32, (1, 128), 1)
        begin, end = jnp.zeros((1, 128), F32), jnp.zeros((1, 128), F32)
        for r in range(SUBREGIONS):
            begin = jnp.where(lane_row == r, starts[r], begin)
            end = jnp.where(lane_row == r, starts[r + 1], end)
        target = jnp.where(alive, rank[8:9, :] + shift, -1.0)
        wide = lax.broadcasted_iota(jnp.int32, (GROUPS * 32, 1), 0).astype(F32)
        hot = jnp.where(wide == target, 1.0, 0.0).astype(BF16)
        rhs = jnp.concatenate([attrs, jnp.zeros((240, n), BF16)], axis=0)
        half_rows = GROUPS * 16
        for half in range(2):
            cols = slice(256 * half, 256 * half + 256)
            for mxu, acc in ((0, tall0), (1, tall1)):
                pltpu.matmul_push_rhs(rhs[:, cols], staging_register=0, mxu_index=mxu, transpose=True)
                pltpu.matmul_acc_lhs(acc, hot[half_rows * mxu : half_rows * mxu + half_rows, cols], load_staged_rhs=0)
        quarter = lax.broadcasted_iota(jnp.int32, (8, 128), 1) // 32
        for mxu, acc in ((0, tall0), (1, tall1)):
            got = pltpu.matmul_pop(acc)[:, 0:128]
            for g in range(GROUPS // 2):
                parts = []
                for q in range(4):
                    block = got[32 * g + 8 * q : 32 * g + 8 * q + 8]
                    deep = block[:, 2:3] * 128.0 + block[:, 3:4]
                    parts.append([jnp.broadcast_to(v, (8, 128)) for v in (block[:, 0:1], block[:, 1:2], deep, block[:, 4:5])])
                for k in range(4):
                    value = parts[0][k]
                    for q in range(1, 4):
                        value = jnp.where(quarter == q, parts[q][k], value)
                    own_ref[k, mxu * (GROUPS // 2) + g] = value

        zs, ws = own_ref[2], own_ref[3]
        z_min = jnp.min(jnp.min(jnp.where(ws > 0.0, zs, 1e6), axis=1), axis=1, keepdims=True)
        z_max = jnp.max(jnp.max(jnp.where(ws > 0.0, zs, -1e6), axis=1), axis=1, keepdims=True)
        lane = lax.broadcasted_iota(jnp.int32, (GROUPS, 128), 1)
        chunk = lane.astype(F32) * 2.0
        even = jnp.full((GROUPS, 128), float(DUMMY), F32)
        odd = even
        total = jnp.zeros((GROUPS, 1), F32)
        lane8 = lax.broadcasted_iota(jnp.int32, (8, 128), 1)
        rows_ref[DUMMY] = jnp.zeros((8, 128), F32)
        for d in (8, 1, 6, 3, 4, 0, 2, 5, 7):
            if d < 8:

                @pl.when(present(*DIRS[d]))
                def _():
                    copy(7 - d).wait_recv()

            src = lists_ref.at[8] if d == 8 else got_ref.at[d]
            z_row = jnp.where(src[3:4, :] > 0.0, src[2:3, :], 2e6)
            low = jnp.sum(jnp.where(z_row < z_min - float(REACH), 1.0, 0.0), axis=1, keepdims=True)
            high = jnp.sum(jnp.where(z_row <= z_max + float(REACH), 1.0, 0.0), axis=1, keepdims=True)
            first = jnp.floor(low * (1.0 / STEP))
            count = jnp.where(high > low, jnp.floor((high - STEP * first + 31.0) * (1.0 / 32.0)), 0.0)
            at = chunk - total
            even = jnp.where((at >= 0.0) & (at < count), at * 2.0 + (first + float(ROWS * d)), even)
            at = at + 1.0
            odd = jnp.where((at >= 0.0) & (at < count), at * 2.0 + (first + float(ROWS * d)), odd)
            total = total + count
            parts = []
            for t in range(4):
                block = src[:, 128 * t : 128 * t + 128]
                block = jnp.concatenate([block, block], axis=0)
                for k in range(4):
                    part = block if k == 0 else pltpu.roll(block, 128 - 32 * k, 1)
                    part = jnp.where(lane8 < 32, part, pltpu.roll(part, 32, 1))
                    part = jnp.where(lane8 < 64, part, pltpu.roll(part, 64, 1))
                    parts.append(part)
            turned = [pltpu.roll(part, 16, 1) for part in parts] + [jnp.zeros((8, 128), F32)]
            for k in range(16):
                rows_ref[ROWS * d + 2 * k] = parts[k]
                rows_ref[ROWS * d + 2 * k + 1] = jnp.where((lane8 & 31) < 16, turned[k], turned[k + 1])
        units = jnp.floor((total + 1.0) * 0.5)
        name = lax.broadcasted_iota(jnp.int32, (GROUPS, 128), 0).astype(F32)
        number = jnp.sum(jnp.where((name >= begin) & (name < end), units, 0.0), axis=0, keepdims=True)
        turns = jnp.floor((number + 3.0) * 0.25)
        extra = 4.0 * turns - number
        units = units + jnp.sum(jnp.where(name == end - 1.0, extra, 0.0), axis=1, keepdims=True)
        skip = 4.0 * EARLY
        other = lane.astype(F32)
        units_row = jnp.sum(jnp.where(name == other, units, 0.0), axis=0, keepdims=True)
        origin = jnp.zeros((GROUPS, 1), F32)
        for r in range(SUBREGIONS):
            origin = jnp.where(name[:, 0:1] >= starts[r], starts[r], origin)
        passed = jnp.sum(jnp.where((other < name) & (other >= origin), units_row, 0.0), axis=1, keepdims=True)
        hit = (name >= begin) & (name < end) & (passed <= skip) & (skip < passed + units)
        found = jnp.sum(jnp.where(hit, 1.0, 0.0), axis=0, keepdims=True)
        start_g = jnp.sum(jnp.where(hit, name, 0.0), axis=0, keepdims=True)
        start_b = jnp.sum(jnp.where(hit, skip - passed, 0.0), axis=0, keepdims=True)
        real = lane_row < SUBREGIONS
        late = jnp.where(real, jnp.maximum(turns - EARLY, 1.0), float(1 << 18))
        start_g = jnp.where(found > 0.0, start_g, float(GROUPS))
        open_g = jnp.where(real & (begin < end), begin, float(GROUPS))
        table = jnp.where(lane == 127, units, even + 512.0 * odd)
        idle = jnp.where(lane_row == 127, float(1 << 20), float(DUMMY * 513))
        tail = [idle, late, start_g, start_b, open_g, end, jnp.zeros((2, 128), F32)]
        table_ref[...] = jnp.concatenate([table] + tail, axis=0).astype(jnp.int32)
        for d, (da, db) in enumerate(DIRS):

            @pl.when(present(da, db))
            def _():
                copy(d).wait_send()

    pl.run_scoped(
        body,
        pltpu.ACC(0)((16, 256), F32),
        pltpu.ACC(1)((16, 256), F32),
        pltpu.ACC(0)((16, 256), F32),
        pltpu.ACC(1)((16, 256), F32),
        pltpu.ACC(0)((GROUPS * 16, 256), F32),
        pltpu.ACC(1)((GROUPS * 16, 256), F32),
    )


def send_call(coords, weights, live):
    far = pl.BlockSpec(memory_space=pltpu.HBM)
    return pl.pallas_call(
        send_kernel,
        out_shape=(
            jax.ShapeDtypeStruct((GROUPS + 8, 128), jnp.int32),
            jax.ShapeDtypeStruct((DUMMY + 1, 8, 128), F32),
            jax.ShapeDtypeStruct((4, GROUPS, 8, 128), F32),
        ),
        in_specs=[far] * 3,
        out_specs=[pl.BlockSpec(memory_space=pltpu.VMEM)] * 3,
        scratch_shapes=[
            pltpu.VMEM((3, 1, 1, PART_DEV), jnp.int32),
            pltpu.VMEM((1, 1, PART_DEV), BF16),
            pltpu.VMEM((1, 1), jnp.int32),
            pltpu.VMEM((9, 4, PART_DEV), F32),
            pltpu.VMEM((8, 4, PART_DEV), F32),
            pltpu.SemaphoreType.DMA((3,)),
            pltpu.SemaphoreType.DMA((8,)),
            pltpu.SemaphoreType.DMA((8,)),
        ],
        compiler_params=pltpu.CompilerParams(collective_id=0, has_side_effects=True, vmem_limit_bytes=12 << 20),
    )(*[pltpu.with_memory_space_constraint(v, pltpu.HBM) for v in (coords, weights)], live)


LOG_SCALE = (S_BINS / 4.0) / math.log2(10.0)
LOG_BASE = -4.515457845
LEVELS_U = 24
LEVELS_V = 25
V_ROWS = 208
BINS = (2, TILES, 16, 128)
ENGINE = (
    ((2, 256, 128 * TILES), BF16),
    ((2, V_ROWS, 128 * TILES), BF16),
    (BINS, BF16),
    (BINS, BF16),
    (BINS, BF16),
    ((2, 2, 16, 128), BF16),
)


def engine(table_sm, rows_ref, own_ref, hot_u, hot_v, bin_u, bin_v, far_w, own_w):
    zero = jnp.zeros((16, 128), BF16)
    for half in range(2):
        hot_u[half, 8 * LEVELS_U :, :] = jnp.zeros((256 - 8 * LEVELS_U, 128 * TILES), BF16)

    def index(state, advance):
        for half in range(2):
            for mxu in range(2):
                g, b = state[0], state[1]
                group = jnp.minimum(g, GROUPS - 1)
                xi, yi, zi, wi = own_ref[0, group], own_ref[1, group], own_ref[2, group], own_ref[3, group]
                own_w[half, mxu] = jnp.concatenate([wi, wi], axis=0).astype(BF16)
                pair = table_sm[g, b]
                for t, row in ((2 * mxu, pair & 511), (2 * mxu + 1, pair >> 9)):
                    dx = xi - rows_ref[row, 0:1, :]
                    dy = yi - rows_ref[row, 1:2, :]
                    dz = zi - rows_ref[row, 2:3, :]
                    far_w[half, t] = jnp.broadcast_to(rows_ref[row, 3:4, :].astype(BF16), (16, 128))
                    dx2 = dx * dx
                    q = dx2 + dy * dy + dz * dz
                    s = jnp.floor(jnp.log2(q + 0.48) * LOG_SCALE + LOG_BASE)
                    near = jnp.floor(jnp.abs(dx) * lax.rsqrt(q) * float(MU_BINS) + 0.5)
                    mu = jnp.where(near * near * q > dx2 * float(MU_BINS * MU_BINS), near - 1.0, near)
                    c = s * float(MU_BINS) + jnp.minimum(mu, MU_BINS - 1.0)
                    u = jnp.floor(c * (1.0 / LEVELS_V) + 0.01)
                    v = c - u * float(LEVELS_V)
                    bin_u[half, t] = jnp.concatenate([u, u - 1.0], axis=0).astype(BF16)
                    bin_v[half, t] = jnp.concatenate([v, v - 1.0], axis=0).astype(BF16)
                state = advance(*state)
        return state

    def fill(half):
        for t in range(TILES):
            u2, v2, w_far, w_own = bin_u[half, t], bin_v[half, t], far_w[half, t], own_w[half, t // 2]
            lanes = slice(128 * t, 128 * t + 128)
            for k in range(LEVELS_U // 2):
                hot_u[half, 16 * k : 16 * k + 16, lanes] = jnp.where(u2 == jnp.bfloat16(2 * k), w_far, zero)
            for k in range(V_ROWS // 16):
                hot_v[half, 16 * k : 16 * k + 16, lanes] = jnp.where(v2 == jnp.bfloat16(2 * k), w_own, zero)

    def push(half):
        for mxu in range(2):
            pltpu.matmul_push_rhs(hot_u[half, :, 256 * mxu : 256 * mxu + 256], staging_register=half, mxu_index=mxu, transpose=True)

    def multiply(half, accs):
        for mxu in range(2):
            pltpu.matmul_acc_lhs(accs[mxu], hot_v[half, :, 256 * mxu : 256 * mxu + 256], load_staged_rhs=half)

    def run(state, advance, trips, sets, drain):
        state = index(state, advance)
        for half in range(2):
            fill(half)
            push(half)
        state = index(state, advance)
        for r in range(SUBREGIONS):

            def trip(_, state):
                for half in range(2):
                    multiply(half, sets[r % 2])
                for half in range(2):
                    fill(half)
                    push(half)
                return index(state, advance)

            state = lax.fori_loop(0, trips(r), trip, state)
            if r > 0:
                drain(r - 1, sets[(r - 1) % 2])
        last = sets[(SUBREGIONS - 1) % 2]
        for half in range(2):
            multiply(half, last)
        drain(SUBREGIONS - 1, last)

    return run


def count_kernel(table_ref, rows_ref, own_ref, out_ref, table_sm, sem):
    def body(a0, a1, b0, b1, *buffers):
        copy = pltpu.make_async_copy(table_ref, table_sm, sem)
        copy.start()
        for acc in (a0, a1, b0, b1):
            pltpu.matmul_pop(acc)
        run = engine(table_sm, rows_ref, own_ref, *buffers)
        copy.wait()

        def advance(g, b, left, region):
            over = b + 1 >= table_sm[g, 127]
            left = left - 1
            done = left <= 0
            region = jnp.where(done, jnp.minimum(region + 1, SUBREGIONS), region)
            b = jnp.where(done, table_sm[GROUPS + 3, region], jnp.where(over, 0, b + 1))
            g = jnp.where(done, table_sm[GROUPS + 2, region], jnp.where(over, g + 1, g))
            return g, b, jnp.where(done, 4 * table_sm[GROUPS + 1, region], left), region

        def drain(r, accs):
            out_ref[r] = pltpu.matmul_pop(accs[0]) + pltpu.matmul_pop(accs[1])

        state = (table_sm[GROUPS + 2, 0], table_sm[GROUPS + 3, 0], 4 * table_sm[GROUPS + 1, 0], jnp.int32(0))
        run(state, advance, lambda r: table_sm[GROUPS + 1, r], ((a0, a1), (b0, b1)), drain)

    pl.run_scoped(
        body,
        pltpu.ACC(0)((V_ROWS, 256), F32),
        pltpu.ACC(1)((V_ROWS, 256), F32),
        pltpu.ACC(0)((V_ROWS, 256), F32),
        pltpu.ACC(1)((V_ROWS, 256), F32),
        *(pltpu.VMEM(shape, dtype) for shape, dtype in ENGINE),
    )


def count_call(table, rows, own):
    vmem = pl.BlockSpec(memory_space=pltpu.VMEM)
    return pl.pallas_call(
        count_kernel,
        out_shape=jax.ShapeDtypeStruct((SUBREGIONS, V_ROWS, 256), F32),
        in_specs=[vmem, vmem, vmem],
        out_specs=vmem,
        scratch_shapes=[pltpu.SMEM((GROUPS + 8, 128), jnp.int32), pltpu.SemaphoreType.DMA],
        compiler_params=pltpu.CompilerParams(vmem_limit_bytes=6 << 20),
    )(table, rows, own)


def total_kernel(skies, counts_ref, table_ref, rows_ref, own_ref, packed_ref, total_ref, sum_ref, sent_ref, land_ref, table_sm, sem, send_sem, recv_sem):
    shell, sky = lax.axis_index("shell"), lax.axis_index("sky")
    barrier = pltpu.get_barrier_semaphore()
    load = pltpu.make_async_copy(table_ref, table_sm, sem)
    load.start()
    for k in range(1, skies):
        pl.semaphore_signal(barrier, inc=1, device_id=(shell, lax.rem(sky + k, skies)), device_id_type=MESH)

    def copy(k):
        return pltpu.make_async_remote_copy(
            src_ref=sent_ref,
            dst_ref=land_ref.at[k - 1],
            send_sem=send_sem.at[k - 1],
            recv_sem=recv_sem.at[k - 1],
            device_id=(shell, lax.rem(sky + k, skies)),
            device_id_type=MESH,
        )

    def body(a0, a1, b0, b1, small, large, pick_ref, *buffers):
        for acc in (a0, a1, b0, b1, small, large):
            pltpu.matmul_pop(acc)
        lane_in = lax.broadcasted_iota(jnp.int32, (256, 256), 0) >> 3
        lane_out = lax.broadcasted_iota(jnp.int32, (256, 256), 1)
        for k in range(4):
            pick_ref[k] = jnp.where(lane_in + 32 * k == lane_out, 1.0, 0.0).astype(BF16)
        run = engine(table_sm, rows_ref, own_ref, *buffers)
        load.wait()

        def advance(g, b, left, region):
            over = b + 1 >= table_sm[g, 127]
            b = jnp.where(over, 0, b + 1)
            g = jnp.where(over, g + 1, g)
            g = jnp.where(g >= table_sm[GROUPS + 5, region], GROUPS, g)
            left = left - 1
            done = left <= 0
            region = jnp.where(done, jnp.minimum(region + 1, SUBREGIONS), region)
            g = jnp.where(done, table_sm[GROUPS + 4, region], g)
            return g, jnp.where(done, 0, b), jnp.where(done, 4 * EARLY, left), region

        def drain(r, accs):
            sum_ref[r] = counts_ref[r] + (pltpu.matmul_pop(accs[0]) + pltpu.matmul_pop(accs[1]))

        state = (table_sm[GROUPS + 4, 0], jnp.int32(0), jnp.int32(4 * EARLY), jnp.int32(0))
        run(state, advance, lambda r: EARLY, ((a0, a1), (b0, b1)), drain)

        diagonal = lax.broadcasted_iota(jnp.int32, (V_ROWS, 256), 0) & 7 == lax.broadcasted_iota(jnp.int32, (V_ROWS, 256), 1) & 7

        def folded(block):
            block = jnp.where(diagonal, block, 0.0).reshape(V_ROWS // 8, 8, 256)
            return jnp.concatenate([jnp.sum(block, axis=1), jnp.zeros((32 - V_ROWS // 8, 256), F32)], axis=0)

        def pack(blocks, acc):
            size = 8 * len(blocks)
            for k in range(4):
                rows = jnp.concatenate([block[8 * k : 8 * k + 8] for block in blocks], axis=0)
                high = rows.astype(BF16)
                rest = rows - high.astype(F32)
                middle = rest.astype(BF16)
                low = (rest - middle.astype(F32)).astype(BF16)
                parts = [high.astype(F32), middle.astype(F32), low.astype(F32)]
                if size == 8:
                    parts.append(jnp.zeros((8, 256), F32))
                pltpu.matmul_push_rhs(pick_ref[k], staging_register=0, mxu_index=0)
                pltpu.matmul_acc_lhs(acc, jnp.concatenate(parts, axis=0).astype(BF16), load_staged_rhs=0)
            got = pltpu.matmul_pop(acc)
            return (got[0:size] + got[size : 2 * size] + got[2 * size : 3 * size])[:, 0:128]

        every = sum_ref[0]
        for r in range(1, SUBREGIONS):
            every = every + sum_ref[r]
        mine = pack([folded(every)], small)
        sent_ref[...] = mine
        pl.semaphore_wait(barrier, skies - 1)
        for k in range(1, skies):
            copy(k).start()
        packed_ref[...] = pack([folded(sum_ref[r]) for r in range(SUBREGIONS)], large)
        total = mine
        for k in range(1, skies):
            copy(k).wait_recv()
            total = total + land_ref[k - 1]
        total_ref[...] = total
        for k in range(1, skies):
            copy(k).wait_send()

    pl.run_scoped(
        body,
        pltpu.ACC(0)((V_ROWS, 256), F32),
        pltpu.ACC(1)((V_ROWS, 256), F32),
        pltpu.ACC(0)((V_ROWS, 256), F32),
        pltpu.ACC(1)((V_ROWS, 256), F32),
        pltpu.ACC(0)((32, 256), F32),
        pltpu.ACC(0)((24 * SUBREGIONS, 256), F32),
        pltpu.VMEM((4, 256, 256), BF16),
        *(pltpu.VMEM(shape, dtype) for shape, dtype in ENGINE),
    )


def total_call(counts, table, rows, own):
    skies = lax.axis_size("sky")
    vmem = pl.BlockSpec(memory_space=pltpu.VMEM)
    return pl.pallas_call(
        functools.partial(total_kernel, skies),
        out_shape=(jax.ShapeDtypeStruct((8 * SUBREGIONS, 128), F32), jax.ShapeDtypeStruct((8, 128), F32)),
        in_specs=[vmem] * 4,
        out_specs=(vmem, vmem),
        scratch_shapes=[
            pltpu.VMEM((SUBREGIONS, V_ROWS, 256), F32),
            pltpu.VMEM((8, 128), F32),
            pltpu.VMEM((skies - 1, 8, 128), F32),
            pltpu.SMEM((GROUPS + 8, 128), jnp.int32),
            pltpu.SemaphoreType.DMA,
            pltpu.SemaphoreType.DMA((skies - 1,)),
            pltpu.SemaphoreType.DMA((skies - 1,)),
        ],
        compiler_params=pltpu.CompilerParams(collective_id=1, has_side_effects=True, vmem_limit_bytes=10 << 20),
    )(counts, table, rows, own)


def edge_values():
    return [int(4.0 * 10.0 ** (4.0 * level / S_BINS) + 0.5) for level in range(S_BINS + 1)]


def bin_scale(patches):
    edges = edge_values()
    factor = SIDE_CELLS * SIDE_CELLS * SPAN_CELLS / (patches * PART_DEV * PART_DEV)
    values = []
    for level in range(S_BINS):
        volume = 4.0 * math.pi / 3.0 * (edges[level + 1] ** 1.5 - edges[level] ** 1.5) / MU_BINS
        values = values + [factor / volume] * MU_BINS
    return jnp.asarray(values, dtype=F32)


def unpacked(x):
    x = x.reshape(-1, 8, 4, 32).transpose(0, 3, 2, 1).reshape(-1, 32, 32)
    return x[:, :LEVELS_U, :LEVELS_V].reshape(-1, S_BINS * MU_BINS)


def local(coords, weights, live):
    tables = send_call(coords, weights, live)
    packed, total = total_call(count_call(*tables), *tables)
    leave = total[None] - packed.reshape(SUBREGIONS, 8, 128)
    return (unpacked(leave) * bin_scale(lax.axis_size("sky"))[None, :])[None]


def solution(mesh):
    in_specs = (P(None, "shell", "sky", None), P("shell", "sky", None), P("shell", "sky"))
    out_specs = P("shell", "sky", None)
    return jax.shard_map(local, mesh=mesh, in_specs=in_specs, out_specs=out_specs, check_vma=False)
```
